256 devices in a mesh: tm: 64 (over x, z, core), env: 4 (over y).
Axes of the slice: x: 4, y: 4, z: 8, core: 2. Of those that a mesh axis runs over, the one named last changes fastest.
Arguments:
- init_state: float32 [70, 1024], P(None, 'env'), may hold values from -6 to 6
- torque: float32 [256, 35, 1024], P('tm', None, 'env'), may hold values from -192 to 192
- contact: int32 [256, 1024], P('tm', 'env'), may hold values 0 or 1
- mass_inverse: float32 [128, 35, 35], P('tm'), may hold values from -0.014 to 1.5, as said below
- stiffness: float32 [35], replicated, may hold values from 10 to 100
- damping: float32 [35], replicated, may hold values from 0.5 to 5
- gravity: float32 [35], replicated, may hold values from 1 to 10
- contact_stiffness: float32 [35], replicated, may hold values from 20 to 100
- contact_damping: float32 [35], replicated, may hold values from 0.5 to 3
Outputs:
- final_states: float32 [128, 70, 1024], P('tm', None, 'env')
- corrections: float32 [3, 1024], P(None, 'env')
The draws below stay inside these ranges and needn't reach their ends.
Inputs may be any that keep to these rules, and one draw needn't show every extreme that they name: `mass_inverse`: each matrix is symmetric, and each diagonal entry exceeds the sum of the magnitudes of the other entries of its row.
All inputs are finite; a program needn't handle non-finite values. No bound on the sum of `contact` on one device may be relied on, other than what follows from the above.
Results may differ from the reference program's by a relative error of at most 0.00025.
Values sent between devices are 32-bit elements; how exact they have to be, the bound alone decides.
A program may use at most 64 MiB of HBM per device.

```python
import math
import jax
import jax.numpy as jnp
from jax import lax

DOF = 35
STATE = 70
HS = 2
SUB = 32
ITERS = 3
SLICES = 128
STEPS = 256
ENV = 1024


def draw_mass_inverse(key, part):
    key_diag = jax.random.fold_in(key, 11)
    key_off = jax.random.fold_in(key, 12)
    diagonal = jax.random.uniform(key_diag, (SLICES, DOF), jnp.float32, 0.5, 1.5)
    raw = jnp.clip(0.008 * jax.random.normal(key_off, (SLICES, DOF, DOF), jnp.float32), -0.014, 0.014)
    upper = jnp.triu(raw, 1)
    return upper + jnp.swapaxes(upper, 1, 2) + diagonal[:, :, None] * jnp.eye(DOF, dtype=jnp.float32)


def touch_ends(values, own_key, low, largest):
    spot = [jax.random.randint(jax.random.fold_in(own_key, axis), (), 0, length) for axis, length in enumerate(values.shape)]
    widest = values.shape.index(max(values.shape))
    neighbour = spot[:widest] + [(spot[widest] + 1) % values.shape[widest]] + spot[widest + 1:]
    return values.at[tuple(spot)].set(low).at[tuple(neighbour)].set(largest)


def shard_levels(key, extent, cuts, low, largest):
    factor_of, own = 1.0, jax.random.fold_in(key, 6)
    for position, shards_of in cuts:
        draws = jnp.exp(jax.random.uniform(jax.random.fold_in(own, position), (shards_of,), jnp.float32, low / len(cuts), largest / len(cuts)))
        factor_of = factor_of * jnp.repeat(draws, extent[position] // shards_of).reshape([-1 if axis == position else 1 for axis in range(len(extent))])
    return factor_of


def gaussian(own_key, dims, deviation, most, shards=(), kind=jnp.bfloat16):
    array = jax.random.normal(own_key, dims, jnp.float32) * deviation
    if len(shards) > 0:
        array = shard_levels(own_key, dims, shards, -0.22, 0.18) * array
    return jnp.clip(array, min=-most, max=most).astype(kind)


def setup_inputs(seed: int = 0) -> dict:
    arg_keys = jax.random.split(jax.random.key(seed), 10)
    return {
        "init_state": gaussian(arg_keys[0], (STATE, ENV), 0.5, 6.0, ((1, 4),), jnp.float32),
        "torque": gaussian(arg_keys[1], (STEPS, DOF, ENV), 30.0, 192.0, ((0, 64), (2, 4)), jnp.float32),
        "contact": touch_ends((jax.random.randint(arg_keys[2], (STEPS, ENV), 0, 3) < 1).astype(jnp.int32), jax.random.fold_in(arg_keys[2], 1), 0, 1),
        "mass_inverse": draw_mass_inverse(jax.random.fold_in(arg_keys[9], 71), 0),
        "stiffness": jnp.clip(jnp.exp(jax.random.uniform(arg_keys[4], (DOF,), jnp.float32, math.log(10.0), math.log(100.0))), 10.0, 100.0),
        "damping": jnp.clip(jnp.exp(jax.random.uniform(arg_keys[5], (DOF,), jnp.float32, math.log(0.5), math.log(5.0))), 0.5, 5.0),
        "gravity": jnp.clip(jnp.exp(jax.random.uniform(arg_keys[6], (DOF,), jnp.float32, math.log(1.0), math.log(10.0))), 1.0, 10.0),
        "contact_stiffness": jnp.clip(jnp.exp(jax.random.uniform(arg_keys[7], (DOF,), jnp.float32, math.log(20.0), math.log(100.0))), 20.0, 100.0),
        "contact_damping": jnp.clip(jnp.exp(jax.random.uniform(arg_keys[8], (DOF,), jnp.float32, math.log(0.5), math.log(3.0))), 0.5, 3.0),
    }


step_length = 0.05

def exact_dot(left, right):
    return jnp.dot(left, right, precision=lax.Precision.HIGHEST, preferred_element_type=jnp.float32)

def coarse_one(state_now, torque_steps, mean_steps, inverse, params):
    stiffness, damping, gravity, contact_stiffness, contact_damping = params
    joint_pos = state_now[:DOF]
    joint_vel = state_now[DOF:]
    for step_pos in range(HS):
        spring = (stiffness + gravity + mean_steps[step_pos] * contact_stiffness)[:, None]
        friction = (damping + mean_steps[step_pos] * contact_damping)[:, None]
        force = torque_steps[step_pos] - spring * joint_pos - friction * joint_vel
        joint_vel = joint_vel + step_length * exact_dot(inverse, force)
        joint_pos = joint_pos + step_length * joint_vel
    return jnp.concatenate([joint_pos, joint_vel], axis=0)

def fine_one(state_now, torque_steps, contact_steps, inverse, params):
    stiffness, damping, gravity, contact_stiffness, contact_damping = params
    fine_dt = step_length / SUB
    joint_pair = (state_now[:DOF], state_now[DOF:])
    for step_pos in range(HS):
        torque_here = torque_steps[step_pos]
        contact_here = contact_steps[step_pos][None, :]

        def substep(counter, pair_now):
            joint_pos, joint_vel = pair_now
            force = torque_here - stiffness[:, None] * joint_pos - damping[:, None] * joint_vel - gravity[:, None] * jnp.sin(joint_pos) - contact_here * (contact_stiffness[:, None] * joint_pos + contact_damping[:, None] * joint_vel)
            joint_vel = joint_vel + fine_dt * exact_dot(inverse, force)
            joint_pos = joint_pos + fine_dt * joint_vel
            return (joint_pos, joint_vel)
        joint_pair = lax.fori_loop(0, SUB, substep, joint_pair)
    return jnp.concatenate([joint_pair[0], joint_pair[1]], axis=0)

def reference(init_state, torque, contact, mass_inverse, stiffness, damping, gravity, contact_stiffness, contact_damping):
    params = (stiffness, damping, gravity, contact_stiffness, contact_damping)
    torque_steps = torque.reshape(SLICES, HS, DOF, ENV)
    contact_steps = contact.astype(jnp.float32).reshape(SLICES, HS, ENV)
    mean_steps = lax.optimization_barrier(jnp.mean(contact_steps, axis=2))
    coarse_all = jax.vmap(coarse_one, in_axes=(0, 0, 0, 0, None))
    fine_all = jax.vmap(fine_one, in_axes=(0, 0, 0, 0, None))

    def chain(jumps):

        def advance(state_now, inputs):
            torque_here, mean_here, inverse, jump = inputs
            following = coarse_one(state_now, torque_here, mean_here, inverse, params) + jump
            return (following, following)
        unused, ends = lax.scan(advance, init_state, (torque_steps, mean_steps, mass_inverse, jumps))
        return ends
    ends = chain(jnp.zeros((SLICES, STATE, ENV), jnp.float32))
    records = []
    for iteration in range(ITERS):
        starts = jnp.concatenate([init_state[None], ends[:-1]], axis=0)
        jumps = fine_all(starts, torque_steps, contact_steps, mass_inverse, params) - coarse_all(starts, torque_steps, mean_steps, mass_inverse, params)
        new_ends = chain(jumps)
        records.append(lax.optimization_barrier(jnp.max(jnp.sqrt(lax.optimization_barrier(jnp.sum((new_ends - ends) ** 2, axis=1))), axis=0)))
        ends = new_ends
    return (ends, jnp.stack(records))
```

```python
import functools
import math

import jax
import jax.numpy as jnp
from jax import lax
from jax.experimental import pallas as pl
from jax.experimental.pallas import tpu as pltpu
from jax.sharding import PartitionSpec as P

DOF = 35
STATE = 70
HS = 2
SUB = 32
ITERS = 3
LANES = 128
WIDE = 256
NZ = 8
CORES = 2
BLOCK = 4
UNROLL = 8

step_length = 0.05
fine_dt = step_length / SUB
TWO_PI = 2.0 * math.pi
MESH = pl.DeviceIdType.MESH
F32 = jnp.float32
BF16 = jnp.bfloat16

SIN = (
    6.283182818551188, -41.341421398631915, 81.59618387021051,
    -76.58010048603072, 41.205394649903326, -12.271261959178284,
)

ROWS_IN = 80
ROWS_OUT = 40
DEPTH = 72


def split(value):
    high = value.astype(BF16)
    return high, (value - high.astype(F32)).astype(BF16)


def dot(left, right):
    return jnp.dot(left, right, preferred_element_type=F32)


def through(state, weight):
    high, low = split(state)
    both = dot(jnp.concatenate([high, low], axis=1), weight)
    return both[:, :LANES] + both[:, LANES:]


def put(ref, n, value):
    high, low = split(value)
    ref[n, 0:LANES, 0:LANES] = high
    ref[n, LANES:, 0:LANES] = high
    ref[n, 0:LANES, LANES:] = low
    ref[n, LANES:, LANES:] = jnp.zeros_like(low)


def pad_rows(value, rows):
    return jnp.concatenate([value, jnp.zeros((rows - value.shape[0], value.shape[1]), F32)], axis=0)


class Plan:
    def __init__(self, slices):
        per = LANES // DOF
        self.groups = []
        self.where = []
        for first in range(0, slices, per):
            count = min(per, slices - first)
            base = len(self.groups) * LANES
            self.groups.append((base, first, count))
            for pos in range(count):
                self.where.append(base + pos * DOF)
        self.lanes = len(self.groups) * LANES


def kernel(
    tm, ny,
    init, torque, contact, minv, stiff, damp, gravity, cstiff, cdamp,
    out, corr_out,
    tx, rx, rowtx, rows, raw, inits,
    tq, spring, fric, grav, cspring, cfric, wgt, wtmp, ybuf, ubuf, ly, lu,
    cmap, pmap, qmap, bmap, ctmp, xs, ends_buf,
    btx, brx, stx, srx, otx, orx, ctx, crx,
    tsend, trecv, rsend, rrecv, bsend, brecv, ssend, srecv, osend, orecv, csend, crecv,
):
    nz = NZ
    half = nz // 2
    line = nz * CORES
    blocks = tm // line * CORES
    env_local = init.shape[1]
    epd = env_local // nz
    slices = HS * nz
    per_tile = LANES // epd
    tiles = env_local // LANES
    plan = Plan(slices)
    me_t = lax.axis_index("tm")
    me_e = lax.axis_index("env")
    x = me_t // line
    z = lax.rem(me_t // CORES, nz)
    c = lax.rem(me_t, CORES)
    block_t = x * CORES + c
    dest_core = z // half
    my_source = lax.rem(z, half) * CORES + c
    own_here = dest_core == c
    barrier = pltpu.get_barrier_semaphore()

    def source_index(i):
        return x * line + (c * half + i // CORES) * CORES + lax.rem(i, CORES)

    def dest_index(k):
        return x * line + lax.rem(z + k, nz) * CORES + dest_core

    def block_index(t):
        return t // CORES * line + z * CORES + lax.rem(t, CORES)

    @pl.loop(1, tm)
    def _(k):
        pl.semaphore_signal(
            barrier, inc=1, device_id={"tm": lax.rem(me_t + k, tm), "env": me_e}, device_id_type=MESH
        )

    @pl.loop(1, ny)
    def _(r):
        @pl.loop(0, nz)
        def _(i):
            pl.semaphore_signal(
                barrier, inc=1,
                device_id={"tm": source_index(i), "env": lax.rem(me_e + r, ny)},
                device_id_type=MESH,
            )

    lane_of = lax.broadcasted_iota(jnp.int32, (1, LANES), 1)
    lane_group = lane_of // epd

    raw[...] = jnp.zeros(raw.shape, F32)
    hits = contact[...].astype(F32)
    for k in range(2 * HS):
        raw[k, 0:DOF, :] = torque[:, k, :]
        raw[k, DOF : DOF + 1, :] = hits[k : k + 1, :]
    mtx = raw[0, :, 0:LANES] * 0.0
    wtmp[...] = jnp.zeros(wtmp.shape, F32)
    wtmp[0:DOF, 0:DOF] = minv[:, 0, :]
    wtmp[0:DOF, LANES // 2 : LANES // 2 + DOF] = minv[:, 1, :]
    mtx = wtmp[0:40, :]
    for h in range(tiles):
        rolled = {}
        for k in range(2 * HS):
            v = raw[k, :, h * LANES : (h + 1) * LANES]
            for r in range(per_tile):
                rolled[k, r] = v if r == 0 else pltpu.roll(v, r * epd, 1)
        for q in range(per_tile):
            acc = rolled[0, (0 - q) % per_tile]
            for k in range(1, 2 * HS):
                acc = jnp.where(lane_group == k, rolled[k, (k - q) % per_tile], acc)
            tx[h * per_tile + q, 0:40, :] = acc
            tx[h * per_tile + q, 40:80, :] = mtx
    rowtx[...] = jnp.zeros(rowtx.shape, F32)
    rowtx[0 : 2 * HS, :] = jnp.broadcast_to(jnp.sum(hits, axis=1, keepdims=True), (2 * HS, LANES))

    pl.semaphore_wait(barrier, tm - 1 + (ny - 1) * nz)

    def in_copy(k):
        return pltpu.make_async_remote_copy(
            src_ref=tx.at[lax.rem(z + k, nz)],
            dst_ref=rx.at[my_source],
            send_sem=tsend.at[k],
            recv_sem=trecv.at[my_source],
            device_id={"tm": dest_index(k), "env": me_e},
            device_id_type=MESH,
        )

    def in_arrival(i):
        return pltpu.make_async_remote_copy(
            src_ref=tx.at[0],
            dst_ref=rx.at[i],
            send_sem=tsend.at[0],
            recv_sem=trecv.at[i],
            device_id={"tm": dest_index(0), "env": me_e},
            device_id_type=MESH,
        )

    def row_copy(k, r):
        return pltpu.make_async_remote_copy(
            src_ref=rowtx,
            dst_ref=rows.at[my_source, me_e],
            send_sem=rsend.at[k, r],
            recv_sem=rrecv.at[my_source, r],
            device_id={"tm": dest_index(k), "env": lax.rem(me_e + r, ny)},
            device_id_type=MESH,
        )

    def row_arrival(i, r):
        return pltpu.make_async_remote_copy(
            src_ref=rowtx,
            dst_ref=rows.at[i, lax.rem(me_e - r + ny, ny)],
            send_sem=rsend.at[0, r],
            recv_sem=rrecv.at[i, r],
            device_id={"tm": dest_index(0), "env": lax.rem(me_e + r, ny)},
            device_id_type=MESH,
        )

    def other(k):
        return jnp.logical_not(jnp.logical_and(own_here, k == 0))

    def other_source(i):
        return jnp.logical_not(jnp.logical_and(own_here, i == my_source))

    @pl.loop(0, nz)
    def _(k):
        @pl.when(other(k))
        def _():
            in_copy(k).start()
            row_copy(k, 0).start()

        @pl.loop(1, ny)
        def _(r):
            row_copy(k, r).start()

    @pl.when(own_here)
    def _():
        rx[my_source] = tx[z]
        rows[my_source, me_e] = rowtx[...]

    ratio = float(SUB)
    stiff, damp, gravity, cstiff, cdamp = (r[...] for r in (stiff, damp, gravity, cstiff, cdamp))
    to_u = TWO_PI / fine_dt
    scale = jnp.where(lane_of < DOF, TWO_PI, to_u)
    shrink = jnp.where(lane_of < DOF, 1.0 / TWO_PI, 1.0 / to_u)

    for ref in (tq, spring, fric, grav, cspring, cfric, ybuf, ubuf, ly, lu):
        ref[...] = jnp.zeros(ref.shape, ref.dtype)
    ctmp[...] = jnp.zeros(ctmp.shape, F32)
    for h in range(tiles):
        inits[h * LANES : (h + 1) * LANES, :] = (
            pad_rows(init[:, h * LANES : (h + 1) * LANES], LANES).T * shrink
        )
    start_state = inits[pl.ds(pl.multiple_of(z * epd, epd), epd), :]
    deep = DEPTH + epd
    rank = lax.broadcasted_iota(jnp.int32, (deep, DOF), 0)
    col = lax.broadcasted_iota(jnp.int32, (deep, DOF), 1)
    for n in range(slices):
        cut = pl.ds(plan.where[n], DOF)
        ly[:, cut] = jnp.where(rank == col, 1.0, 0.0)
        lu[:, cut] = jnp.where(rank == col + DOF, 1.0, 0.0)
        grav[:, cut] = jnp.broadcast_to(gravity, (1, DOF))

    @pl.loop(0, nz)
    def _(i):
        @pl.when(other_source(i))
        def _():
            in_arrival(i).wait_recv()
            row_arrival(i, 0).wait_recv()

        @pl.loop(1, ny)
        def _(r):
            row_arrival(i, r).wait_recv()

    for i in range(nz):
        turned = pad_rows(rx[i], LANES).T
        means = jnp.sum(rows[i], axis=0)[0 : 2 * HS, 0:DOF] * (1.0 / (env_local * ny))
        for a in range(HS):
            cut = pl.ds(plan.where[HS * i + a], DOF)
            for j in range(HS):
                k = a * HS + j
                piece = turned[k * epd : (k + 1) * epd, :]
                hit = piece[:, DOF : DOF + 1]
                mean = means[k : k + 1, :]
                tq[j, :, cut] = piece[:, 0:DOF]
                spring[j, :, cut] = TWO_PI * (stiff + hit * cstiff)
                fric[j, :, cut] = to_u * (damp + hit * cdamp)
                cspring[j, :, cut] = TWO_PI * (stiff + gravity + mean * cstiff)
                cfric[j, :, cut] = to_u * (damp + mean * cdamp)

    for g, (base, first, count) in enumerate(plan.groups):
        wtmp[...] = jnp.zeros(wtmp.shape, F32)
        for pos in range(count):
            src, a = divmod(first + pos, HS)
            lane = a * (LANES // 2)
            wtmp[pl.ds(pos * DOF, DOF), pl.ds(pos * DOF, DOF)] = (
                fine_dt * fine_dt / TWO_PI
            ) * rx[src, 40 : 40 + DOF, lane : lane + DOF]
        put(wgt, g, wtmp[...])

    def product(force, g):
        return through(force, wgt[g])

    for g, (base, first, count) in enumerate(plan.groups):
        cut = pl.ds(base, LANES)
        y, u = ly[:, cut], lu[:, cut]
        for j in range(HS):
            push = jnp.concatenate([jnp.zeros((DEPTH, LANES), F32), tq[j, :, cut]], axis=0)
            force = push - cspring[j, :, cut] * y - cfric[j, :, cut] * u
            u = u + ratio * product(force, g)
            y = y + ratio * u
        ly[:, cut] = y
        lu[:, cut] = u
    offsets = []
    for n in range(slices):
        cut = pl.ds(plan.where[n], DOF)
        ctmp[0:DEPTH, 0:DOF] = ly[0:DEPTH, cut]
        ctmp[0:DEPTH, DOF : 2 * DOF] = lu[0:DEPTH, cut]
        put(cmap, n, ctmp[...])
        xs[n + 1, :, :] = jnp.zeros((epd, LANES), F32)
        xs[n + 1, :, 0:DOF] = ly[DEPTH:, cut]
        xs[n + 1, :, DOF : 2 * DOF] = lu[DEPTH:, cut]

    firsts = list(range(0, slices, BLOCK))
    running = {}
    for m in firsts:
        cut = pl.ds(plan.where[m], DOF)
        ctmp[0:DEPTH, 0:DOF] = ly[0:DEPTH, cut]
        ctmp[0:DEPTH, DOF : 2 * DOF] = lu[0:DEPTH, cut]
        running[m] = ctmp[0:DEPTH, :]
    whole = running[0]
    put(qmap, 0, pad_rows(running[0], LANES))
    for i in range(1, BLOCK):
        for m in firsts:
            running[m] = through(running[m], cmap[m + i])
            put(pmap, m + i, pad_rows(running[m], LANES))
            if m == 0:
                put(qmap, i, pad_rows(running[m], LANES))
    whole = running[0]
    for m in firsts[1:]:
        entry = whole
        for i in range(BLOCK):
            part = cmap if i == 0 else pmap
            whole = through(entry, part[m + i])
            put(qmap, m + i, pad_rows(whole, LANES))

    def sweep_to_end(ends):
        for i in range(1, BLOCK):
            for m in firsts:
                ends[m + i] = through(ends[m + i - 1], cmap[m + i]) + ends[m + i]
        for m in firsts[1:]:
            last = m + BLOCK - 1
            ends[last] = ends[last] + through(ends[m - 1], pmap[last])

    def sweep_rest(ends):
        for i in range(BLOCK - 1):
            for m in firsts[1:]:
                part = cmap if i == 0 else pmap
                ends[m + i] = ends[m + i] + through(ends[m - 1], part[m + i])

    def first_copy(d):
        return pltpu.make_async_remote_copy(
            src_ref=btx,
            dst_ref=brx.at[block_t],
            send_sem=bsend.at[d],
            recv_sem=brecv.at[d],
            device_id={"tm": block_index(block_t + d), "env": me_e},
            device_id_type=MESH,
        )

    def first_arrival(d):
        return pltpu.make_async_remote_copy(
            src_ref=btx,
            dst_ref=brx.at[block_t - d],
            send_sem=bsend.at[d],
            recv_sem=brecv.at[d],
            device_id={"tm": block_index(block_t - d), "env": me_e},
            device_id_type=MESH,
        )

    def sweep_copy(k, d):
        return pltpu.make_async_remote_copy(
            src_ref=stx.at[k],
            dst_ref=srx.at[k, block_t],
            send_sem=ssend.at[k, d],
            recv_sem=srecv.at[k, d],
            device_id={"tm": block_index(block_t + d), "env": me_e},
            device_id_type=MESH,
        )

    def sweep_arrival(k, d):
        return pltpu.make_async_remote_copy(
            src_ref=stx.at[k],
            dst_ref=srx.at[k, block_t - d],
            send_sem=ssend.at[k, d],
            recv_sem=srecv.at[k, d],
            device_id={"tm": block_index(block_t - d), "env": me_e},
            device_id_type=MESH,
        )

    def send_blocks(copy):
        @pl.loop(1, blocks)
        def _(d):
            @pl.when(block_t + d < blocks)
            def _():
                copy(d).start()

    def await_blocks(arrival):
        @pl.loop(1, blocks)
        def _(d):
            @pl.when(block_t - d >= 0)
            def _():
                arrival(d).wait_recv()

    def drain_blocks(copy):
        @pl.loop(1, blocks)
        def _(d):
            @pl.when(block_t + d < blocks)
            def _():
                copy(d).wait_send()

    ends = [xs[n + 1] for n in range(slices)]
    sweep_to_end(ends)
    btx[0:DEPTH, :] = whole
    btx[DEPTH:, :] = ends[slices - 1]
    send_blocks(first_copy)
    sweep_rest(ends)
    for n in range(slices):
        ends_buf[n] = ends[n]
    await_blocks(first_arrival)
    for t in range(blocks - 1):
        put(bmap, t, pad_rows(brx[t, 0:DEPTH, :], LANES))

    state = start_state
    entry = start_state
    for t in range(blocks - 1):
        state = through(state, bmap[t]) + brx[t, DEPTH:, :]
        entry = jnp.where(block_t == t + 1, state, entry)
    xs[0] = entry
    for n in range(slices):
        xs[n + 1] = ends_buf[n] + through(entry, qmap[n])

    def iteration(k, corrections):
        for n in range(slices):
            cut = pl.ds(plan.where[n], DOF)
            ybuf[:, cut] = xs[n, :, 0:DOF]
            ubuf[:, cut] = xs[n, :, DOF : 2 * DOF]
        for j in range(HS):

            def substep(counter, carry):
                result = []
                for g, (base, first, count) in enumerate(plan.groups):
                    y, u = carry[g]
                    cut = pl.ds(base, LANES)
                    t = y - jnp.round(y)
                    s = t * t
                    poly = jnp.full_like(s, SIN[-1])
                    for coef in SIN[-2::-1]:
                        poly = poly * s + coef
                    force = (
                        tq[j, :, cut]
                        - spring[j, :, cut] * y
                        - fric[j, :, cut] * u
                        - (grav[:, cut] * t) * poly
                    )
                    u = u + product(force, g)
                    y = y + u
                    result.append((y, u))
                return tuple(result)

            first_state = tuple(
                (ybuf[:, pl.ds(base, LANES)], ubuf[:, pl.ds(base, LANES)])
                for base, first, count in plan.groups
            )
            last = lax.fori_loop(0, SUB, substep, first_state, unroll=UNROLL)
            for g, (base, first, count) in enumerate(plan.groups):
                ybuf[:, pl.ds(base, LANES)] = last[g][0]
                ubuf[:, pl.ds(base, LANES)] = last[g][1]

        zero = jnp.zeros((epd, LANES - 2 * DOF), F32)
        ends = []
        for n in range(slices):
            cut = pl.ds(plan.where[n], DOF)
            ends.append(jnp.concatenate([ybuf[:, cut], ubuf[:, cut], zero], axis=1) - xs[n + 1])
        sweep_to_end(ends)
        stx[k] = ends[slices - 1]
        send_blocks(functools.partial(sweep_copy, k))
        sweep_rest(ends)
        for n in range(slices):
            ends_buf[n] = ends[n]
        await_blocks(functools.partial(sweep_arrival, k))
        state = jnp.zeros((epd, LANES), F32)
        entry = state
        for t in range(blocks - 1):
            state = through(state, bmap[t]) + srx[k, t] if t > 0 else srx[k, t]
            entry = jnp.where(block_t == t + 1, state, entry)
        xs[0] = xs[0] + entry
        worst = jnp.zeros((epd, 1), F32)
        for n in range(slices):
            change = ends_buf[n] + through(entry, qmap[n])
            real = change * scale
            worst = jnp.maximum(worst, jnp.sum(real * real, axis=1, keepdims=True))
            xs[n + 1] = xs[n + 1] + change
        return jnp.where(lane_of == k, jnp.sqrt(worst), corrections)

    corrections = lax.fori_loop(0, ITERS, iteration, jnp.zeros((epd, LANES), F32))

    ctx[...] = pad_rows(corrections, LANES).T[0:8, :]
    for i in range(nz):
        parts = []
        for a in range(HS):
            real = xs[HS * i + a + 1] * scale
            parts.append(real)
            parts.append(pltpu.roll(real, LANES - DOF, 1))
        otx[i] = jnp.concatenate(parts, axis=0).T[0:ROWS_OUT, :]

    def out_copy(i):
        return pltpu.make_async_remote_copy(
            src_ref=otx.at[i],
            dst_ref=orx.at[z],
            send_sem=osend.at[i],
            recv_sem=orecv.at[z],
            device_id={"tm": source_index(i), "env": me_e},
            device_id_type=MESH,
        )

    def out_arrival(k):
        return pltpu.make_async_remote_copy(
            src_ref=otx.at[0],
            dst_ref=orx.at[lax.rem(z + k, nz)],
            send_sem=osend.at[0],
            recv_sem=orecv.at[lax.rem(z + k, nz)],
            device_id={"tm": dest_index(k), "env": me_e},
            device_id_type=MESH,
        )

    def corr_copy(k):
        return pltpu.make_async_remote_copy(
            src_ref=ctx,
            dst_ref=crx.at[block_t, z],
            send_sem=csend.at[k],
            recv_sem=crecv.at[k],
            device_id={"tm": lax.rem(me_t + k, tm), "env": me_e},
            device_id_type=MESH,
        )

    @pl.loop(1, tm)
    def _(k):
        corr_copy(k).start()

    @pl.loop(0, nz)
    def _(i):
        @pl.when(other_source(i))
        def _():
            out_copy(i).start()

    crx[block_t, z] = ctx[...]

    @pl.when(own_here)
    def _():
        orx[z] = otx[my_source]

    @pl.loop(0, nz)
    def _(k):
        @pl.when(other(k))
        def _():
            out_arrival(k).wait_recv()

    for h in range(tiles):
        for k in range(2 * HS):
            a, half_state = divmod(k, 2)
            tile = None
            for q in range(per_tile):
                r = (q - k) % per_tile
                v = orx[h * per_tile + q]
                v = v if r == 0 else pltpu.roll(v, r * epd, 1)
                tile = v if tile is None else jnp.where(lane_group == q, v, tile)
            out[half_state * DOF : half_state * DOF + DOF, a, h * LANES : (h + 1) * LANES] = tile[0:DOF]

    @pl.loop(1, tm)
    def _(k):
        corr_copy(k).wait()

    worst = crx[0]
    for t in range(1, blocks):
        worst = jnp.maximum(worst, crx[t])
    for h in range(tiles):
        tile = worst[h * per_tile]
        for q in range(1, per_tile):
            tile = jnp.where(lane_group == q, pltpu.roll(worst[h * per_tile + q], q * epd, 1), tile)
        corr_out[:, h * LANES : (h + 1) * LANES] = tile[0:ITERS]

    @pl.loop(0, nz)
    def _(k):
        @pl.when(other(k))
        def _():
            in_copy(k).wait_send()
            row_copy(k, 0).wait_send()

        @pl.loop(1, ny)
        def _(r):
            row_copy(k, r).wait_send()

        @pl.when(other_source(k))
        def _():
            out_copy(k).wait_send()

    drain_blocks(first_copy)
    for k in range(ITERS):
        drain_blocks(functools.partial(sweep_copy, k))


def body(tm, env, init_state, torque, contact, mass_inverse, stiffness, damping, gravity,
         contact_stiffness, contact_damping):
    nz = NZ
    env_local = init_state.shape[1]
    epd = env_local // nz
    slices = HS * nz
    blocks = tm // (nz * CORES) * CORES
    plan = Plan(slices)
    groups = len(plan.groups)
    lanes = plan.lanes
    vm = pltpu.VMEM
    dma = pltpu.SemaphoreType.DMA
    vmem = pl.BlockSpec(memory_space=pltpu.VMEM)
    both = vm((HS, epd, lanes), F32)
    thin = vm((HS, 1, lanes), F32)
    deep = DEPTH + epd
    prm = [p.reshape(1, DOF) for p in (stiffness, damping, gravity, contact_stiffness, contact_damping)]
    states, corrections = pl.pallas_call(
        functools.partial(kernel, tm, env),
        out_shape=(
            jax.ShapeDtypeStruct((STATE, HS, env_local), F32),
            jax.ShapeDtypeStruct((ITERS, env_local), F32),
        ),
        in_specs=[vmem] * 9,
        out_specs=(vmem, vmem),
        scratch_shapes=[
            vm((nz, ROWS_IN, LANES), F32), vm((nz, ROWS_IN, LANES), F32),
            vm((8, LANES), F32), vm((nz, env, 8, LANES), F32),
            vm((2 * HS, 40, env_local), F32), vm((env_local, LANES), F32),
            both, both, both, vm((1, lanes), F32), thin, thin,
            vm((groups, WIDE, WIDE), BF16), vm((LANES, LANES), F32),
            vm((epd, lanes), F32), vm((epd, lanes), F32),
            vm((deep, lanes), F32), vm((deep, lanes), F32),
            vm((slices, WIDE, WIDE), BF16), vm((slices, WIDE, WIDE), BF16),
            vm((slices, WIDE, WIDE), BF16), vm((blocks, WIDE, WIDE), BF16),
            vm((LANES, LANES), F32),
            vm((slices + 1, epd, LANES), F32), vm((slices, epd, LANES), F32),
            vm((deep, LANES), F32), vm((blocks, deep, LANES), F32),
            vm((ITERS, epd, LANES), F32), vm((ITERS, blocks, epd, LANES), F32),
            vm((nz, ROWS_OUT, LANES), F32), vm((nz, ROWS_OUT, LANES), F32),
            vm((8, LANES), F32), vm((blocks, nz, 8, LANES), F32),
            dma((nz,)), dma((nz,)), dma((nz, env)), dma((nz, env)),
            dma((blocks,)), dma((blocks,)), dma((ITERS, blocks)), dma((ITERS, blocks)),
            dma((nz,)), dma((nz,)), dma((tm,)), dma((tm,)),
        ],
        compiler_params=pltpu.CompilerParams(collective_id=0, has_side_effects=True),
        name="parareal",
    )(
        init_state, torque.transpose(1, 0, 2), contact, mass_inverse.transpose(1, 0, 2), *prm
    )
    return states.transpose(1, 0, 2), corrections


def solution(mesh):
    placed = (
        P(None, "env"),
        P("tm", None, "env"),
        P("tm", "env"),
        P("tm", None, None),
        P(),
        P(),
        P(),
        P(),
        P(),
    )
    return jax.shard_map(
        functools.partial(body, mesh.shape["tm"], mesh.shape["env"]),
        mesh=mesh,
        in_specs=placed,
        out_specs=(P("tm", None, "env"), P(None, "env")),
        check_vma=False,
    )
```

```python
import functools
import math

import jax
import jax.numpy as jnp
from jax import lax
from jax.experimental import pallas as pl
from jax.experimental.pallas import tpu as pltpu
from jax.sharding import PartitionSpec as P

DOF = 35
STATE = 70
HS = 2
SUB = 32
ITERS = 3
LANES = 128
WIDE = 256
NZ = 8
CORES = 2
UNROLL = 32

step_length = 0.05
fine_dt = step_length / SUB
TWO_PI = 2.0 * math.pi
MESH = pl.DeviceIdType.MESH
F32 = jnp.float32
BF16 = jnp.bfloat16

SIN = (
    6.283182818551188, -41.341421398631915, 81.59618387021051,
    -76.58010048603072, 41.205394649903326, -12.271261959178284,
)

ROWS_IN = 56
FOLD = 36
KEEP = 80
ROWS_OUT = 40
DEPTH = 72


def split(value):
    high = value.astype(BF16)
    return high, (value - high.astype(F32)).astype(BF16)


def dot(left, right):
    return jnp.dot(left, right, preferred_element_type=F32)


def through(state, weight):
    high, low = split(state)
    both = dot(jnp.concatenate([high, low], axis=1), weight)
    return both[:, :LANES] + both[:, LANES:]


def clear(ref):
    ref[...] = jnp.zeros(ref.shape, ref.dtype)


def put(ref, n, value):
    high, low = split(value)
    rows = value.shape[0]
    ref[n, 0:rows, 0:LANES] = high
    ref[n, LANES : LANES + rows, 0:LANES] = high
    ref[n, 0:rows, LANES:] = low


def pad_rows(value, rows):
    return jnp.concatenate([value, jnp.zeros((rows - value.shape[0], value.shape[1]), F32)], axis=0)


class Plan:
    def __init__(self, slices):
        per = LANES // DOF
        self.groups = []
        self.where = []
        for first in range(0, slices, per):
            count = min(per, slices - first)
            base = len(self.groups) * LANES
            self.groups.append((base, first, count))
            for pos in range(count):
                self.where.append(base + pos * DOF)
        self.lanes = len(self.groups) * LANES


def kernel(
    tm, ny,
    init_hbm, torque_hbm, contact_hbm, minv_hbm, stiff_hbm, damp_hbm, gravity_hbm, cstiff_hbm, cdamp_hbm,
    out, corr_out,
    init, torque, contact, minv, stiff, damp, gravity, cstiff, cdamp,
    tx, rx, rowtx, rows, raw, inits,
    tq, spring, fric, grav, cspring, cfric, wgt, stage, wtmp, ybuf, ubuf, ly, lu,
    cmap, qmap, bmap, ctmp, xs, ends_buf,
    btx, brx, stx, srx, otx, orx, ctx, crx,
    lsem, tsend, trecv, rsend, rrecv, bsend, brecv, ssend, srecv, osend, orecv, csend, crecv,
):
    pairs = (
        (torque_hbm, torque), (contact_hbm, contact), (minv_hbm, minv), (init_hbm, init), (stiff_hbm, stiff),
        (damp_hbm, damp), (gravity_hbm, gravity), (cstiff_hbm, cstiff), (cdamp_hbm, cdamp),
    )
    local = [pltpu.make_async_copy(src, dst, lsem.at[i]) for i, (src, dst) in enumerate(pairs)]
    for copy in local:
        copy.start()
    nz = NZ
    half = nz // 2
    line = nz * CORES
    blocks = tm // line * CORES
    env_local = init.shape[1]
    epd = env_local // nz
    slices = HS * nz
    per_tile = LANES // epd
    tiles = env_local // LANES
    plan = Plan(slices)
    me_t = lax.axis_index("tm")
    me_e = lax.axis_index("env")
    x = me_t // line
    z = lax.rem(me_t // CORES, nz)
    c = lax.rem(me_t, CORES)
    block_t = x * CORES + c
    dest_core = z // half
    my_source = lax.rem(z, half) * CORES + c
    own_here = dest_core == c
    barrier = pltpu.get_barrier_semaphore()

    def source_index(i):
        return x * line + (c * half + i // CORES) * CORES + lax.rem(i, CORES)

    def dest_index(k):
        return x * line + lax.rem(z + k, nz) * CORES + dest_core

    def block_index(t):
        return t // CORES * line + z * CORES + lax.rem(t, CORES)

    @pl.loop(1, tm)
    def _(k):
        pl.semaphore_signal(
            barrier, inc=1, device_id={"tm": lax.rem(me_t + k, tm), "env": me_e}, device_id_type=MESH
        )

    @pl.loop(1, ny)
    def _(r):
        @pl.loop(0, nz)
        def _(i):
            pl.semaphore_signal(
                barrier, inc=1,
                device_id={"tm": source_index(i), "env": lax.rem(me_e + r, ny)},
                device_id_type=MESH,
            )

    for copy in local:
        copy.wait()
    lane_of = lax.broadcasted_iota(jnp.int32, (1, LANES), 1)
    lane_group = lane_of // epd

    raw[...] = jnp.zeros(raw.shape, F32)
    hits = contact[...].astype(F32)
    for k in range(2 * HS):
        raw[k, 0:DOF, :] = torque[:, k, :]
        raw[k, DOF : DOF + 1, :] = hits[k : k + 1, :]
    wtmp[...] = jnp.zeros(wtmp.shape, F32)
    wtmp[0:DOF, 0:DOF] = minv[:, 0, :]
    wtmp[40 : 40 + DOF, 0:DOF] = minv[:, 1, :]
    row_of = lax.broadcasted_iota(jnp.int32, (40, LANES), 0)
    lower = lane_of <= row_of
    packed = jnp.where(lower, wtmp[0:40, :], pltpu.roll(wtmp[40:80, :], 1, 1))
    last = jnp.concatenate([packed[32:40], jnp.zeros((8, LANES), F32)], axis=0)
    mtx = packed[0:16] + pltpu.roll(packed[16:32], FOLD, 1) + pltpu.roll(last, 2 * FOLD, 1)
    for h in range(tiles):
        rolled = {}
        for k in range(2 * HS):
            v = raw[k, :, h * LANES : (h + 1) * LANES]
            for r in range(per_tile):
                rolled[k, r] = v if r == 0 else pltpu.roll(v, r * epd, 1)
        for q in range(per_tile):
            acc = rolled[0, (0 - q) % per_tile]
            for k in range(1, 2 * HS):
                acc = jnp.where(lane_group == k, rolled[k, (k - q) % per_tile], acc)
            tx[h * per_tile + q, 0:40, :] = acc
            tx[h * per_tile + q, 40:ROWS_IN, :] = mtx
    totals = jnp.sum(hits, axis=1, keepdims=True)
    row = jnp.broadcast_to(totals[0:1], (1, LANES))
    for k in range(1, 2 * HS):
        row = jnp.where(lane_group == k, jnp.broadcast_to(totals[k : k + 1], (1, LANES)), row)
    rowtx[...] = row

    pl.semaphore_wait(barrier, tm - 1 + (ny - 1) * nz)

    def in_copy(k):
        return pltpu.make_async_remote_copy(
            src_ref=tx.at[lax.rem(z + k, nz)],
            dst_ref=rx.at[my_source],
            send_sem=tsend.at[k],
            recv_sem=trecv.at[my_source],
            device_id={"tm": dest_index(k), "env": me_e},
            device_id_type=MESH,
        )

    def in_arrival(i):
        return pltpu.make_async_remote_copy(
            src_ref=tx.at[0],
            dst_ref=rx.at[i],
            send_sem=tsend.at[0],
            recv_sem=trecv.at[i],
            device_id={"tm": dest_index(0), "env": me_e},
            device_id_type=MESH,
        )

    def row_copy(k, r):
        return pltpu.make_async_remote_copy(
            src_ref=rowtx,
            dst_ref=rows.at[my_source, me_e],
            send_sem=rsend.at[k, r],
            recv_sem=rrecv.at[my_source, r],
            device_id={"tm": dest_index(k), "env": lax.rem(me_e + r, ny)},
            device_id_type=MESH,
        )

    def row_arrival(i, r):
        return pltpu.make_async_remote_copy(
            src_ref=rowtx,
            dst_ref=rows.at[i, lax.rem(me_e - r + ny, ny)],
            send_sem=rsend.at[0, r],
            recv_sem=rrecv.at[i, r],
            device_id={"tm": dest_index(0), "env": lax.rem(me_e + r, ny)},
            device_id_type=MESH,
        )

    def other(k):
        return jnp.logical_not(jnp.logical_and(own_here, k == 0))

    def other_source(i):
        return jnp.logical_not(jnp.logical_and(own_here, i == my_source))

    @pl.loop(0, nz)
    def _(k):
        @pl.when(other(k))
        def _():
            row_copy(k, 0).start()

        @pl.loop(1, ny)
        def _(r):
            row_copy(k, r).start()

    for k in sorted(range(nz), key=lambda k: -min(k, nz - k)):
        @pl.when(other(k))
        def _(k=k):
            in_copy(k).start()

    @pl.when(own_here)
    def _():
        rx[my_source] = tx[z]
        rows[my_source, me_e] = rowtx[...]

    ratio = float(SUB)
    stiff, damp, gravity, cstiff, cdamp = (r[...] for r in (stiff, damp, gravity, cstiff, cdamp))
    to_u = TWO_PI / fine_dt
    scale = jnp.where(lane_of < DOF, TWO_PI, to_u)
    shrink = jnp.where(lane_of < DOF, 1.0 / TWO_PI, 1.0 / to_u)

    for ref in (tq, spring, fric, grav, cspring, cfric, ybuf, ubuf, ly, lu, ctmp, stage, wgt, cmap, qmap, bmap):
        clear(ref)
    for h in range(tiles):
        inits[h * LANES : (h + 1) * LANES, :] = (
            pad_rows(init[:, h * LANES : (h + 1) * LANES], LANES).T * shrink
        )
    start_state = inits[pl.ds(pl.multiple_of(z * epd, epd), epd), :]
    deep = DEPTH + epd
    first_start = jnp.where(block_t == 0, start_state, 0.0)
    rank = lax.broadcasted_iota(jnp.int32, (deep, DOF), 0)
    col = lax.broadcasted_iota(jnp.int32, (deep, DOF), 1)
    for n in range(slices):
        cut = pl.ds(plan.where[n], DOF)
        ly[:, cut] = jnp.where(rank == col, 1.0, 0.0)
        lu[:, cut] = jnp.where(rank == col + DOF, 1.0, 0.0)
        grav[:, cut] = jnp.broadcast_to(gravity, (1, DOF))
    ly[DEPTH:, 0:DOF] = first_start[:, 0:DOF]
    lu[DEPTH:, 0:DOF] = first_start[:, DOF : 2 * DOF]

    square_row = lax.broadcasted_iota(jnp.int32, (40, LANES), 0)
    for i in range(nz):
        @pl.when(other_source(i))
        def _(i=i):
            in_arrival(i).wait_recv()
            row_arrival(i, 0).wait_recv()

        @pl.loop(1, ny)
        def _(r, i=i):
            row_arrival(i, r).wait_recv()

        folded = rx[i, 40:ROWS_IN, :]
        square = jnp.concatenate(
            [folded, pltpu.roll(folded, LANES - FOLD, 1), pltpu.roll(folded[0:8], LANES - 2 * FOLD, 1)], axis=0
        )
        shifted = pltpu.roll(square, LANES - 1, 1)
        turned = jnp.concatenate([rx[i, 0:40, :], square, shifted, jnp.zeros((8, LANES), F32)], axis=0).T
        matrices = (
            jnp.where(lane_of <= square_row, square, pltpu.roll(turned[0:40], LANES - 40, 1)),
            jnp.where(lane_of >= square_row, shifted, pltpu.roll(turned[0:40], LANES - 80, 1)),
        )
        means = jnp.sum(rows[i], axis=0) * (1.0 / (env_local * ny))
        for a in range(HS):
            n = HS * i + a
            cut = pl.ds(plan.where[n], DOF)
            g, pos = divmod(n, LANES // DOF)
            stage[g, pl.ds(pos * DOF, DOF), pl.ds(pos * DOF, DOF)] = (
                fine_dt * fine_dt / TWO_PI
            ) * matrices[a][0:DOF, 0:DOF]
            for j in range(HS):
                k = a * HS + j
                piece = turned[k * epd : (k + 1) * epd, :]
                hit = piece[:, DOF : DOF + 1]
                mean = means[:, k * epd : k * epd + 1]
                tq[j, :, cut] = piece[:, 0:DOF]
                spring[j, :, cut] = TWO_PI * (stiff + hit * cstiff)
                fric[j, :, cut] = to_u * (damp + hit * cdamp)
                cspring[j, :, cut] = TWO_PI * (stiff + gravity + mean * cstiff)
                cfric[j, :, cut] = to_u * (damp + mean * cdamp)

    for g, (base, first, count) in enumerate(plan.groups):
        put(wgt, g, stage[g])

    def product(force, g):
        return through(force, wgt[g])

    for g, (base, first, count) in enumerate(plan.groups):
        cut = pl.ds(base, LANES)
        y, u = ly[:, cut], lu[:, cut]
        for j in range(HS):
            push = jnp.concatenate([jnp.zeros((DEPTH, LANES), F32), tq[j, :, cut]], axis=0)
            force = push - cspring[j, :, cut] * y - cfric[j, :, cut] * u
            u = u + ratio * product(force, g)
            y = y + ratio * u
        ly[:, cut] = y
        lu[:, cut] = u
    levels = slices.bit_length() - 1
    stacks = []
    for n in range(slices):
        cut = pl.ds(plan.where[n], DOF)
        ctmp[:, 0:DOF] = ly[:, cut]
        ctmp[:, DOF : 2 * DOF] = lu[:, cut]
        stacks.append(ctmp[...])

    def right_half(level):
        step = 1 << level
        place = 0
        for m in range(0, slices, 2 * step):
            for i in range(step):
                yield place, m + step - 1, m + step + i
                place += 1

    keep_offsets = lax.broadcasted_iota(jnp.int32, (deep, LANES), 0) >= DEPTH
    for level in range(levels):
        for place, left, n in right_half(level):
            put(cmap, level * (slices // 2) + place, stacks[n][0:DEPTH])
        for place, left, n in right_half(level):
            moved = through(stacks[left], cmap[level * (slices // 2) + place])
            stacks[n] = moved + jnp.where(keep_offsets, stacks[n], 0.0)
    for n in range(slices):
        put(qmap, n, stacks[n][0:DEPTH])
    ends = [stack[DEPTH:] for stack in stacks]

    def sweep(ends):
        for level in range(levels):
            for place, left, n in right_half(level):
                ends[n] = ends[n] + through(ends[left], cmap[level * (slices // 2) + place])

    def first_copy(d):
        return pltpu.make_async_remote_copy(
            src_ref=btx,
            dst_ref=brx.at[block_t],
            send_sem=bsend.at[d],
            recv_sem=brecv.at[d],
            device_id={"tm": block_index(block_t + d), "env": me_e},
            device_id_type=MESH,
        )

    def first_arrival(d):
        return pltpu.make_async_remote_copy(
            src_ref=btx,
            dst_ref=brx.at[block_t - d],
            send_sem=bsend.at[d],
            recv_sem=brecv.at[d],
            device_id={"tm": block_index(block_t - d), "env": me_e},
            device_id_type=MESH,
        )

    def sweep_copy(k, d):
        return pltpu.make_async_remote_copy(
            src_ref=stx.at[k],
            dst_ref=srx.at[k, block_t],
            send_sem=ssend.at[k, d],
            recv_sem=srecv.at[k, d],
            device_id={"tm": block_index(block_t + d), "env": me_e},
            device_id_type=MESH,
        )

    def sweep_arrival(k, d):
        return pltpu.make_async_remote_copy(
            src_ref=stx.at[k],
            dst_ref=srx.at[k, block_t - d],
            send_sem=ssend.at[k, d],
            recv_sem=srecv.at[k, d],
            device_id={"tm": block_index(block_t - d), "env": me_e},
            device_id_type=MESH,
        )

    def send_blocks(copy):
        @pl.loop(1, blocks)
        def _(d):
            @pl.when(block_t + d < blocks)
            def _():
                copy(d).start()

    def await_blocks(arrival):
        @pl.loop(1, blocks)
        def _(d):
            @pl.when(block_t - d >= 0)
            def _():
                arrival(d).wait_recv()

    def drain_blocks(copy):
        @pl.loop(1, blocks)
        def _(d):
            @pl.when(block_t + d < blocks)
            def _():
                copy(d).wait_send()

    btx[...] = stacks[slices - 1][0:DEPTH]
    stx[0] = ends[slices - 1]
    for n in range(slices):
        ends_buf[n] = ends[n]
    send_blocks(first_copy)
    send_blocks(functools.partial(sweep_copy, 0))
    await_blocks(first_arrival)
    eye = jnp.where(
        lax.broadcasted_iota(jnp.int32, (DEPTH, LANES), 0) == lane_of, 1.0, 0.0
    )
    maps = {t: jnp.where(t < block_t, brx[t], eye) for t in range(1, blocks - 1)}
    pieces = {(t, t): maps[t] for t in maps}

    def join(a, b, c):
        if (a, c) not in pieces:
            slot = weights.setdefault((b, c), len(weights))
            if slot == len(weights) - 1:
                put(bmap, slot, pieces[b, c])
            pieces[a, c] = through(pieces[a, b - 1], bmap[slot])

    weights = {}
    top = blocks - 2
    span = 1
    while span < blocks:
        for last in range(top, 0, -2 * span):
            mid = last - span + 1
            if mid <= 1:
                continue
            for first in range(max(1, mid - span), mid):
                join(first, mid, last)
        span *= 2
    for t in range(blocks - 2):
        if (t + 1, top) not in weights:
            weights[t + 1, top] = len(weights)
            put(bmap, weights[t + 1, top], pieces[t + 1, top])

    def enter(k):
        total = jnp.where(blocks - 2 < block_t, srx[k, blocks - 2], 0.0)
        for t in range(blocks - 2):
            total = total + through(jnp.where(t < block_t, srx[k, t], 0.0), bmap[weights[t + 1, top]])
        return total

    await_blocks(functools.partial(sweep_arrival, 0))
    entry = enter(0)
    xs[0] = jnp.where(block_t == 0, start_state, entry)
    for n in range(slices):
        xs[n + 1] = ends_buf[n] + through(entry, qmap[n])

    def iteration(k, corrections):
        for n in range(slices):
            cut = pl.ds(plan.where[n], DOF)
            ybuf[:, cut] = xs[n, :, 0:DOF]
            ubuf[:, cut] = xs[n, :, DOF : 2 * DOF]
        for j in range(HS):

            def substep(counter, carry):
                result = []
                for g, (base, first, count) in enumerate(plan.groups):
                    y, u = carry[g]
                    cut = pl.ds(base, LANES)
                    t = y - jnp.round(y)
                    s = t * t
                    s2 = s * s
                    poly = (SIN[0] + SIN[1] * s) + s2 * ((SIN[2] + SIN[3] * s) + s2 * (SIN[4] + SIN[5] * s))
                    force = (
                        tq[j, :, cut]
                        - spring[j, :, cut] * y
                        - fric[j, :, cut] * u
                        - (grav[:, cut] * t) * poly
                    )
                    u = u + product(force, g)
                    y = y + u
                    result.append((y, u))
                return tuple(result)

            first_state = tuple(
                (ybuf[:, pl.ds(base, LANES)], ubuf[:, pl.ds(base, LANES)])
                for base, first, count in plan.groups
            )
            last = lax.fori_loop(0, SUB, substep, first_state, unroll=UNROLL)
            for g, (base, first, count) in enumerate(plan.groups):
                ybuf[:, pl.ds(base, LANES)] = last[g][0]
                ubuf[:, pl.ds(base, LANES)] = last[g][1]

        zero = jnp.zeros((epd, LANES - 2 * DOF), F32)
        ends = []
        for n in range(slices):
            cut = pl.ds(plan.where[n], DOF)
            ends.append(jnp.concatenate([ybuf[:, cut], ubuf[:, cut], zero], axis=1) - xs[n + 1])
        sweep(ends)
        stx[k + 1] = ends[slices - 1]
        for n in range(slices):
            ends_buf[n] = ends[n]
        send_blocks(functools.partial(sweep_copy, k + 1))
        await_blocks(functools.partial(sweep_arrival, k + 1))
        entry = enter(k + 1)
        xs[0] = xs[0] + entry
        worst = jnp.zeros((epd, 1), F32)
        for n in range(slices):
            change = ends_buf[n] + through(entry, qmap[n])
            real = change * scale
            worst = jnp.maximum(worst, jnp.sum(real * real, axis=1, keepdims=True))
            xs[n + 1] = xs[n + 1] + change
        return jnp.where(lane_of == k, jnp.sqrt(worst), corrections)

    corrections = lax.fori_loop(0, ITERS, iteration, jnp.zeros((epd, LANES), F32))

    turned = pad_rows(corrections, LANES).T
    row = turned[0:1]
    for k in range(1, ITERS):
        row = jnp.where(lane_group == k, pltpu.roll(turned[k : k + 1], k * epd, 1), row)
    ctx[...] = row
    for i in range(nz):
        parts = []
        for a in range(HS):
            real = xs[HS * i + a + 1] * scale
            parts.append(real)
            parts.append(pltpu.roll(real, LANES - DOF, 1))
        otx[i] = jnp.concatenate(parts, axis=0).T[0:ROWS_OUT, :]

    def out_copy(i):
        return pltpu.make_async_remote_copy(
            src_ref=otx.at[i],
            dst_ref=orx.at[z],
            send_sem=osend.at[i],
            recv_sem=orecv.at[z],
            device_id={"tm": source_index(i), "env": me_e},
            device_id_type=MESH,
        )

    def out_arrival(k):
        return pltpu.make_async_remote_copy(
            src_ref=otx.at[0],
            dst_ref=orx.at[lax.rem(z + k, nz)],
            send_sem=osend.at[0],
            recv_sem=orecv.at[lax.rem(z + k, nz)],
            device_id={"tm": dest_index(k), "env": me_e},
            device_id_type=MESH,
        )

    def corr_copy(k):
        return pltpu.make_async_remote_copy(
            src_ref=ctx,
            dst_ref=crx.at[block_t, z],
            send_sem=csend.at[k],
            recv_sem=crecv.at[k],
            device_id={"tm": lax.rem(me_t + k, tm), "env": me_e},
            device_id_type=MESH,
        )

    @pl.loop(0, nz)
    def _(i):
        @pl.when(other_source(i))
        def _():
            out_copy(i).start()

    @pl.loop(1, tm)
    def _(k):
        corr_copy(k).start()

    crx[block_t, z] = ctx[...]

    @pl.when(own_here)
    def _():
        orx[z] = otx[my_source]

    @pl.loop(0, nz)
    def _(k):
        @pl.when(other(k))
        def _():
            out_arrival(k).wait_recv()

    for h in range(tiles):
        for k in range(2 * HS):
            a, half_state = divmod(k, 2)
            tile = None
            for q in range(per_tile):
                r = (q - k) % per_tile
                v = orx[h * per_tile + q]
                v = v if r == 0 else pltpu.roll(v, r * epd, 1)
                tile = v if tile is None else jnp.where(lane_group == q, v, tile)
            out[half_state * DOF : half_state * DOF + DOF, a, h * LANES : (h + 1) * LANES] = tile[0:DOF]

    @pl.loop(1, tm)
    def _(k):
        corr_copy(k).wait()

    worst = crx[0]
    for t in range(1, blocks):
        worst = jnp.maximum(worst, crx[t])
    for h in range(tiles):
        for k in range(ITERS):
            tile = None
            for q in range(per_tile):
                r = (q - k) % per_tile
                v = worst[h * per_tile + q]
                v = v if r == 0 else pltpu.roll(v, r * epd, 1)
                tile = v if tile is None else jnp.where(lane_group == q, v, tile)
            corr_out[k : k + 1, h * LANES : (h + 1) * LANES] = tile

    @pl.loop(0, nz)
    def _(k):
        @pl.when(other(k))
        def _():
            in_copy(k).wait_send()
            row_copy(k, 0).wait_send()

        @pl.loop(1, ny)
        def _(r):
            row_copy(k, r).wait_send()

        @pl.when(other_source(k))
        def _():
            out_copy(k).wait_send()

    drain_blocks(first_copy)
    for k in range(ITERS + 1):
        drain_blocks(functools.partial(sweep_copy, k))


def body(tm, env, init_state, torque, contact, mass_inverse, stiffness, damping, gravity,
         contact_stiffness, contact_damping):
    nz = NZ
    env_local = init_state.shape[1]
    epd = env_local // nz
    slices = HS * nz
    blocks = tm // (nz * CORES) * CORES
    plan = Plan(slices)
    groups = len(plan.groups)
    lanes = plan.lanes
    vm = pltpu.VMEM
    dma = pltpu.SemaphoreType.DMA
    vmem = pl.BlockSpec(memory_space=pltpu.VMEM)
    both = vm((HS, epd, lanes), F32)
    thin = vm((HS, 1, lanes), F32)
    deep = DEPTH + epd
    levels = slices.bit_length() - 1
    prm = [p.reshape(1, DOF) for p in (stiffness, damping, gravity, contact_stiffness, contact_damping)]
    states, corrections = pl.pallas_call(
        functools.partial(kernel, tm, env),
        out_shape=(
            jax.ShapeDtypeStruct((STATE, HS, env_local), F32),
            jax.ShapeDtypeStruct((ITERS, env_local), F32),
        ),
        in_specs=[pl.BlockSpec(memory_space=pl.ANY)] * 9,
        out_specs=(vmem, vmem),
        scratch_shapes=[
            vm(init_state.shape, F32), vm((DOF, 2 * HS, env_local), F32), vm(contact.shape, jnp.int32),
            vm((DOF, HS, DOF), F32), *[vm((1, DOF), F32)] * 5,
            vm((nz, ROWS_IN, LANES), F32), vm((nz, ROWS_IN, LANES), F32),
            vm((1, LANES), F32), vm((nz, env, 1, LANES), F32),
            vm((2 * HS, 40, env_local), F32), vm((env_local, LANES), F32),
            both, both, both, vm((1, lanes), F32), thin, thin,
            vm((groups, WIDE, WIDE), BF16), vm((groups, LANES, LANES), F32), vm((LANES, LANES), F32),
            vm((epd, lanes), F32), vm((epd, lanes), F32),
            vm((deep, lanes), F32), vm((deep, lanes), F32),
            vm((levels * slices // 2, WIDE, WIDE), BF16),
            vm((slices, WIDE, WIDE), BF16), vm((2 * blocks, WIDE, WIDE), BF16),
            vm((deep, LANES), F32),
            vm((slices + 1, epd, LANES), F32), vm((slices, epd, LANES), F32),
            vm((DEPTH, LANES), F32), vm((blocks, DEPTH, LANES), F32),
            vm((ITERS + 1, epd, LANES), F32), vm((ITERS + 1, blocks, epd, LANES), F32),
            vm((nz, ROWS_OUT, LANES), F32), vm((nz, ROWS_OUT, LANES), F32),
            vm((1, LANES), F32), vm((blocks, nz, 1, LANES), F32),
            dma((9,)), dma((nz,)), dma((nz,)), dma((nz, env)), dma((nz, env)),
            dma((blocks,)), dma((blocks,)), dma((ITERS + 1, blocks)), dma((ITERS + 1, blocks)),
            dma((nz,)), dma((nz,)), dma((tm,)), dma((tm,)),
        ],
        compiler_params=pltpu.CompilerParams(collective_id=0, has_side_effects=True),
        name="parareal",
    )(
        init_state, torque.transpose(1, 0, 2), contact, mass_inverse.transpose(1, 0, 2), *prm
    )
    return states.transpose(1, 0, 2), corrections


def solution(mesh):
    placed = (
        P(None, "env"),
        P("tm", None, "env"),
        P("tm", "env"),
        P("tm", None, None),
        P(),
        P(),
        P(),
        P(),
        P(),
    )
    return jax.shard_map(
        functools.partial(body, mesh.shape["tm"], mesh.shape["env"]),
        mesh=mesh,
        in_specs=placed,
        out_specs=(P("tm", None, "env"), P(None, "env")),
        check_vma=False,
    )
```

```python
import functools
import math

import jax
import jax.numpy as jnp
from jax import lax
from jax.experimental import pallas as pl
from jax.experimental.pallas import tpu as pltpu
from jax.sharding import PartitionSpec as P

DOF = 35
STATE = 70
HS = 2
SUB = 32
ITERS = 3
LANES = 128
WIDE = 256
NZ = 8
CORES = 2
UNROLL = 32

step_length = 0.05
fine_dt = step_length / SUB
TWO_PI = 2.0 * math.pi
MESH = pl.DeviceIdType.MESH
F32 = jnp.float32
BF16 = jnp.bfloat16

SIN = (
    6.283182818551188, -41.341421398631915, 81.59618387021051,
    -76.58010048603072, 41.205394649903326, -12.271261959178284,
)

ROWS_IN = 40
ROWS_MAT = 16
FOLD = 36
ROWS_OUT = 40
DEPTH = 72


def split(value):
    high = value.astype(BF16)
    return high, (value - high.astype(F32)).astype(BF16)


def dot(left, right):
    return jnp.dot(left, right, preferred_element_type=F32)


def through(state, weight):
    high, low = split(state)
    both = dot(jnp.concatenate([high, low], axis=1), weight)
    return both[:, :LANES] + both[:, LANES:]


def clear(ref):
    ref[...] = jnp.zeros(ref.shape, ref.dtype)


def put(ref, n, value):
    high, low = split(value)
    rows = value.shape[0]
    ref[n, 0:rows, 0:LANES] = high
    ref[n, LANES : LANES + rows, 0:LANES] = high
    ref[n, 0:rows, LANES:] = low


def pad_rows(value, rows):
    return jnp.concatenate([value, jnp.zeros((rows - value.shape[0], value.shape[1]), F32)], axis=0)


class Plan:
    def __init__(self, sources):
        self.per = LANES // DOF
        self.groups = []
        self.slot = {}
        for first in range(0, sources, self.per):
            members = range(first, min(first + self.per, sources))
            for a in range(HS):
                for pos, i in enumerate(members):
                    self.slot[HS * i + a] = (len(self.groups), pos)
                self.groups.append((len(self.groups) * LANES, members, a))
        self.where = [self.slot[n][0] * LANES + self.slot[n][1] * DOF for n in range(HS * sources)]
        self.lanes = len(self.groups) * LANES


def kernel(
    tm, ny,
    init_hbm, torque_hbm, contact_hbm, minv_hbm, stiff_hbm, damp_hbm, gravity_hbm, cstiff_hbm, cdamp_hbm,
    out, corr_out,
    init, torque, contact, minv, stiff, damp, gravity, cstiff, cdamp,
    tx, rx, mtx, mrx, rowtx, rows, raw, inits,
    tstage, gains, tq, spring, fric, grav, cspring, cfric, wgt, stage, wtmp, ybuf, ubuf, ly, lu,
    cmap, qmap, bmap, ctmp, xs, ends_buf,
    btx, brx, stx, srx, otx, orx, ctx, crx,
    lsem, tsend, trecv, msend, mrecv, rsend, rrecv, bsend, brecv, ssend, srecv, osend, orecv, csend, crecv,
):
    pairs = (
        (torque_hbm, torque), (contact_hbm, contact), (minv_hbm, minv), (init_hbm, init), (stiff_hbm, stiff),
        (damp_hbm, damp), (gravity_hbm, gravity), (cstiff_hbm, cstiff), (cdamp_hbm, cdamp),
    )
    local = [pltpu.make_async_copy(src, dst, lsem.at[i]) for i, (src, dst) in enumerate(pairs)]
    for copy in local:
        copy.start()
    nz = NZ
    half = nz // 2
    line = nz * CORES
    blocks = tm // line * CORES
    env_local = init.shape[1]
    epd = env_local // nz
    slices = HS * nz
    per_tile = LANES // epd
    tiles = env_local // LANES
    plan = Plan(nz)
    me_t = lax.axis_index("tm")
    me_e = lax.axis_index("env")
    x = me_t // line
    z = lax.rem(me_t // CORES, nz)
    c = lax.rem(me_t, CORES)
    block_t = x * CORES + c
    dest_core = z // half
    my_source = lax.rem(z, half) * CORES + c
    own_here = dest_core == c
    barrier = pltpu.get_barrier_semaphore()

    def source_index(i):
        return x * line + (c * half + i // CORES) * CORES + lax.rem(i, CORES)

    def dest_index(k):
        return x * line + lax.rem(z + k, nz) * CORES + dest_core

    def block_index(t):
        return t // CORES * line + z * CORES + lax.rem(t, CORES)

    @pl.loop(1, tm, unroll=True)
    def _(k):
        pl.semaphore_signal(
            barrier, inc=1, device_id={"tm": lax.rem(me_t + k, tm), "env": me_e}, device_id_type=MESH
        )

    @pl.loop(1, ny)
    def _(r):
        @pl.loop(0, nz)
        def _(i):
            pl.semaphore_signal(
                barrier, inc=1,
                device_id={"tm": source_index(i), "env": lax.rem(me_e + r, ny)},
                device_id_type=MESH,
            )

    for copy in local:
        copy.wait()
    lane_of = lax.broadcasted_iota(jnp.int32, (1, LANES), 1)
    lane_group = lane_of // epd

    raw[...] = jnp.zeros(raw.shape, F32)
    hits = contact[...].astype(F32)
    for k in range(2 * HS):
        raw[k, 0:DOF, :] = torque[:, k, :]
        raw[k, DOF : DOF + 1, :] = hits[k : k + 1, :]
    wtmp[...] = jnp.zeros(wtmp.shape, F32)
    wtmp[0:DOF, 0:DOF] = minv[:, 0, :]
    wtmp[40 : 40 + DOF, 0:DOF] = minv[:, 1, :]
    row_of = lax.broadcasted_iota(jnp.int32, (40, LANES), 0)
    lower = lane_of <= row_of
    packed = jnp.where(lower, wtmp[0:40, :], pltpu.roll(wtmp[40:80, :], 1, 1))
    last = jnp.concatenate([packed[32:40], jnp.zeros((8, LANES), F32)], axis=0)
    mtx[...] = packed[0:16] + pltpu.roll(packed[16:32], FOLD, 1) + pltpu.roll(last, 2 * FOLD, 1)
    for h in range(tiles):
        rolled = {}
        for k in range(2 * HS):
            v = raw[k, :, h * LANES : (h + 1) * LANES]
            for r in range(per_tile):
                rolled[k, r] = v if r == 0 else pltpu.roll(v, r * epd, 1)
        for q in range(per_tile):
            acc = rolled[0, (0 - q) % per_tile]
            for k in range(1, 2 * HS):
                acc = jnp.where(lane_group == k, rolled[k, (k - q) % per_tile], acc)
            tx[h * per_tile + q] = acc
    totals = jnp.sum(hits, axis=1, keepdims=True)
    row = jnp.broadcast_to(totals[0:1], (1, LANES))
    for k in range(1, 2 * HS):
        row = jnp.where(lane_group == k, jnp.broadcast_to(totals[k : k + 1], (1, LANES)), row)
    rowtx[...] = row

    pl.semaphore_wait(barrier, tm - 1 + (ny - 1) * nz)

    def in_copy(k):
        return pltpu.make_async_remote_copy(
            src_ref=tx.at[lax.rem(z + k, nz)],
            dst_ref=rx.at[my_source],
            send_sem=tsend.at[k],
            recv_sem=trecv.at[my_source],
            device_id={"tm": dest_index(k), "env": me_e},
            device_id_type=MESH,
        )

    def in_arrival(i):
        return pltpu.make_async_remote_copy(
            src_ref=tx.at[0],
            dst_ref=rx.at[i],
            send_sem=tsend.at[0],
            recv_sem=trecv.at[i],
            device_id={"tm": dest_index(0), "env": me_e},
            device_id_type=MESH,
        )

    def mat_copy(k):
        return pltpu.make_async_remote_copy(
            src_ref=mtx,
            dst_ref=mrx.at[my_source],
            send_sem=msend.at[k],
            recv_sem=mrecv.at[my_source],
            device_id={"tm": dest_index(k), "env": me_e},
            device_id_type=MESH,
        )

    def mat_arrival(i):
        return pltpu.make_async_remote_copy(
            src_ref=mtx,
            dst_ref=mrx.at[i],
            send_sem=msend.at[0],
            recv_sem=mrecv.at[i],
            device_id={"tm": dest_index(0), "env": me_e},
            device_id_type=MESH,
        )

    def row_copy(k, r):
        return pltpu.make_async_remote_copy(
            src_ref=rowtx,
            dst_ref=rows.at[my_source, me_e],
            send_sem=rsend.at[k, r],
            recv_sem=rrecv.at[my_source, r],
            device_id={"tm": dest_index(k), "env": lax.rem(me_e + r, ny)},
            device_id_type=MESH,
        )

    def row_arrival(i, r):
        return pltpu.make_async_remote_copy(
            src_ref=rowtx,
            dst_ref=rows.at[i, lax.rem(me_e - r + ny, ny)],
            send_sem=rsend.at[0, r],
            recv_sem=rrecv.at[i, r],
            device_id={"tm": dest_index(0), "env": lax.rem(me_e + r, ny)},
            device_id_type=MESH,
        )

    def other(k):
        return jnp.logical_not(jnp.logical_and(own_here, k == 0))

    def other_source(i):
        return jnp.logical_not(jnp.logical_and(own_here, i == my_source))

    @pl.loop(0, nz)
    def _(k):
        @pl.when(other(k))
        def _():
            row_copy(k, 0).start()

        @pl.loop(1, ny)
        def _(r):
            row_copy(k, r).start()

    far_first = sorted(range(nz), key=lambda k: -min(k, nz - k))
    for make in (mat_copy, in_copy):
        for k in far_first:
            @pl.when(other(k))
            def _(k=k, make=make):
                make(k).start()

    @pl.when(own_here)
    def _():
        rx[my_source] = tx[z]
        mrx[my_source] = mtx[...]
        rows[my_source, me_e] = rowtx[...]

    ratio = float(SUB)
    stiff, damp, gravity, cstiff, cdamp = (r[...] for r in (stiff, damp, gravity, cstiff, cdamp))
    to_u = TWO_PI / fine_dt
    scale = jnp.where(lane_of < DOF, TWO_PI, to_u)
    shrink = jnp.where(lane_of < DOF, 1.0 / TWO_PI, 1.0 / to_u)

    for ref in (tstage, gains, tq, spring, fric, grav, cspring, cfric, ybuf, ubuf, ly, lu, ctmp, stage, wgt, cmap, qmap, bmap):
        clear(ref)
    for h in range(tiles):
        inits[h * LANES : (h + 1) * LANES, :] = (
            pad_rows(init[:, h * LANES : (h + 1) * LANES], LANES).T * shrink
        )
    start_state = inits[pl.ds(pl.multiple_of(z * epd, epd), epd), :]
    first_start = jnp.where(block_t == 0, start_state, 0.0)
    rank = lax.broadcasted_iota(jnp.int32, (DEPTH, DOF), 0)
    col = lax.broadcasted_iota(jnp.int32, (DEPTH, DOF), 1)
    for n in range(slices):
        cut = pl.ds(plan.where[n], DOF)
        ly[:, cut] = jnp.where(rank == col, 1.0, 0.0)
        lu[:, cut] = jnp.where(rank == col + DOF, 1.0, 0.0)
        grav[:, cut] = gravity
        gains[0, :, cut] = TWO_PI * stiff
        gains[1, :, cut] = TWO_PI * cstiff
        gains[2, :, cut] = to_u * damp
        gains[3, :, cut] = to_u * cdamp
    ybuf[:, 0:DOF] = first_start[:, 0:DOF]
    ubuf[:, 0:DOF] = first_start[:, DOF : 2 * DOF]

    square_row = lax.broadcasted_iota(jnp.int32, (40, LANES), 0)
    for i in range(nz):
        @pl.when(other_source(i))
        def _(i=i):
            mat_arrival(i).wait_recv()
            row_arrival(i, 0).wait_recv()

        @pl.loop(1, ny)
        def _(r, i=i):
            row_arrival(i, r).wait_recv()

        folded = mrx[i]
        square = jnp.concatenate(
            [folded, pltpu.roll(folded, LANES - FOLD, 1), pltpu.roll(folded[0:8], LANES - 2 * FOLD, 1)], axis=0
        )
        shifted = pltpu.roll(square, LANES - 1, 1)
        turned = pad_rows(jnp.concatenate([square, shifted], axis=0), LANES).T
        matrices = (
            jnp.where(lane_of <= square_row, square, turned[0:40]),
            jnp.where(lane_of >= square_row, shifted, pltpu.roll(turned[0:40], LANES - 40, 1)),
        )
        means = jnp.sum(rows[i], axis=0) * (1.0 / (env_local * ny))
        for a in range(HS):
            n = HS * i + a
            cut = pl.ds(plan.where[n], DOF)
            g, pos = plan.slot[n]
            stage[g, pl.ds(pos * DOF, DOF), pl.ds(pos * DOF, DOF)] = (
                fine_dt * fine_dt / TWO_PI
            ) * matrices[a][0:DOF, 0:DOF]
            for j in range(HS):
                k = a * HS + j
                mean = means[:, k * epd : k * epd + 1]
                cspring[j, :, cut] = TWO_PI * (stiff + gravity + mean * cstiff)
                cfric[j, :, cut] = to_u * (damp + mean * cdamp)

    for g, (base, members, a) in enumerate(plan.groups):
        put(wgt, g, stage[g])

    def product(force, g):
        return through(force, wgt[g])

    for g, (base, members, a) in enumerate(plan.groups):
        cut = pl.ds(base, LANES)
        y, u = ly[:, cut], lu[:, cut]
        for j in range(HS):
            force = -cspring[j, :, cut] * y - cfric[j, :, cut] * u
            u = u + ratio * product(force, g)
            y = y + ratio * u
        ly[:, cut] = y
        lu[:, cut] = u
    levels = slices.bit_length() - 1
    stacks = []
    for n in range(slices):
        cut = pl.ds(plan.where[n], DOF)
        ctmp[:, 0:DOF] = ly[:, cut]
        ctmp[:, DOF : 2 * DOF] = lu[:, cut]
        stacks.append(ctmp[...])

    def right_half(level):
        step = 1 << level
        place = 0
        for m in range(0, slices, 2 * step):
            for i in range(step):
                yield level * (slices // 2) + place, m + step - 1, m + step + i
                place += 1

    for level in range(levels):
        for place, left, n in right_half(level):
            put(cmap, place, stacks[n])
        for place, left, n in right_half(level):
            stacks[n] = through(stacks[left], cmap[place])
    btx[...] = stacks[slices - 1]
    for n in range(slices):
        put(qmap, n, stacks[n])

    def sweep(ends):
        for level in range(levels):
            for place, left, n in right_half(level):
                ends[n] = ends[n] + through(ends[left], cmap[place])

    def first_copy(d):
        return pltpu.make_async_remote_copy(
            src_ref=btx,
            dst_ref=brx.at[block_t],
            send_sem=bsend.at[d],
            recv_sem=brecv.at[d],
            device_id={"tm": block_index(block_t + d), "env": me_e},
            device_id_type=MESH,
        )

    def first_arrival(d):
        return pltpu.make_async_remote_copy(
            src_ref=btx,
            dst_ref=brx.at[block_t - d],
            send_sem=bsend.at[d],
            recv_sem=brecv.at[d],
            device_id={"tm": block_index(block_t - d), "env": me_e},
            device_id_type=MESH,
        )

    def sweep_copy(k, d):
        return pltpu.make_async_remote_copy(
            src_ref=stx.at[k],
            dst_ref=srx.at[k, block_t],
            send_sem=ssend.at[k, d],
            recv_sem=srecv.at[k, d],
            device_id={"tm": block_index(block_t + d), "env": me_e},
            device_id_type=MESH,
        )

    def sweep_arrival(k, d):
        return pltpu.make_async_remote_copy(
            src_ref=stx.at[k],
            dst_ref=srx.at[k, block_t - d],
            send_sem=ssend.at[k, d],
            recv_sem=srecv.at[k, d],
            device_id={"tm": block_index(block_t - d), "env": me_e},
            device_id_type=MESH,
        )

    def send_blocks(copy):
        @pl.loop(1, blocks)
        def _(d):
            @pl.when(block_t + d < blocks)
            def _():
                copy(d).start()

    def await_blocks(arrival):
        @pl.loop(1, blocks)
        def _(d):
            @pl.when(block_t - d >= 0)
            def _():
                arrival(d).wait_recv()

    def drain_blocks(copy):
        @pl.loop(1, blocks)
        def _(d):
            @pl.when(block_t + d < blocks)
            def _():
                copy(d).wait_send()

    @pl.when(block_t > 0)
    def _():
        send_blocks(first_copy)

    mark = plan.per * DOF
    for part in range(0, nz, plan.per):
        for pos, i in enumerate(range(part, min(part + plan.per, nz))):
            @pl.when(other_source(i))
            def _(i=i):
                in_arrival(i).wait_recv()

            tstage[part // plan.per, pos * DOF : (pos + 1) * DOF, :] = rx[i, 0:DOF, :]
            tstage[part // plan.per, mark + pos : mark + pos + 1, :] = rx[i, DOF : DOF + 1, :]
        turned = tstage[part // plan.per].T
        for a in range(HS):
            base = (part // plan.per * HS + a) * LANES
            cut = pl.ds(base, LANES)
            for j in range(HS):
                k = a * HS + j
                piece = turned[k * epd : (k + 1) * epd, :]
                hit = piece[:, mark : mark + 1]
                for pos in range(1, plan.per):
                    hit = jnp.where(lane_of >= pos * DOF, piece[:, mark + pos : mark + pos + 1], hit)
                tq[j, :, cut] = jnp.where(lane_of < mark, piece, 0.0)
                spring[j, :, cut] = gains[0, :, cut] + hit * gains[1, :, cut]
                fric[j, :, cut] = gains[2, :, cut] + hit * gains[3, :, cut]

    for g, (base, members, a) in enumerate(plan.groups):
        cut = pl.ds(base, LANES)
        y, u = ybuf[:, cut], ubuf[:, cut]
        for j in range(HS):
            force = tq[j, :, cut] - cspring[j, :, cut] * y - cfric[j, :, cut] * u
            u = u + ratio * product(force, g)
            y = y + ratio * u
        ybuf[:, cut] = y
        ubuf[:, cut] = u

    def packed_state(n):
        cut = pl.ds(plan.where[n], DOF)
        zero = jnp.zeros((epd, LANES - 2 * DOF), F32)
        return jnp.concatenate([ybuf[:, cut], ubuf[:, cut], zero], axis=1)

    ends = [packed_state(n) for n in range(slices)]
    sweep(ends)
    stx[0] = ends[slices - 1]
    for n in range(slices):
        ends_buf[n] = ends[n]
    send_blocks(functools.partial(sweep_copy, 0))
    @pl.loop(1, blocks)
    def _(d):
        @pl.when(block_t - d > 0)
        def _():
            first_arrival(d).wait_recv()

    eye = jnp.where(
        lax.broadcasted_iota(jnp.int32, (DEPTH, LANES), 0) == lane_of, 1.0, 0.0
    )
    maps = {t: jnp.where(t < block_t, brx[t], eye) for t in range(1, blocks - 1)}
    pieces = {(t, t): maps[t] for t in maps}

    def join(a, b, c):
        if (a, c) not in pieces:
            slot = weights.setdefault((b, c), len(weights))
            if slot == len(weights) - 1:
                put(bmap, slot, pieces[b, c])
            pieces[a, c] = through(pieces[a, b - 1], bmap[slot])

    weights = {}
    top = blocks - 2
    span = 1
    while span < blocks:
        for last in range(top, 0, -2 * span):
            mid = last - span + 1
            if mid <= 1:
                continue
            for first in range(max(1, mid - span), mid):
                join(first, mid, last)
        span *= 2
    for t in range(blocks - 2):
        if (t + 1, top) not in weights:
            weights[t + 1, top] = len(weights)
            put(bmap, weights[t + 1, top], pieces[t + 1, top])

    def enter(k):
        total = jnp.where(blocks - 2 < block_t, srx[k, blocks - 2], 0.0)
        for t in range(blocks - 2):
            total = total + through(jnp.where(t < block_t, srx[k, t], 0.0), bmap[weights[t + 1, top]])
        return total

    await_blocks(functools.partial(sweep_arrival, 0))
    entry = enter(0)
    xs[0] = jnp.where(block_t == 0, start_state, entry)
    for n in range(slices):
        xs[n + 1] = ends_buf[n] + through(entry, qmap[n])

    def iteration(k, corrections):
        for n in range(slices):
            cut = pl.ds(plan.where[n], DOF)
            ybuf[:, cut] = xs[n, :, 0:DOF]
            ubuf[:, cut] = xs[n, :, DOF : 2 * DOF]
        for j in range(HS):

            def substep(counter, carry):
                result = []
                for g, (base, members, a) in enumerate(plan.groups):
                    y, u = carry[g]
                    cut = pl.ds(base, LANES)
                    t = y - jnp.round(y)
                    s = t * t
                    s2 = s * s
                    poly = (SIN[0] + SIN[1] * s) + s2 * ((SIN[2] + SIN[3] * s) + s2 * (SIN[4] + SIN[5] * s))
                    force = (
                        tq[j, :, cut]
                        - spring[j, :, cut] * y
                        - fric[j, :, cut] * u
                        - (grav[:, cut] * t) * poly
                    )
                    u = u + product(force, g)
                    y = y + u
                    result.append((y, u))
                return tuple(result)

            first_state = tuple(
                (ybuf[:, pl.ds(base, LANES)], ubuf[:, pl.ds(base, LANES)])
                for base, members, a in plan.groups
            )
            last = lax.fori_loop(0, SUB, substep, first_state, unroll=UNROLL)
            for g, (base, members, a) in enumerate(plan.groups):
                ybuf[:, pl.ds(base, LANES)] = last[g][0]
                ubuf[:, pl.ds(base, LANES)] = last[g][1]

        ends = [packed_state(n) - xs[n + 1] for n in range(slices)]
        sweep(ends)
        stx[k + 1] = ends[slices - 1]
        for n in range(slices):
            ends_buf[n] = ends[n]
        send_blocks(functools.partial(sweep_copy, k + 1))
        await_blocks(functools.partial(sweep_arrival, k + 1))
        entry = enter(k + 1)
        xs[0] = xs[0] + entry
        worst = jnp.zeros((epd, 1), F32)
        for n in range(slices):
            change = ends_buf[n] + through(entry, qmap[n])
            real = change * scale
            worst = jnp.maximum(worst, jnp.sum(real * real, axis=1, keepdims=True))
            xs[n + 1] = xs[n + 1] + change
        return jnp.where(lane_of == k, jnp.sqrt(worst), corrections)

    corrections = lax.fori_loop(0, ITERS, iteration, jnp.zeros((epd, LANES), F32))

    turned = pad_rows(corrections, LANES).T
    row = turned[0:1]
    for k in range(1, ITERS):
        row = jnp.where(lane_group == k, pltpu.roll(turned[k : k + 1], k * epd, 1), row)
    ctx[...] = row
    for i in range(nz):
        parts = []
        for a in range(HS):
            real = xs[HS * i + a + 1] * scale
            parts.append(real)
            parts.append(pltpu.roll(real, LANES - DOF, 1))
        otx[i] = jnp.concatenate(parts, axis=0).T[0:ROWS_OUT, :]

    def out_copy(i):
        return pltpu.make_async_remote_copy(
            src_ref=otx.at[i],
            dst_ref=orx.at[z],
            send_sem=osend.at[i],
            recv_sem=orecv.at[z],
            device_id={"tm": source_index(i), "env": me_e},
            device_id_type=MESH,
        )

    def out_arrival(k):
        return pltpu.make_async_remote_copy(
            src_ref=otx.at[0],
            dst_ref=orx.at[lax.rem(z + k, nz)],
            send_sem=osend.at[0],
            recv_sem=orecv.at[lax.rem(z + k, nz)],
            device_id={"tm": dest_index(k), "env": me_e},
            device_id_type=MESH,
        )

    def corr_copy(k):
        return pltpu.make_async_remote_copy(
            src_ref=ctx,
            dst_ref=crx.at[block_t, z],
            send_sem=csend.at[k],
            recv_sem=crecv.at[k],
            device_id={"tm": lax.rem(me_t + k, tm), "env": me_e},
            device_id_type=MESH,
        )

    @pl.loop(1, tm, unroll=True)
    def _(k):
        corr_copy(k).start()

    @pl.loop(0, nz)
    def _(i):
        @pl.when(other_source(i))
        def _():
            out_copy(i).start()

    crx[block_t, z] = ctx[...]

    @pl.when(own_here)
    def _():
        orx[z] = otx[my_source]

    @pl.loop(0, nz)
    def _(k):
        @pl.when(other(k))
        def _():
            out_arrival(k).wait_recv()

    for h in range(tiles):
        for k in range(2 * HS):
            a, half_state = divmod(k, 2)
            tile = None
            for q in range(per_tile):
                r = (q - k) % per_tile
                v = orx[h * per_tile + q]
                v = v if r == 0 else pltpu.roll(v, r * epd, 1)
                tile = v if tile is None else jnp.where(lane_group == q, v, tile)
            out[half_state * DOF : half_state * DOF + DOF, a, h * LANES : (h + 1) * LANES] = tile[0:DOF]

    @pl.loop(1, tm, unroll=True)
    def _(k):
        corr_copy(k).wait()

    worst = crx[0]
    for t in range(1, blocks):
        worst = jnp.maximum(worst, crx[t])
    for h in range(tiles):
        for k in range(ITERS):
            tile = None
            for q in range(per_tile):
                r = (q - k) % per_tile
                v = worst[h * per_tile + q]
                v = v if r == 0 else pltpu.roll(v, r * epd, 1)
                tile = v if tile is None else jnp.where(lane_group == q, v, tile)
            corr_out[k : k + 1, h * LANES : (h + 1) * LANES] = tile

    @pl.loop(0, nz)
    def _(k):
        @pl.when(other(k))
        def _():
            in_copy(k).wait_send()
            mat_copy(k).wait_send()
            row_copy(k, 0).wait_send()

        @pl.loop(1, ny)
        def _(r):
            row_copy(k, r).wait_send()

        @pl.when(other_source(k))
        def _():
            out_copy(k).wait_send()

    @pl.when(block_t > 0)
    def _():
        drain_blocks(first_copy)

    for k in range(ITERS + 1):
        drain_blocks(functools.partial(sweep_copy, k))


def body(tm, env, init_state, torque, contact, mass_inverse, stiffness, damping, gravity,
         contact_stiffness, contact_damping):
    nz = NZ
    env_local = init_state.shape[1]
    epd = env_local // nz
    slices = HS * nz
    blocks = tm // (nz * CORES) * CORES
    plan = Plan(nz)
    groups = len(plan.groups)
    lanes = plan.lanes
    vm = pltpu.VMEM
    dma = pltpu.SemaphoreType.DMA
    vmem = pl.BlockSpec(memory_space=pltpu.VMEM)
    both = vm((HS, epd, lanes), F32)
    thin = vm((HS, 1, lanes), F32)
    levels = slices.bit_length() - 1
    prm = [p.reshape(1, DOF) for p in (stiffness, damping, gravity, contact_stiffness, contact_damping)]
    states, corrections = pl.pallas_call(
        functools.partial(kernel, tm, env),
        out_shape=(
            jax.ShapeDtypeStruct((STATE, HS, env_local), F32),
            jax.ShapeDtypeStruct((ITERS, env_local), F32),
        ),
        in_specs=[pl.BlockSpec(memory_space=pl.ANY)] * 9,
        out_specs=(vmem, vmem),
        scratch_shapes=[
            vm(init_state.shape, F32), vm((DOF, 2 * HS, env_local), F32), vm(contact.shape, jnp.int32),
            vm((DOF, HS, DOF), F32), *[vm((1, DOF), F32)] * 5,
            vm((nz, ROWS_IN, LANES), F32), vm((nz, ROWS_IN, LANES), F32),
            vm((ROWS_MAT, LANES), F32), vm((nz, ROWS_MAT, LANES), F32),
            vm((1, LANES), F32), vm((nz, env, 1, LANES), F32),
            vm((2 * HS, 40, env_local), F32), vm((env_local, LANES), F32),
            vm((-(-nz // plan.per), LANES, LANES), F32), vm((4, 1, lanes), F32),
            both, both, both, vm((1, lanes), F32), thin, thin,
            vm((groups, WIDE, WIDE), BF16), vm((groups, LANES, LANES), F32), vm((LANES, LANES), F32),
            vm((epd, lanes), F32), vm((epd, lanes), F32),
            vm((DEPTH, lanes), F32), vm((DEPTH, lanes), F32),
            vm((levels * slices // 2, WIDE, WIDE), BF16),
            vm((slices, WIDE, WIDE), BF16), vm((2 * blocks, WIDE, WIDE), BF16),
            vm((DEPTH, LANES), F32),
            vm((slices + 1, epd, LANES), F32), vm((slices, epd, LANES), F32),
            vm((DEPTH, LANES), F32), vm((blocks, DEPTH, LANES), F32),
            vm((ITERS + 1, epd, LANES), F32), vm((ITERS + 1, blocks, epd, LANES), F32),
            vm((nz, ROWS_OUT, LANES), F32), vm((nz, ROWS_OUT, LANES), F32),
            vm((1, LANES), F32), vm((blocks, nz, 1, LANES), F32),
            dma((9,)), dma((nz,)), dma((nz,)), dma((nz,)), dma((nz,)), dma((nz, env)), dma((nz, env)),
            dma((blocks,)), dma((blocks,)), dma((ITERS + 1, blocks)), dma((ITERS + 1, blocks)),
            dma((nz,)), dma((nz,)), dma((tm,)), dma((tm,)),
        ],
        compiler_params=pltpu.CompilerParams(collective_id=0, has_side_effects=True),
        name="parareal",
    )(
        init_state, torque.transpose(1, 0, 2), contact, mass_inverse.transpose(1, 0, 2), *prm
    )
    return states.transpose(1, 0, 2), corrections


def solution(mesh):
    placed = (
        P(None, "env"),
        P("tm", None, "env"),
        P("tm", "env"),
        P("tm", None, None),
        P(),
        P(),
        P(),
        P(),
        P(),
    )
    return jax.shard_map(
        functools.partial(body, mesh.shape["tm"], mesh.shape["env"]),
        mesh=mesh,
        in_specs=placed,
        out_specs=(P("tm", None, "env"), P(None, "env")),
        check_vma=False,
    )
```

```python
import functools
import math

import jax
import jax.numpy as jnp
from jax import lax
from jax.experimental import pallas as pl
from jax.experimental.pallas import tpu as pltpu
from jax.sharding import PartitionSpec as P

DOF = 35
STATE = 70
HS = 2
SUB = 32
ITERS = 3
LANES = 128
WIDE = 256
NZ = 8
CORES = 2
UNROLL = 32

step_length = 0.05
fine_dt = step_length / SUB
TWO_PI = 2.0 * math.pi
MESH = pl.DeviceIdType.MESH
F32 = jnp.float32
BF16 = jnp.bfloat16

SIN = (
    6.283182818551188, -41.341421398631915, 81.59618387021051,
    -76.58010048603072, 41.205394649903326, -12.271261959178284,
)

ROWS_IN = 40
ROWS_MAT = 16
FOLD = 36
ROWS_OUT = 40
DEPTH = 72
ROWS_MAP = 48


def split(value):
    high = value.astype(BF16)
    return high, (value - high.astype(F32)).astype(BF16)


def dot(left, right):
    return jnp.dot(left, right, preferred_element_type=F32)


def through(state, weight):
    high, low = split(state)
    both = dot(jnp.concatenate([high, low], axis=1), weight)
    return both[:, :LANES] + both[:, LANES:]


def clear(ref):
    ref[...] = jnp.zeros(ref.shape, ref.dtype)


def put(ref, n, value):
    high, low = split(value)
    rows = value.shape[0]
    ref[n, 0:rows, 0:LANES] = high
    ref[n, LANES : LANES + rows, 0:LANES] = high
    ref[n, 0:rows, LANES:] = low


def pad_rows(value, rows):
    return jnp.concatenate([value, jnp.zeros((rows - value.shape[0], value.shape[1]), F32)], axis=0)


def fold_map(value, lane_of):
    value = jnp.where(lane_of < DOF, value, 0.0), jnp.where(lane_of < DOF, pltpu.roll(value, LANES - DOF, 1), 0.0)
    tall = jnp.concatenate(value, axis=0)
    first, second, third = (tall[r : r + ROWS_MAP] for r in range(0, 2 * DEPTH, ROWS_MAP))
    return first + pltpu.roll(second, DOF, 1) + pltpu.roll(third, 2 * DOF, 1)


def unfold_map(value, lane_of):
    tall = jnp.concatenate(
        [value, pltpu.roll(value, LANES - DOF, 1), pltpu.roll(value, LANES - 2 * DOF, 1)], axis=0
    )
    right = jnp.where(lane_of < 2 * DOF, pltpu.roll(tall[DEPTH:], DOF, 1), 0.0)
    return jnp.where(lane_of < DOF, tall[0:DEPTH], right)


class Plan:
    def __init__(self, sources):
        self.per = LANES // DOF
        self.groups = []
        self.slot = {}
        for first in range(0, sources, self.per):
            members = range(first, min(first + self.per, sources))
            for a in range(HS):
                for pos, i in enumerate(members):
                    self.slot[HS * i + a] = (len(self.groups), pos)
                self.groups.append((len(self.groups) * LANES, members, a))
        self.where = [self.slot[n][0] * LANES + self.slot[n][1] * DOF for n in range(HS * sources)]
        self.lanes = len(self.groups) * LANES


def kernel(
    tm, ny,
    init_hbm, torque_hbm, contact_hbm, minv_hbm, stiff_hbm, damp_hbm, gravity_hbm, cstiff_hbm, cdamp_hbm,
    out, corr_out,
    init, torque, contact, minv, stiff, damp, gravity, cstiff, cdamp,
    tx, rx, mtx, mrx, rowtx, rows, raw, inits,
    tstage, gains, tq, spring, fric, grav, cspring, cfric, wgt, stage, wtmp, ybuf, ubuf, ly, lu,
    cmap, qmap, bmap, ctmp, xs, ends_buf,
    btx, brx, stx, srx, otx, orx, ctx, crx,
    lsem, tsend, trecv, msend, mrecv, rsend, rrecv, bsend, brecv, ssend, srecv, osend, orecv, csend, crecv,
):
    pairs = (
        (torque_hbm, torque), (contact_hbm, contact), (minv_hbm, minv), (init_hbm, init), (stiff_hbm, stiff),
        (damp_hbm, damp), (gravity_hbm, gravity), (cstiff_hbm, cstiff), (cdamp_hbm, cdamp),
    )
    local = [pltpu.make_async_copy(src, dst, lsem.at[i]) for i, (src, dst) in enumerate(pairs)]
    nz = NZ
    half = nz // 2
    line = nz * CORES
    blocks = tm // line * CORES
    env_local = init.shape[1]
    epd = env_local // nz
    slices = HS * nz
    per_tile = LANES // epd
    tiles = env_local // LANES
    plan = Plan(nz)
    me_t = lax.axis_index("tm")
    me_e = lax.axis_index("env")
    x = me_t // line
    z = lax.rem(me_t // CORES, nz)
    c = lax.rem(me_t, CORES)
    block_t = x * CORES + c
    dest_core = z // half
    my_source = lax.rem(z, half) * CORES + c
    own_here = dest_core == c
    barrier = pltpu.get_barrier_semaphore()

    def source_index(i):
        return x * line + (c * half + i // CORES) * CORES + lax.rem(i, CORES)

    def dest_index(k):
        return x * line + lax.rem(z + k, nz) * CORES + dest_core

    def block_index(t):
        return t // CORES * line + z * CORES + lax.rem(t, CORES)

    @pl.loop(1, tm, unroll=True)
    def _(k):
        pl.semaphore_signal(
            barrier, inc=1, device_id={"tm": lax.rem(me_t + k, tm), "env": me_e}, device_id_type=MESH
        )

    for copy in local:
        copy.start()

    @pl.loop(1, ny)
    def _(r):
        @pl.loop(0, nz, unroll=True)
        def _(i):
            pl.semaphore_signal(
                barrier, inc=1,
                device_id={"tm": source_index(i), "env": lax.rem(me_e + r, ny)},
                device_id_type=MESH,
            )

    for copy in local:
        copy.wait()
    lane_of = lax.broadcasted_iota(jnp.int32, (1, LANES), 1)
    lane_group = lane_of // epd

    raw[...] = jnp.zeros(raw.shape, F32)
    hits = contact[...].astype(F32)
    for k in range(2 * HS):
        raw[k, 0:DOF, :] = torque[:, k, :]
        raw[k, DOF : DOF + 1, :] = hits[k : k + 1, :]
    wtmp[...] = jnp.zeros(wtmp.shape, F32)
    wtmp[0:DOF, 0:DOF] = minv[:, 0, :]
    wtmp[40 : 40 + DOF, 0:DOF] = minv[:, 1, :]
    row_of = lax.broadcasted_iota(jnp.int32, (40, LANES), 0)
    lower = lane_of <= row_of
    packed = jnp.where(lower, wtmp[0:40, :], pltpu.roll(wtmp[40:80, :], 1, 1))
    last = jnp.concatenate([packed[32:40], jnp.zeros((8, LANES), F32)], axis=0)
    mtx[...] = packed[0:16] + pltpu.roll(packed[16:32], FOLD, 1) + pltpu.roll(last, 2 * FOLD, 1)
    for h in range(tiles):
        rolled = {}
        for k in range(2 * HS):
            v = raw[k, :, h * LANES : (h + 1) * LANES]
            for r in range(per_tile):
                rolled[k, r] = v if r == 0 else pltpu.roll(v, r * epd, 1)
        for q in range(per_tile):
            acc = rolled[0, (0 - q) % per_tile]
            for k in range(1, 2 * HS):
                acc = jnp.where(lane_group == k, rolled[k, (k - q) % per_tile], acc)
            tx[h * per_tile + q] = acc
    totals = jnp.sum(hits, axis=1, keepdims=True)
    row = jnp.zeros((1, LANES), F32)
    for k in range(2 * HS):
        row = jnp.where(lane_of == 3 * FOLD + k, jnp.broadcast_to(totals[k : k + 1], (1, LANES)), row)
    rowtx[...] = row
    mtx[0:1, :] = mtx[0:1, :] + row

    pl.semaphore_wait(barrier, tm - 1 + (ny - 1) * nz)

    def in_copy(k):
        return pltpu.make_async_remote_copy(
            src_ref=tx.at[lax.rem(z + k, nz)],
            dst_ref=rx.at[my_source],
            send_sem=tsend.at[k],
            recv_sem=trecv.at[my_source],
            device_id={"tm": dest_index(k), "env": me_e},
            device_id_type=MESH,
        )

    def in_arrival(i):
        return pltpu.make_async_remote_copy(
            src_ref=tx.at[0],
            dst_ref=rx.at[i],
            send_sem=tsend.at[0],
            recv_sem=trecv.at[i],
            device_id={"tm": dest_index(0), "env": me_e},
            device_id_type=MESH,
        )

    def mat_copy(k):
        return pltpu.make_async_remote_copy(
            src_ref=mtx,
            dst_ref=mrx.at[my_source],
            send_sem=msend.at[k],
            recv_sem=mrecv.at[my_source],
            device_id={"tm": dest_index(k), "env": me_e},
            device_id_type=MESH,
        )

    def mat_arrival(i):
        return pltpu.make_async_remote_copy(
            src_ref=mtx,
            dst_ref=mrx.at[i],
            send_sem=msend.at[0],
            recv_sem=mrecv.at[i],
            device_id={"tm": dest_index(0), "env": me_e},
            device_id_type=MESH,
        )

    def row_copy(k, r):
        return pltpu.make_async_remote_copy(
            src_ref=rowtx,
            dst_ref=rows.at[r, my_source],
            send_sem=rsend.at[0],
            recv_sem=rrecv.at[0],
            device_id={"tm": dest_index(k), "env": lax.rem(me_e + r, ny)},
            device_id_type=MESH,
        )

    def rows_all():
        return pltpu.make_async_remote_copy(
            src_ref=rows.at[pl.ds(1, ny - 1)],
            dst_ref=rows.at[pl.ds(1, ny - 1)],
            send_sem=rsend.at[0],
            recv_sem=rrecv.at[0],
            device_id={"tm": dest_index(0), "env": lax.rem(me_e + 1, ny)},
            device_id_type=MESH,
        )

    def other(k):
        return jnp.logical_not(jnp.logical_and(own_here, k == 0))

    def other_source(i):
        return jnp.logical_not(jnp.logical_and(own_here, i == my_source))

    for r in range(1, ny):
        for k in range(nz):
            row_copy(k, r).start()
    far_first = sorted(range(nz), key=lambda k: -min(k, nz - k))
    for make in (mat_copy, in_copy):
        for k in far_first:
            @pl.when(other(k))
            def _(k=k, make=make):
                make(k).start()

    @pl.when(own_here)
    def _():
        rx[my_source] = tx[z]
        mrx[my_source] = mtx[...]

    ratio = float(SUB)
    stiff, damp, gravity, cstiff, cdamp = (r[...] for r in (stiff, damp, gravity, cstiff, cdamp))
    to_u = TWO_PI / fine_dt
    scale = jnp.where(lane_of < DOF, TWO_PI, to_u)
    shrink = jnp.where(lane_of < DOF, 1.0 / TWO_PI, 1.0 / to_u)

    for ref in (tstage, gains, tq, spring, fric, grav, cspring, cfric, ybuf, ubuf, ly, lu, ctmp, stage, wgt, cmap, qmap, bmap):
        clear(ref)
    for h in range(tiles):
        inits[h * LANES : (h + 1) * LANES, :] = (
            pad_rows(init[:, h * LANES : (h + 1) * LANES], LANES).T * shrink
        )
    start_state = inits[pl.ds(pl.multiple_of(z * epd, epd), epd), :]
    first_start = jnp.where(block_t == 0, start_state, 0.0)
    rank = lax.broadcasted_iota(jnp.int32, (DEPTH, DOF), 0)
    col = lax.broadcasted_iota(jnp.int32, (DEPTH, DOF), 1)
    for n in range(slices):
        cut = pl.ds(plan.where[n], DOF)
        ly[:, cut] = jnp.where(rank == col, 1.0, 0.0)
        lu[:, cut] = jnp.where(rank == col + DOF, 1.0, 0.0)
        grav[:, cut] = gravity
        gains[0, :, cut] = TWO_PI * stiff
        gains[1, :, cut] = TWO_PI * cstiff
        gains[2, :, cut] = to_u * damp
        gains[3, :, cut] = to_u * cdamp
        gains[4, :, cut] = TWO_PI * gravity
    ybuf[:, 0:DOF] = first_start[:, 0:DOF]
    ubuf[:, 0:DOF] = first_start[:, DOF : 2 * DOF]

    square_row = lax.broadcasted_iota(jnp.int32, (40, LANES), 0)
    for i in range(nz):
        @pl.when(other_source(i))
        def _(i=i):
            mat_arrival(i).wait_recv()

        folded = mrx[i]
        square = jnp.concatenate(
            [folded, pltpu.roll(folded, LANES - FOLD, 1), pltpu.roll(folded[0:8], LANES - 2 * FOLD, 1)], axis=0
        )
        shifted = pltpu.roll(square, LANES - 1, 1)
        turned = pad_rows(jnp.concatenate([square, shifted], axis=0), LANES).T
        matrices = (
            jnp.where(lane_of <= square_row, square, turned[0:40]),
            jnp.where(lane_of >= square_row, shifted, pltpu.roll(turned[0:40], LANES - 40, 1)),
        )
        for a in range(HS):
            n = HS * i + a
            cut = pl.ds(plan.where[n], DOF)
            g, pos = plan.slot[n]
            stage[g, pl.ds(pos * DOF, DOF), pl.ds(pos * DOF, DOF)] = (
                fine_dt * fine_dt / TWO_PI
            ) * matrices[a][0:DOF, 0:DOF]
    for g, (base, members, a) in enumerate(plan.groups):
        put(wgt, g, stage[g])

    def product(force, g):
        return through(force, wgt[g])

    if ny > 1:
        rows_all().wait_recv()
    counts = []
    for i in range(nz):
        total = mrx[i, 0:1, :]
        for r in range(1, ny):
            total = total + rows[r, i]
        counts.append(total * (1.0 / (env_local * ny)))
    for base, members, a in plan.groups:
        cut = pl.ds(base, LANES)
        for j in range(HS):
            spot = 3 * FOLD + a * HS + j
            mean = counts[members[0]][:, spot : spot + 1]
            for pos, i in enumerate(members):
                mean = jnp.where(lane_of >= pos * DOF, counts[i][:, spot : spot + 1], mean)
            cspring[j, :, cut] = gains[0, :, cut] + gains[4, :, cut] + mean * gains[1, :, cut]
            cfric[j, :, cut] = gains[2, :, cut] + mean * gains[3, :, cut]

    for g, (base, members, a) in enumerate(plan.groups):
        cut = pl.ds(base, LANES)
        y, u = ly[:, cut], lu[:, cut]
        for j in range(HS):
            force = -cspring[j, :, cut] * y - cfric[j, :, cut] * u
            u = u + ratio * product(force, g)
            y = y + ratio * u
        ly[:, cut] = y
        lu[:, cut] = u
    levels = slices.bit_length() - 1
    stacks = []
    for n in range(slices):
        cut = pl.ds(plan.where[n], DOF)
        ctmp[:, 0:DOF] = ly[:, cut]
        ctmp[:, DOF : 2 * DOF] = lu[:, cut]
        stacks.append(ctmp[...])

    def right_half(level):
        step = 1 << level
        found = []
        for m in range(0, slices, 2 * step):
            for i in range(step):
                found.append((level * (slices // 2) + len(found), m + step - 1, m + step + i))
        if level == levels - 1:
            found = found[-1:] + found[:-1]
        return found

    for level in range(levels):
        for place, left, n in right_half(level):
            put(cmap, place, stacks[n])
        for place, left, n in right_half(level):
            stacks[n] = through(stacks[left], cmap[place])
    btx[...] = fold_map(stacks[slices - 1], lane_of)
    for n in range(slices):
        put(qmap, n, stacks[n])

    def sweep(ends, k):
        for level in range(levels):
            for place, left, n in right_half(level):
                ends[n] = ends[n] + through(ends[left], cmap[place])
                if n == slices - 1 and level == levels - 1:
                    stx[k] = ends[n]
                    send_blocks(functools.partial(sweep_copy, k))
        for n in range(slices):
            ends_buf[n] = ends[n]

    def first_copy(d):
        return pltpu.make_async_remote_copy(
            src_ref=btx,
            dst_ref=brx.at[block_t],
            send_sem=bsend.at[d],
            recv_sem=brecv.at[d],
            device_id={"tm": block_index(block_t + d), "env": me_e},
            device_id_type=MESH,
        )

    def first_arrival(d):
        return pltpu.make_async_remote_copy(
            src_ref=btx,
            dst_ref=brx.at[block_t - d],
            send_sem=bsend.at[d],
            recv_sem=brecv.at[d],
            device_id={"tm": block_index(block_t - d), "env": me_e},
            device_id_type=MESH,
        )

    def sweep_copy(k, d):
        return pltpu.make_async_remote_copy(
            src_ref=stx.at[k],
            dst_ref=srx.at[k, block_t],
            send_sem=ssend.at[k, d],
            recv_sem=srecv.at[k, d],
            device_id={"tm": block_index(block_t + d), "env": me_e},
            device_id_type=MESH,
        )

    def sweep_arrival(k, d):
        return pltpu.make_async_remote_copy(
            src_ref=stx.at[k],
            dst_ref=srx.at[k, block_t - d],
            send_sem=ssend.at[k, d],
            recv_sem=srecv.at[k, d],
            device_id={"tm": block_index(block_t - d), "env": me_e},
            device_id_type=MESH,
        )

    def send_blocks(copy):
        @pl.loop(1, blocks)
        def _(d):
            @pl.when(block_t + d < blocks)
            def _():
                copy(d).start()

    def await_blocks(arrival):
        @pl.loop(1, blocks)
        def _(d):
            @pl.when(block_t - d >= 0)
            def _():
                arrival(d).wait_recv()

    def drain_blocks(copy):
        @pl.loop(1, blocks)
        def _(d):
            @pl.when(block_t + d < blocks)
            def _():
                copy(d).wait_send()

    @pl.when(block_t > 0)
    def _():
        send_blocks(first_copy)

    mark = plan.per * DOF
    for part in range(0, nz, plan.per):
        for pos, i in enumerate(range(part, min(part + plan.per, nz))):
            @pl.when(other_source(i))
            def _(i=i):
                in_arrival(i).wait_recv()

            tstage[part // plan.per, pos * DOF : (pos + 1) * DOF, :] = rx[i, 0:DOF, :]
            tstage[part // plan.per, mark + pos : mark + pos + 1, :] = rx[i, DOF : DOF + 1, :]
        turned = tstage[part // plan.per].T
        for a in range(HS):
            base = (part // plan.per * HS + a) * LANES
            cut = pl.ds(base, LANES)
            for j in range(HS):
                k = a * HS + j
                piece = turned[k * epd : (k + 1) * epd, :]
                hit = piece[:, mark : mark + 1]
                for pos in range(1, plan.per):
                    hit = jnp.where(lane_of >= pos * DOF, piece[:, mark + pos : mark + pos + 1], hit)
                tq[j, :, cut] = jnp.where(lane_of < mark, piece, 0.0)
                spring[j, :, cut] = gains[0, :, cut] + hit * gains[1, :, cut]
                fric[j, :, cut] = gains[2, :, cut] + hit * gains[3, :, cut]

    for g, (base, members, a) in enumerate(plan.groups):
        cut = pl.ds(base, LANES)
        y, u = ybuf[:, cut], ubuf[:, cut]
        for j in range(HS):
            force = tq[j, :, cut] - cspring[j, :, cut] * y - cfric[j, :, cut] * u
            u = u + ratio * product(force, g)
            y = y + ratio * u
        ybuf[:, cut] = y
        ubuf[:, cut] = u

    def packed_state(n):
        cut = pl.ds(plan.where[n], DOF)
        zero = jnp.zeros((epd, LANES - 2 * DOF), F32)
        return jnp.concatenate([ybuf[:, cut], ubuf[:, cut], zero], axis=1)

    ends = [packed_state(n) for n in range(slices)]
    sweep(ends, 0)
    @pl.loop(1, blocks)
    def _(d):
        @pl.when(block_t - d > 0)
        def _():
            first_arrival(d).wait_recv()

    eye = jnp.where(
        lax.broadcasted_iota(jnp.int32, (DEPTH, LANES), 0) == lane_of, 1.0, 0.0
    )
    maps = {t: jnp.where(t < block_t, unfold_map(brx[t], lane_of), eye) for t in range(1, blocks - 1)}
    pieces = {(t, t): maps[t] for t in maps}

    def join(a, b, c):
        if (a, c) not in pieces:
            slot = weights.setdefault((b, c), len(weights))
            if slot == len(weights) - 1:
                put(bmap, slot, pieces[b, c])
            pieces[a, c] = through(pieces[a, b - 1], bmap[slot])

    weights = {}
    top = blocks - 2
    span = 1
    while span < blocks:
        for last in range(top, 0, -2 * span):
            mid = last - span + 1
            if mid <= 1:
                continue
            for first in range(max(1, mid - span), mid):
                join(first, mid, last)
        span *= 2
    for t in range(blocks - 2):
        if (t + 1, top) not in weights:
            weights[t + 1, top] = len(weights)
            put(bmap, weights[t + 1, top], pieces[t + 1, top])

    def enter(k):
        total = jnp.where(blocks - 2 < block_t, srx[k, blocks - 2], 0.0)
        for t in range(blocks - 2):
            total = total + through(jnp.where(t < block_t, srx[k, t], 0.0), bmap[weights[t + 1, top]])
        return total

    await_blocks(functools.partial(sweep_arrival, 0))
    entry = enter(0)
    xs[0] = jnp.where(block_t == 0, start_state, entry)
    for n in range(slices):
        xs[n + 1] = ends_buf[n] + through(entry, qmap[n])

    def iteration(k, corrections):
        for n in range(slices):
            cut = pl.ds(plan.where[n], DOF)
            ybuf[:, cut] = xs[n, :, 0:DOF]
            ubuf[:, cut] = xs[n, :, DOF : 2 * DOF]
        for j in range(HS):

            def substep(counter, carry):
                result = []
                for g, (base, members, a) in enumerate(plan.groups):
                    y, u = carry[g]
                    cut = pl.ds(base, LANES)
                    t = y - jnp.round(y)
                    s = t * t
                    s2 = s * s
                    poly = (SIN[0] + SIN[1] * s) + s2 * ((SIN[2] + SIN[3] * s) + s2 * (SIN[4] + SIN[5] * s))
                    force = (
                        tq[j, :, cut]
                        - spring[j, :, cut] * y
                        - fric[j, :, cut] * u
                        - (grav[:, cut] * t) * poly
                    )
                    u = u + product(force, g)
                    y = y + u
                    result.append((y, u))
                return tuple(result)

            first_state = tuple(
                (ybuf[:, pl.ds(base, LANES)], ubuf[:, pl.ds(base, LANES)])
                for base, members, a in plan.groups
            )
            last = lax.fori_loop(0, SUB, substep, first_state, unroll=UNROLL)
            for g, (base, members, a) in enumerate(plan.groups):
                ybuf[:, pl.ds(base, LANES)] = last[g][0]
                ubuf[:, pl.ds(base, LANES)] = last[g][1]

        ends = [packed_state(n) - xs[n + 1] for n in range(slices)]
        sweep(ends, k + 1)
        await_blocks(functools.partial(sweep_arrival, k + 1))
        entry = enter(k + 1)
        xs[0] = xs[0] + entry
        worst = jnp.zeros((epd, 1), F32)
        for n in range(slices):
            change = ends_buf[n] + through(entry, qmap[n])
            real = change * scale
            worst = jnp.maximum(worst, jnp.sum(real * real, axis=1, keepdims=True))
            xs[n + 1] = xs[n + 1] + change
        return jnp.where(lane_of == k, jnp.sqrt(worst), corrections)

    corrections = lax.fori_loop(0, ITERS, iteration, jnp.zeros((epd, LANES), F32))

    turned = pad_rows(corrections, LANES).T
    row = turned[0:1]
    for k in range(1, ITERS):
        row = jnp.where(lane_group == k, pltpu.roll(turned[k : k + 1], k * epd, 1), row)
    ctx[...] = row
    for i in range(nz):
        parts = []
        for a in range(HS):
            real = xs[HS * i + a + 1] * scale
            parts.append(real)
            parts.append(pltpu.roll(real, LANES - DOF, 1))
        otx[i] = jnp.concatenate(parts, axis=0).T[0:ROWS_OUT, :]

    def out_copy(i):
        return pltpu.make_async_remote_copy(
            src_ref=otx.at[i],
            dst_ref=orx.at[z],
            send_sem=osend.at[i],
            recv_sem=orecv.at[z],
            device_id={"tm": source_index(i), "env": me_e},
            device_id_type=MESH,
        )

    def out_arrival(k):
        return pltpu.make_async_remote_copy(
            src_ref=otx.at[0],
            dst_ref=orx.at[lax.rem(z + k, nz)],
            send_sem=osend.at[0],
            recv_sem=orecv.at[lax.rem(z + k, nz)],
            device_id={"tm": dest_index(k), "env": me_e},
            device_id_type=MESH,
        )

    def corr_copy(k):
        return pltpu.make_async_remote_copy(
            src_ref=ctx,
            dst_ref=crx.at[k],
            send_sem=csend.at[0],
            recv_sem=crecv.at[0],
            device_id={"tm": lax.rem(me_t + k, tm), "env": me_e},
            device_id_type=MESH,
        )

    @pl.loop(1, tm, unroll=True)
    def _(k):
        corr_copy(k).start()

    @pl.loop(0, nz)
    def _(i):
        @pl.when(other_source(i))
        def _():
            out_copy(i).start()

    crx[0] = ctx[...]

    @pl.when(own_here)
    def _():
        orx[z] = otx[my_source]

    @pl.loop(0, nz)
    def _(k):
        @pl.when(other(k))
        def _():
            out_arrival(k).wait_recv()

    for h in range(tiles):
        for k in range(2 * HS):
            a, half_state = divmod(k, 2)
            tile = None
            for q in range(per_tile):
                r = (q - k) % per_tile
                v = orx[h * per_tile + q]
                v = v if r == 0 else pltpu.roll(v, r * epd, 1)
                tile = v if tile is None else jnp.where(lane_group == q, v, tile)
            out[half_state * DOF : half_state * DOF + DOF, a, h * LANES : (h + 1) * LANES] = tile[0:DOF]

    pltpu.make_async_remote_copy(
        src_ref=crx.at[pl.ds(1, tm - 1)],
        dst_ref=crx.at[pl.ds(1, tm - 1)],
        send_sem=csend.at[0],
        recv_sem=crecv.at[0],
        device_id={"tm": lax.rem(me_t + 1, tm), "env": me_e},
        device_id_type=MESH,
    ).wait()
    worst = []
    for p in range(nz):
        most = None
        for t in range(blocks):
            sender = t // CORES * line + p * CORES + t % CORES
            value = crx[lax.rem(me_t - sender + tm, tm)]
            most = value if most is None else jnp.maximum(most, value)
        worst.append(most)
    for h in range(tiles):
        for k in range(ITERS):
            tile = None
            for q in range(per_tile):
                r = (q - k) % per_tile
                v = worst[h * per_tile + q]
                v = v if r == 0 else pltpu.roll(v, r * epd, 1)
                tile = v if tile is None else jnp.where(lane_group == q, v, tile)
            corr_out[k : k + 1, h * LANES : (h + 1) * LANES] = tile

    @pl.loop(0, nz)
    def _(k):
        @pl.when(other(k))
        def _():
            in_copy(k).wait_send()
            mat_copy(k).wait_send()

        @pl.when(other_source(k))
        def _():
            out_copy(k).wait_send()

    if ny > 1:
        rows_all().wait_send()

    @pl.when(block_t > 0)
    def _():
        drain_blocks(first_copy)

    for k in range(ITERS + 1):
        drain_blocks(functools.partial(sweep_copy, k))


def body(tm, env, init_state, torque, contact, mass_inverse, stiffness, damping, gravity,
         contact_stiffness, contact_damping):
    nz = NZ
    env_local = init_state.shape[1]
    epd = env_local // nz
    slices = HS * nz
    blocks = tm // (nz * CORES) * CORES
    plan = Plan(nz)
    groups = len(plan.groups)
    lanes = plan.lanes
    vm = pltpu.VMEM
    dma = pltpu.SemaphoreType.DMA
    vmem = pl.BlockSpec(memory_space=pltpu.VMEM)
    both = vm((HS, epd, lanes), F32)
    thin = vm((HS, 1, lanes), F32)
    levels = slices.bit_length() - 1
    prm = [p.reshape(1, DOF) for p in (stiffness, damping, gravity, contact_stiffness, contact_damping)]
    states, corrections = pl.pallas_call(
        functools.partial(kernel, tm, env),
        out_shape=(
            vm((STATE, HS, env_local), F32),
            vm((ITERS, env_local), F32),
        ),
        in_specs=[pl.BlockSpec(memory_space=pl.ANY)] * 9,
        out_specs=(vmem, vmem),
        scratch_shapes=[
            vm(init_state.shape, F32), vm((DOF, 2 * HS, env_local), F32), vm(contact.shape, jnp.int32),
            vm((DOF, HS, DOF), F32), *[vm((1, DOF), F32)] * 5,
            vm((nz, ROWS_IN, LANES), F32), vm((nz, ROWS_IN, LANES), F32),
            vm((ROWS_MAT, LANES), F32), vm((nz, ROWS_MAT, LANES), F32),
            vm((1, LANES), F32), vm((env, nz, 1, LANES), F32),
            vm((2 * HS, 40, env_local), F32), vm((env_local, LANES), F32),
            vm((-(-nz // plan.per), LANES, LANES), F32), vm((5, 1, lanes), F32),
            both, both, both, vm((1, lanes), F32), thin, thin,
            vm((groups, WIDE, WIDE), BF16), vm((groups, LANES, LANES), F32), vm((LANES, LANES), F32),
            vm((epd, lanes), F32), vm((epd, lanes), F32),
            vm((DEPTH, lanes), F32), vm((DEPTH, lanes), F32),
            vm((levels * slices // 2, WIDE, WIDE), BF16),
            vm((slices, WIDE, WIDE), BF16), vm((2 * blocks, WIDE, WIDE), BF16),
            vm((DEPTH, LANES), F32),
            vm((slices + 1, epd, LANES), F32), vm((slices, epd, LANES), F32),
            vm((ROWS_MAP, LANES), F32), vm((blocks, ROWS_MAP, LANES), F32),
            vm((ITERS + 1, epd, LANES), F32), vm((ITERS + 1, blocks, epd, LANES), F32),
            vm((nz, ROWS_OUT, LANES), F32), vm((nz, ROWS_OUT, LANES), F32),
            vm((1, LANES), F32), vm((tm, 1, LANES), F32),
            dma((9,)), dma((nz,)), dma((nz,)), dma((nz,)), dma((nz,)), dma((1,)), dma((1,)),
            dma((blocks,)), dma((blocks,)), dma((ITERS + 1, blocks)), dma((ITERS + 1, blocks)),
            dma((nz,)), dma((nz,)), dma((1,)), dma((1,)),
        ],
        compiler_params=pltpu.CompilerParams(collective_id=0, has_side_effects=True),
        name="parareal",
    )(
        init_state, torque.transpose(1, 0, 2), contact, mass_inverse.transpose(1, 0, 2), *prm
    )
    return states.transpose(1, 0, 2), corrections


def solution(mesh):
    placed = (
        P(None, "env"),
        P("tm", None, "env"),
        P("tm", "env"),
        P("tm", None, None),
        P(),
        P(),
        P(),
        P(),
        P(),
    )
    return jax.shard_map(
        functools.partial(body, mesh.shape["tm"], mesh.shape["env"]),
        mesh=mesh,
        in_specs=placed,
        out_specs=(P("tm", None, "env"), P(None, "env")),
        check_vma=False,
    )
```

```python
import functools
import math

import jax
import jax.numpy as jnp
from jax import lax
from jax.experimental import pallas as pl
from jax.experimental.pallas import tpu as pltpu
from jax.sharding import PartitionSpec as P

DOF = 35
STATE = 70
HS = 2
SUB = 32
ITERS = 3
LANES = 128
WIDE = 256
NZ = 8
CORES = 2
UNROLL = 32

step_length = 0.05
fine_dt = step_length / SUB
TWO_PI = 2.0 * math.pi
MESH = pl.DeviceIdType.MESH
F32 = jnp.float32
BF16 = jnp.bfloat16

SIN = (
    6.283182818551188, -41.341421398631915, 81.59618387021051,
    -76.58010048603072, 41.205394649903326, -12.271261959178284,
)

ROWS_IN = 40
ROWS_MAT = 16
FOLD = 36
ROWS_OUT = 40
DEPTH = 72
ROWS_MAP = 48


def split(value):
    high = value.astype(BF16)
    return high, (value - high.astype(F32)).astype(BF16)


def dot(left, right):
    return jnp.dot(left, right, preferred_element_type=F32)


def through(state, weight):
    high, low = split(state)
    both = dot(jnp.concatenate([high, low], axis=1), weight)
    return both[:, :LANES] + both[:, LANES:]


def clear(ref):
    ref[...] = jnp.zeros(ref.shape, ref.dtype)


def put(ref, n, value):
    high, low = split(value)
    rows = value.shape[0]
    ref[n, 0:rows, 0:LANES] = high
    ref[n, LANES : LANES + rows, 0:LANES] = high
    ref[n, 0:rows, LANES:] = low


def pad_rows(value, rows):
    return jnp.concatenate([value, jnp.zeros((rows - value.shape[0], value.shape[1]), F32)], axis=0)


def fold_map(value, lane_of):
    value = jnp.where(lane_of < DOF, value, 0.0), jnp.where(lane_of < DOF, pltpu.roll(value, LANES - DOF, 1), 0.0)
    tall = jnp.concatenate(value, axis=0)
    first, second, third = (tall[r : r + ROWS_MAP] for r in range(0, 2 * DEPTH, ROWS_MAP))
    return first + pltpu.roll(second, DOF, 1) + pltpu.roll(third, 2 * DOF, 1)


def unfold_map(value, lane_of):
    tall = jnp.concatenate(
        [value, pltpu.roll(value, LANES - DOF, 1), pltpu.roll(value, LANES - 2 * DOF, 1)], axis=0
    )
    right = jnp.where(lane_of < 2 * DOF, pltpu.roll(tall[DEPTH:], DOF, 1), 0.0)
    return jnp.where(lane_of < DOF, tall[0:DEPTH], right)


class Plan:
    def __init__(self, sources):
        self.per = LANES // DOF
        self.groups = []
        self.slot = {}
        for first in range(0, sources, self.per):
            members = range(first, min(first + self.per, sources))
            for a in range(HS):
                for pos, i in enumerate(members):
                    self.slot[HS * i + a] = (len(self.groups), pos)
                self.groups.append((len(self.groups) * LANES, members, a))
        self.where = [self.slot[n][0] * LANES + self.slot[n][1] * DOF for n in range(HS * sources)]
        self.lanes = len(self.groups) * LANES


def kernel(
    tm, ny,
    init_hbm, torque_hbm, contact_hbm, minv_hbm, stiff_hbm, damp_hbm, gravity_hbm, cstiff_hbm, cdamp_hbm,
    out, corr_out,
    init, torque, contact, minv, stiff, damp, gravity, cstiff, cdamp,
    tx, rx, mtx, mrx, rowtx, rows, raw, inits,
    tstage, hstage, gains, tq, spring, fric, grav, cspring, cfric, wgt, stage, wtmp, ybuf, ubuf, ly, lu,
    cmap, qmap, bmap, ctmp, xs, ends_buf,
    btx, brx, stx, srx, otx, orx, ctx, crx,
    lsem, tsend, trecv, msend, mrecv, rsend, rrecv, bsend, brecv, ssend, srecv, osend, orecv, csend, crecv,
):
    pairs = (
        (torque_hbm, torque), (contact_hbm, contact), (minv_hbm, minv), (init_hbm, init), (stiff_hbm, stiff),
        (damp_hbm, damp), (gravity_hbm, gravity), (cstiff_hbm, cstiff), (cdamp_hbm, cdamp),
    )
    local = [pltpu.make_async_copy(src, dst, lsem.at[i]) for i, (src, dst) in enumerate(pairs)]
    nz = NZ
    half = nz // 2
    line = nz * CORES
    blocks = tm // line * CORES
    env_local = init.shape[1]
    epd = env_local // nz
    slices = HS * nz
    per_tile = LANES // epd
    tiles = env_local // LANES
    plan = Plan(nz)
    me_t = lax.axis_index("tm")
    me_e = lax.axis_index("env")
    x = me_t // line
    z = lax.rem(me_t // CORES, nz)
    c = lax.rem(me_t, CORES)
    block_t = x * CORES + c
    dest_core = z // half
    my_source = lax.rem(z, half) * CORES + c
    own_here = dest_core == c
    barrier = pltpu.get_barrier_semaphore()

    def source_index(i):
        return x * line + (c * half + i // CORES) * CORES + lax.rem(i, CORES)

    def dest_index(k):
        return x * line + lax.rem(z + k, nz) * CORES + dest_core

    def block_index(t):
        return t // CORES * line + z * CORES + lax.rem(t, CORES)

    @pl.loop(1, tm, unroll=True)
    def _(k):
        pl.semaphore_signal(
            barrier, inc=1, device_id={"tm": lax.rem(me_t + k, tm), "env": me_e}, device_id_type=MESH
        )

    for copy in local:
        copy.start()

    @pl.loop(1, ny)
    def _(r):
        @pl.loop(0, nz, unroll=True)
        def _(i):
            pl.semaphore_signal(
                barrier, inc=1,
                device_id={"tm": source_index(i), "env": lax.rem(me_e + r, ny)},
                device_id_type=MESH,
            )

    for copy in local:
        copy.wait()
    lane_of = lax.broadcasted_iota(jnp.int32, (1, LANES), 1)
    lane_group = lane_of // epd

    raw[...] = jnp.zeros(raw.shape, F32)
    hits = contact[...].astype(F32)
    for k in range(2 * HS):
        raw[k, 0:DOF, :] = torque[:, k, :]
        raw[k, DOF : DOF + 1, :] = hits[k : k + 1, :]
    wtmp[...] = jnp.zeros(wtmp.shape, F32)
    wtmp[0:DOF, 0:DOF] = minv[:, 0, :]
    wtmp[40 : 40 + DOF, 0:DOF] = minv[:, 1, :]
    row_of = lax.broadcasted_iota(jnp.int32, (40, LANES), 0)
    lower = lane_of <= row_of
    packed = jnp.where(lower, wtmp[0:40, :], pltpu.roll(wtmp[40:80, :], 1, 1))
    last = jnp.concatenate([packed[32:40], jnp.zeros((8, LANES), F32)], axis=0)
    mtx[...] = packed[0:16] + pltpu.roll(packed[16:32], FOLD, 1) + pltpu.roll(last, 2 * FOLD, 1)
    for h in range(tiles):
        rolled = {}
        for k in range(2 * HS):
            v = raw[k, :, h * LANES : (h + 1) * LANES]
            for r in range(per_tile):
                rolled[k, r] = v if r == 0 else pltpu.roll(v, r * epd, 1)
        for q in range(per_tile):
            acc = rolled[0, (0 - q) % per_tile]
            for k in range(1, 2 * HS):
                acc = jnp.where(lane_group == k, rolled[k, (k - q) % per_tile], acc)
            tx[h * per_tile + q] = acc
    totals = jnp.sum(hits, axis=1, keepdims=True)
    row = jnp.zeros((1, LANES), F32)
    for k in range(2 * HS):
        row = jnp.where(lane_of == 3 * FOLD + k, jnp.broadcast_to(totals[k : k + 1], (1, LANES)), row)
    rowtx[...] = row
    mtx[0:1, :] = mtx[0:1, :] + row

    pl.semaphore_wait(barrier, tm - 1 + (ny - 1) * nz)

    def in_copy(k):
        return pltpu.make_async_remote_copy(
            src_ref=tx.at[lax.rem(z + k, nz)],
            dst_ref=rx.at[my_source],
            send_sem=tsend.at[0],
            recv_sem=trecv.at[my_source],
            device_id={"tm": dest_index(k), "env": me_e},
            device_id_type=MESH,
        )

    def in_arrival(i):
        return pltpu.make_async_remote_copy(
            src_ref=tx.at[0],
            dst_ref=rx.at[i],
            send_sem=tsend.at[0],
            recv_sem=trecv.at[i],
            device_id={"tm": dest_index(0), "env": me_e},
            device_id_type=MESH,
        )

    def mat_copy(k):
        return pltpu.make_async_remote_copy(
            src_ref=mtx,
            dst_ref=mrx.at[my_source],
            send_sem=msend.at[0],
            recv_sem=mrecv.at[my_source],
            device_id={"tm": dest_index(k), "env": me_e},
            device_id_type=MESH,
        )

    def mat_arrival(i):
        return pltpu.make_async_remote_copy(
            src_ref=mtx,
            dst_ref=mrx.at[i],
            send_sem=msend.at[0],
            recv_sem=mrecv.at[i],
            device_id={"tm": dest_index(0), "env": me_e},
            device_id_type=MESH,
        )

    def row_copy(k, r):
        return pltpu.make_async_remote_copy(
            src_ref=rowtx,
            dst_ref=rows.at[r, my_source],
            send_sem=rsend.at[0],
            recv_sem=rrecv.at[0],
            device_id={"tm": dest_index(k), "env": lax.rem(me_e + r, ny)},
            device_id_type=MESH,
        )

    def rows_all():
        return pltpu.make_async_remote_copy(
            src_ref=rows.at[pl.ds(1, ny - 1)],
            dst_ref=rows.at[pl.ds(1, ny - 1)],
            send_sem=rsend.at[0],
            recv_sem=rrecv.at[0],
            device_id={"tm": dest_index(0), "env": lax.rem(me_e + 1, ny)},
            device_id_type=MESH,
        )

    def other(k):
        return jnp.logical_not(jnp.logical_and(own_here, k == 0))

    def other_source(i):
        return jnp.logical_not(jnp.logical_and(own_here, i == my_source))

    for r in range(1, ny):
        for k in range(nz):
            row_copy(k, r).start()
    far_first = sorted(range(nz), key=lambda k: -min(k, nz - k))
    for make in (mat_copy, in_copy):
        for k in far_first:
            @pl.when(other(k))
            def _(k=k, make=make):
                make(k).start()

    @pl.when(own_here)
    def _():
        rx[my_source] = tx[z]
        mrx[my_source] = mtx[...]

    ratio = float(SUB)
    stiff, damp, gravity, cstiff, cdamp = (r[...] for r in (stiff, damp, gravity, cstiff, cdamp))
    to_u = TWO_PI / fine_dt
    scale = jnp.where(lane_of < DOF, TWO_PI, to_u)
    shrink = jnp.where(lane_of < DOF, 1.0 / TWO_PI, 1.0 / to_u)

    for ref in (tstage, hstage, gains, tq, spring, fric, grav, cspring, cfric, ybuf, ubuf, ly, lu, ctmp, stage, wgt, cmap, qmap, bmap):
        clear(ref)
    for h in range(tiles):
        inits[h * LANES : (h + 1) * LANES, :] = (
            pad_rows(init[:, h * LANES : (h + 1) * LANES], LANES).T * shrink
        )
    start_state = inits[pl.ds(pl.multiple_of(z * epd, epd), epd), :]
    first_start = jnp.where(block_t == 0, start_state, 0.0)
    rank = lax.broadcasted_iota(jnp.int32, (DEPTH, DOF), 0)
    col = lax.broadcasted_iota(jnp.int32, (DEPTH, DOF), 1)
    for n in range(slices):
        cut = pl.ds(plan.where[n], DOF)
        ly[:, cut] = jnp.where(rank == col, 1.0, 0.0)
        lu[:, cut] = jnp.where(rank == col + DOF, 1.0, 0.0)
        grav[:, cut] = gravity
        gains[0, :, cut] = TWO_PI * stiff
        gains[1, :, cut] = TWO_PI * cstiff
        gains[2, :, cut] = to_u * damp
        gains[3, :, cut] = to_u * cdamp
        gains[4, :, cut] = TWO_PI * gravity
    ybuf[:, 0:DOF] = first_start[:, 0:DOF]
    ubuf[:, 0:DOF] = first_start[:, DOF : 2 * DOF]

    square_row = lax.broadcasted_iota(jnp.int32, (40, LANES), 0)
    for i in range(nz):
        @pl.when(other_source(i))
        def _(i=i):
            mat_arrival(i).wait_recv()

        folded = mrx[i]
        square = jnp.concatenate(
            [folded, pltpu.roll(folded, LANES - FOLD, 1), pltpu.roll(folded[0:8], LANES - 2 * FOLD, 1)], axis=0
        )
        shifted = pltpu.roll(square, LANES - 1, 1)
        turned = pad_rows(jnp.concatenate([square, shifted], axis=0), LANES).T
        matrices = (
            jnp.where(lane_of <= square_row, square, turned[0:40]),
            jnp.where(lane_of >= square_row, shifted, pltpu.roll(turned[0:40], LANES - 40, 1)),
        )
        for a in range(HS):
            n = HS * i + a
            cut = pl.ds(plan.where[n], DOF)
            g, pos = plan.slot[n]
            stage[g, pl.ds(pos * DOF, DOF), pl.ds(pos * DOF, DOF)] = (
                fine_dt * fine_dt / TWO_PI
            ) * matrices[a][0:DOF, 0:DOF]
    for g, (base, members, a) in enumerate(plan.groups):
        put(wgt, g, stage[g])

    def product(force, g):
        return through(force, wgt[g])

    if ny > 1:
        rows_all().wait_recv()
    counts = []
    for i in range(nz):
        total = mrx[i, 0:1, :]
        for r in range(1, ny):
            total = total + rows[r, i]
        counts.append(total * (1.0 / (env_local * ny)))
    for base, members, a in plan.groups:
        cut = pl.ds(base, LANES)
        for j in range(HS):
            spot = 3 * FOLD + a * HS + j
            mean = counts[members[0]][:, spot : spot + 1]
            for pos, i in enumerate(members):
                mean = jnp.where(lane_of >= pos * DOF, counts[i][:, spot : spot + 1], mean)
            cspring[j, :, cut] = gains[0, :, cut] + gains[4, :, cut] + mean * gains[1, :, cut]
            cfric[j, :, cut] = gains[2, :, cut] + mean * gains[3, :, cut]

    for g, (base, members, a) in enumerate(plan.groups):
        cut = pl.ds(base, LANES)
        y, u = ly[:, cut], lu[:, cut]
        for j in range(HS):
            force = -cspring[j, :, cut] * y - cfric[j, :, cut] * u
            u = u + ratio * product(force, g)
            y = y + ratio * u
        ly[:, cut] = y
        lu[:, cut] = u
    levels = slices.bit_length() - 1
    stacks = []
    for n in range(slices):
        cut = pl.ds(plan.where[n], DOF)
        ctmp[:, 0:DOF] = ly[:, cut]
        ctmp[:, DOF : 2 * DOF] = lu[:, cut]
        stacks.append(ctmp[...])

    def right_half(level):
        step = 1 << level
        found = []
        for m in range(0, slices, 2 * step):
            for i in range(step):
                found.append((level * (slices // 2) + len(found), m + step - 1, m + step + i))
        return found

    def steps(spine):
        return [
            [entry for entry in right_half(level) if ((entry[2] + 1) % (2 << level) == 0) == spine]
            for level in range(levels)
        ]


    for level in range(levels):
        for place, left, n in right_half(level):
            put(cmap, place, stacks[n])
        for place, left, n in right_half(level):
            stacks[n] = through(stacks[left], cmap[place])
    btx[...] = fold_map(stacks[slices - 1], lane_of)
    for n in range(slices):
        put(qmap, n, stacks[n])

    def sweep(ends, k):
        def advance(spine):
            for entries in steps(spine):
                for place, left, n in entries:
                    ends[n] = ends[n] + through(ends[left], cmap[place])

        advance(True)
        stx[k] = ends[slices - 1]
        send_blocks(functools.partial(sweep_copy, k))
        advance(False)
        for n in range(slices):
            ends_buf[n] = ends[n]

    def first_copy(d):
        return pltpu.make_async_remote_copy(
            src_ref=btx,
            dst_ref=brx.at[block_t],
            send_sem=bsend.at[0],
            recv_sem=brecv.at[0],
            device_id={"tm": block_index(block_t + d), "env": me_e},
            device_id_type=MESH,
        )

    def sweep_copy(k, d):
        return pltpu.make_async_remote_copy(
            src_ref=stx.at[k],
            dst_ref=srx.at[k, block_t],
            send_sem=ssend.at[k],
            recv_sem=srecv.at[k],
            device_id={"tm": block_index(block_t + d), "env": me_e},
            device_id_type=MESH,
        )

    def whole_copy(ref, send, recv):
        return pltpu.make_async_remote_copy(
            src_ref=ref, dst_ref=ref, send_sem=send, recv_sem=recv,
            device_id={"tm": block_index(lax.rem(block_t + 1, blocks)), "env": me_e},
            device_id_type=MESH,
        )

    def first_whole(count):
        return whole_copy(brx.at[pl.ds(0, count)], bsend.at[0], brecv.at[0])

    def sweep_whole(k, count):
        return whole_copy(srx.at[k, pl.ds(0, count)], ssend.at[k], srecv.at[k])

    def send_blocks(copy):
        for d in range(1, blocks):
            @pl.when(block_t + d < blocks)
            def _(d=d):
                copy(d).start()

    def await_blocks(whole, skip=0):
        for count in range(1, blocks - skip):
            @pl.when(block_t - skip == count)
            def _(count=count):
                whole(count).wait_recv()

    def drain_blocks(whole):
        for count in range(1, blocks):
            @pl.when(blocks - 1 - block_t == count)
            def _(count=count):
                whole(count).wait_send()

    @pl.when(block_t > 0)
    def _():
        send_blocks(first_copy)

    for part in range(0, nz, plan.per):
        for pos, i in enumerate(range(part, min(part + plan.per, nz))):
            @pl.when(other_source(i))
            def _(i=i):
                in_arrival(i).wait_recv()

            tstage[part // plan.per, pos * DOF : (pos + 1) * DOF, :] = rx[i, 0:DOF, :]
            hstage[part // plan.per, pos * DOF : (pos + 1) * DOF, :] = jnp.broadcast_to(
                rx[i, DOF : DOF + 1, :], (DOF, LANES)
            )
        turned = tstage[part // plan.per].T
        touched = hstage[part // plan.per].T
        for a in range(HS):
            base = (part // plan.per * HS + a) * LANES
            cut = pl.ds(base, LANES)
            for j in range(HS):
                k = a * HS + j
                hit = touched[k * epd : (k + 1) * epd, :]
                tq[j, :, cut] = turned[k * epd : (k + 1) * epd, :]
                spring[j, :, cut] = gains[0, :, cut] + hit * gains[1, :, cut]
                fric[j, :, cut] = gains[2, :, cut] + hit * gains[3, :, cut]

    for g, (base, members, a) in enumerate(plan.groups):
        cut = pl.ds(base, LANES)
        y, u = ybuf[:, cut], ubuf[:, cut]
        for j in range(HS):
            force = tq[j, :, cut] - cspring[j, :, cut] * y - cfric[j, :, cut] * u
            u = u + ratio * product(force, g)
            y = y + ratio * u
        ybuf[:, cut] = y
        ubuf[:, cut] = u

    def packed_state(n):
        cut = pl.ds(plan.where[n], DOF)
        zero = jnp.zeros((epd, LANES - 2 * DOF), F32)
        return jnp.concatenate([ybuf[:, cut], ubuf[:, cut], zero], axis=1)

    ends = [packed_state(n) for n in range(slices)]
    sweep(ends, 0)
    await_blocks(first_whole, 1)
    eye = jnp.where(
        lax.broadcasted_iota(jnp.int32, (DEPTH, LANES), 0) == lane_of, 1.0, 0.0
    )
    maps = {t: jnp.where(t < block_t, unfold_map(brx[t], lane_of), eye) for t in range(1, blocks - 1)}
    pieces = {(t, t): maps[t] for t in maps}

    def join(a, b, c):
        if (a, c) not in pieces:
            slot = weights.setdefault((b, c), len(weights))
            if slot == len(weights) - 1:
                put(bmap, slot, pieces[b, c])
            pieces[a, c] = through(pieces[a, b - 1], bmap[slot])

    weights = {}
    top = blocks - 2
    span = 1
    while span < blocks:
        for last in range(top, 0, -2 * span):
            mid = last - span + 1
            if mid <= 1:
                continue
            for first in range(max(1, mid - span), mid):
                join(first, mid, last)
        span *= 2
    for t in range(blocks - 2):
        if (t + 1, top) not in weights:
            weights[t + 1, top] = len(weights)
            put(bmap, weights[t + 1, top], pieces[t + 1, top])

    def enter(k):
        total = jnp.where(blocks - 2 < block_t, srx[k, blocks - 2], 0.0)
        for t in range(blocks - 2):
            total = total + through(jnp.where(t < block_t, srx[k, t], 0.0), bmap[weights[t + 1, top]])
        return total

    await_blocks(functools.partial(sweep_whole, 0))
    entry = enter(0)
    xs[0] = jnp.where(block_t == 0, start_state, entry)
    for n in range(slices):
        xs[n + 1] = ends_buf[n] + through(entry, qmap[n])

    def iteration(k, corrections):
        for n in range(slices):
            cut = pl.ds(plan.where[n], DOF)
            ybuf[:, cut] = xs[n, :, 0:DOF]
            ubuf[:, cut] = xs[n, :, DOF : 2 * DOF]
        for j in range(HS):

            def substep(counter, carry):
                result = []
                for g, (base, members, a) in enumerate(plan.groups):
                    y, u = carry[g]
                    cut = pl.ds(base, LANES)
                    t = y - jnp.round(y)
                    s = t * t
                    s2 = s * s
                    poly = ((SIN[0] + SIN[1] * s) + s2 * (SIN[2] + SIN[3] * s)) + (s2 * s2) * (SIN[4] + SIN[5] * s)
                    force = (
                        tq[j, :, cut]
                        - spring[j, :, cut] * y
                        - fric[j, :, cut] * u
                        - (grav[:, cut] * t) * poly
                    )
                    change = product(force, g)
                    result.append(((y + u) + change, u + change))
                return tuple(result)

            first_state = tuple(
                (ybuf[:, pl.ds(base, LANES)], ubuf[:, pl.ds(base, LANES)])
                for base, members, a in plan.groups
            )
            last = lax.fori_loop(0, SUB, substep, first_state, unroll=UNROLL)
            for g, (base, members, a) in enumerate(plan.groups):
                ybuf[:, pl.ds(base, LANES)] = last[g][0]
                ubuf[:, pl.ds(base, LANES)] = last[g][1]

        ends = [packed_state(n) - xs[n + 1] for n in range(slices)]
        sweep(ends, k + 1)
        await_blocks(functools.partial(sweep_whole, k + 1))
        entry = enter(k + 1)
        xs[0] = xs[0] + entry
        worst = jnp.zeros((epd, 1), F32)
        for n in range(slices):
            change = ends_buf[n] + through(entry, qmap[n])
            real = change * scale
            worst = jnp.maximum(worst, jnp.sum(real * real, axis=1, keepdims=True))
            xs[n + 1] = xs[n + 1] + change
        return jnp.where(lane_of == k, jnp.sqrt(worst), corrections)

    corrections = lax.fori_loop(0, ITERS, iteration, jnp.zeros((epd, LANES), F32))

    turned = pad_rows(corrections, LANES).T
    row = turned[0:1]
    for k in range(1, ITERS):
        row = jnp.where(lane_group == k, pltpu.roll(turned[k : k + 1], k * epd, 1), row)
    ctx[...] = row
    for i in range(nz):
        parts = []
        for a in range(HS):
            real = xs[HS * i + a + 1] * scale
            parts.append(real)
            parts.append(pltpu.roll(real, LANES - DOF, 1))
        otx[i] = jnp.concatenate(parts, axis=0).T[0:ROWS_OUT, :]

    def out_copy(i):
        return pltpu.make_async_remote_copy(
            src_ref=otx.at[i],
            dst_ref=orx.at[z],
            send_sem=osend.at[0],
            recv_sem=orecv.at[z],
            device_id={"tm": source_index(i), "env": me_e},
            device_id_type=MESH,
        )

    def out_arrival(k):
        return pltpu.make_async_remote_copy(
            src_ref=otx.at[0],
            dst_ref=orx.at[lax.rem(z + k, nz)],
            send_sem=osend.at[0],
            recv_sem=orecv.at[lax.rem(z + k, nz)],
            device_id={"tm": dest_index(k), "env": me_e},
            device_id_type=MESH,
        )

    def corr_copy(k):
        return pltpu.make_async_remote_copy(
            src_ref=ctx,
            dst_ref=crx.at[k],
            send_sem=csend.at[0],
            recv_sem=crecv.at[0],
            device_id={"tm": lax.rem(me_t + k, tm), "env": me_e},
            device_id_type=MESH,
        )

    @pl.loop(1, tm, unroll=True)
    def _(k):
        corr_copy(k).start()

    @pl.loop(0, nz)
    def _(i):
        @pl.when(other_source(i))
        def _():
            out_copy(i).start()

    crx[0] = ctx[...]

    @pl.when(own_here)
    def _():
        orx[z] = otx[my_source]

    @pl.loop(0, nz)
    def _(k):
        @pl.when(other(k))
        def _():
            out_arrival(k).wait_recv()

    for h in range(tiles):
        for k in range(2 * HS):
            a, half_state = divmod(k, 2)
            tile = None
            for q in range(per_tile):
                r = (q - k) % per_tile
                v = orx[h * per_tile + q]
                v = v if r == 0 else pltpu.roll(v, r * epd, 1)
                tile = v if tile is None else jnp.where(lane_group == q, v, tile)
            out[half_state * DOF : half_state * DOF + DOF, a, h * LANES : (h + 1) * LANES] = tile[0:DOF]

    pltpu.make_async_remote_copy(
        src_ref=crx.at[pl.ds(1, tm - 1)],
        dst_ref=crx.at[pl.ds(1, tm - 1)],
        send_sem=csend.at[0],
        recv_sem=crecv.at[0],
        device_id={"tm": lax.rem(me_t + 1, tm), "env": me_e},
        device_id_type=MESH,
    ).wait()
    worst = []
    for p in range(nz):
        most = None
        for t in range(blocks):
            sender = t // CORES * line + p * CORES + t % CORES
            value = crx[lax.rem(me_t - sender + tm, tm)]
            most = value if most is None else jnp.maximum(most, value)
        worst.append(most)
    for h in range(tiles):
        for k in range(ITERS):
            tile = None
            for q in range(per_tile):
                r = (q - k) % per_tile
                v = worst[h * per_tile + q]
                v = v if r == 0 else pltpu.roll(v, r * epd, 1)
                tile = v if tile is None else jnp.where(lane_group == q, v, tile)
            corr_out[k : k + 1, h * LANES : (h + 1) * LANES] = tile

    def drain(ref, sem, count):
        whole_copy(ref.at[pl.ds(0, count)], sem.at[0], sem.at[0]).wait_send()

    for ref, sem in ((mrx, msend), (tx, tsend), (otx, osend)):
        @pl.when(own_here)
        def _(ref=ref, sem=sem):
            drain(ref, sem, nz - 1)

        @pl.when(jnp.logical_not(own_here))
        def _(ref=ref, sem=sem):
            drain(ref, sem, nz)

    if ny > 1:
        rows_all().wait_send()

    @pl.when(block_t > 0)
    def _():
        drain_blocks(first_whole)

    for k in range(ITERS + 1):
        drain_blocks(functools.partial(sweep_whole, k))


def body(tm, env, init_state, torque, contact, mass_inverse, stiffness, damping, gravity,
         contact_stiffness, contact_damping):
    nz = NZ
    env_local = init_state.shape[1]
    epd = env_local // nz
    slices = HS * nz
    blocks = tm // (nz * CORES) * CORES
    plan = Plan(nz)
    groups = len(plan.groups)
    lanes = plan.lanes
    vm = pltpu.VMEM
    dma = pltpu.SemaphoreType.DMA
    vmem = pl.BlockSpec(memory_space=pltpu.VMEM)
    both = vm((HS, epd, lanes), F32)
    thin = vm((HS, 1, lanes), F32)
    levels = slices.bit_length() - 1
    prm = [p.reshape(1, DOF) for p in (stiffness, damping, gravity, contact_stiffness, contact_damping)]
    states, corrections = pl.pallas_call(
        functools.partial(kernel, tm, env),
        out_shape=(
            vm((STATE, HS, env_local), F32),
            vm((ITERS, env_local), F32),
        ),
        in_specs=[pl.BlockSpec(memory_space=pl.ANY)] * 9,
        out_specs=(vmem, vmem),
        scratch_shapes=[
            vm(init_state.shape, F32), vm((DOF, 2 * HS, env_local), F32), vm(contact.shape, jnp.int32),
            vm((DOF, HS, DOF), F32), *[vm((1, DOF), F32)] * 5,
            vm((nz, ROWS_IN, LANES), F32), vm((nz, ROWS_IN, LANES), F32),
            vm((ROWS_MAT, LANES), F32), vm((nz, ROWS_MAT, LANES), F32),
            vm((1, LANES), F32), vm((env, nz, 1, LANES), F32),
            vm((2 * HS, 40, env_local), F32), vm((env_local, LANES), F32),
            *[vm((-(-nz // plan.per), LANES, LANES), F32)] * 2, vm((5, 1, lanes), F32),
            both, both, both, vm((1, lanes), F32), thin, thin,
            vm((groups, WIDE, WIDE), BF16), vm((groups, LANES, LANES), F32), vm((LANES, LANES), F32),
            vm((epd, lanes), F32), vm((epd, lanes), F32),
            vm((DEPTH, lanes), F32), vm((DEPTH, lanes), F32),
            vm((levels * slices // 2, WIDE, WIDE), BF16),
            vm((slices, WIDE, WIDE), BF16), vm((2 * blocks, WIDE, WIDE), BF16),
            vm((DEPTH, LANES), F32),
            vm((slices + 1, epd, LANES), F32), vm((slices, epd, LANES), F32),
            vm((ROWS_MAP, LANES), F32), vm((blocks, ROWS_MAP, LANES), F32),
            vm((ITERS + 1, epd, LANES), F32), vm((ITERS + 1, blocks, epd, LANES), F32),
            vm((nz, ROWS_OUT, LANES), F32), vm((nz, ROWS_OUT, LANES), F32),
            vm((1, LANES), F32), vm((tm, 1, LANES), F32),
            dma((9,)), dma((1,)), dma((nz,)), dma((1,)), dma((nz,)), dma((1,)), dma((1,)),
            dma((1,)), dma((1,)), dma((ITERS + 1,)), dma((ITERS + 1,)),
            dma((1,)), dma((nz,)), dma((1,)), dma((1,)),
        ],
        compiler_params=pltpu.CompilerParams(collective_id=0, has_side_effects=True),
        name="parareal",
    )(
        init_state, torque.transpose(1, 0, 2), contact, mass_inverse.transpose(1, 0, 2), *prm
    )
    return states.transpose(1, 0, 2), corrections


def solution(mesh):
    placed = (
        P(None, "env"),
        P("tm", None, "env"),
        P("tm", "env"),
        P("tm", None, None),
        P(),
        P(),
        P(),
        P(),
        P(),
    )
    return jax.shard_map(
        functools.partial(body, mesh.shape["tm"], mesh.shape["env"]),
        mesh=mesh,
        in_specs=placed,
        out_specs=(P("tm", None, "env"), P(None, "env")),
        check_vma=False,
    )
```

```python
import functools
import math

import jax
import jax.numpy as jnp
from jax import lax
from jax.experimental import pallas as pl
from jax.experimental.pallas import tpu as pltpu
from jax.sharding import PartitionSpec as P

DOF = 35
STATE = 70
HS = 2
SUB = 32
ITERS = 3
LANES = 128
WIDE = 256
NZ = 8
CORES = 2
UNROLL = 32

step_length = 0.05
fine_dt = step_length / SUB
TWO_PI = 2.0 * math.pi
MESH = pl.DeviceIdType.MESH
F32 = jnp.float32
BF16 = jnp.bfloat16

SIN = (
    6.283182818551188, -41.341421398631915, 81.59618387021051,
    -76.58010048603072, 41.205394649903326, -12.271261959178284,
)

ROWS_IN = 40
ROWS_MAT = 16
FOLD = 36
ROWS_OUT = 40
DEPTH = 72
ROWS_MAP = 48


def split(value):
    high = value.astype(BF16)
    return high, (value - high.astype(F32)).astype(BF16)


def dot(left, right):
    return jnp.dot(left, right, preferred_element_type=F32)


def through(state, weight):
    high, low = split(state)
    both = dot(jnp.concatenate([high, low], axis=1), weight)
    return both[:, :LANES] + both[:, LANES:]


def clear(ref):
    ref[...] = jnp.zeros(ref.shape, ref.dtype)


def put(ref, n, value):
    high, low = split(value)
    rows = value.shape[0]
    ref[n, 0:rows, 0:LANES] = high
    ref[n, LANES : LANES + rows, 0:LANES] = high
    ref[n, 0:rows, LANES:] = low


def pad_rows(value, rows):
    return jnp.concatenate([value, jnp.zeros((rows - value.shape[0], value.shape[1]), F32)], axis=0)


def fold_map(value, lane_of):
    value = jnp.where(lane_of < DOF, value, 0.0), jnp.where(lane_of < DOF, pltpu.roll(value, LANES - DOF, 1), 0.0)
    tall = jnp.concatenate(value, axis=0)
    first, second, third = (tall[r : r + ROWS_MAP] for r in range(0, 2 * DEPTH, ROWS_MAP))
    return first + pltpu.roll(second, DOF, 1) + pltpu.roll(third, 2 * DOF, 1)


def unfold_map(value, lane_of):
    tall = jnp.concatenate(
        [value, pltpu.roll(value, LANES - DOF, 1), pltpu.roll(value, LANES - 2 * DOF, 1)], axis=0
    )
    right = jnp.where(lane_of < 2 * DOF, pltpu.roll(tall[DEPTH:], DOF, 1), 0.0)
    return jnp.where(lane_of < DOF, tall[0:DEPTH], right)


class Plan:
    def __init__(self, sources):
        self.per = LANES // DOF
        self.groups = []
        self.slot = {}
        for first in range(0, sources, self.per):
            members = range(first, min(first + self.per, sources))
            for a in range(HS):
                for pos, i in enumerate(members):
                    self.slot[HS * i + a] = (len(self.groups), pos)
                self.groups.append((len(self.groups) * LANES, members, a))
        self.where = [self.slot[n][0] * LANES + self.slot[n][1] * DOF for n in range(HS * sources)]
        self.lanes = len(self.groups) * LANES


def kernel(
    tm, ny,
    init_hbm, torque_hbm, contact_hbm, minv_hbm, stiff_hbm, damp_hbm, gravity_hbm, cstiff_hbm, cdamp_hbm,
    out, corr_out,
    init, torque, contact, minv, stiff, damp, gravity, cstiff, cdamp,
    tx, rx, mtx, mrx, rowtx, rows, raw, inits,
    tstage, hstage, gains, tq, spring, fric, grav, cspring, cfric, wgt, stage, wtmp, ybuf, ubuf, ly, lu,
    cmap, qmap, bmap, ctmp, xs, ends_buf, changes,
    btx, brx, stx, srx, otx, orx, ctx, crx,
    lsem, tsend, trecv, msend, mrecv, rsend, rrecv, bsend, brecv, ssend, srecv, osend, orecv, csend, crecv,
):
    pairs = (
        (torque_hbm, torque), (contact_hbm, contact), (minv_hbm, minv), (init_hbm, init), (stiff_hbm, stiff),
        (damp_hbm, damp), (gravity_hbm, gravity), (cstiff_hbm, cstiff), (cdamp_hbm, cdamp),
    )
    local = [pltpu.make_async_copy(src, dst, lsem.at[i]) for i, (src, dst) in enumerate(pairs)]
    nz = NZ
    half = nz // 2
    line = nz * CORES
    blocks = tm // line * CORES
    env_local = init.shape[1]
    epd = env_local // nz
    slices = HS * nz
    per_tile = LANES // epd
    tiles = env_local // LANES
    plan = Plan(nz)
    me_t = lax.axis_index("tm")
    me_e = lax.axis_index("env")
    x = me_t // line
    z = lax.rem(me_t // CORES, nz)
    c = lax.rem(me_t, CORES)
    block_t = x * CORES + c
    dest_core = z // half
    my_source = lax.rem(z, half) * CORES + c
    own_here = dest_core == c
    barrier = pltpu.get_barrier_semaphore()

    def source_index(i):
        return x * line + (c * half + i // CORES) * CORES + lax.rem(i, CORES)

    def dest_index(k):
        return x * line + lax.rem(z + k, nz) * CORES + dest_core

    def block_index(t):
        return t // CORES * line + z * CORES + lax.rem(t, CORES)

    @pl.loop(1, tm, unroll=True)
    def _(k):
        pl.semaphore_signal(
            barrier, inc=1, device_id={"tm": lax.rem(me_t + k, tm), "env": me_e}, device_id_type=MESH
        )

    for copy in local:
        copy.start()

    @pl.loop(1, ny)
    def _(r):
        @pl.loop(0, nz, unroll=True)
        def _(i):
            pl.semaphore_signal(
                barrier, inc=1,
                device_id={"tm": source_index(i), "env": lax.rem(me_e + r, ny)},
                device_id_type=MESH,
            )

    for copy in local:
        copy.wait()
    lane_of = lax.broadcasted_iota(jnp.int32, (1, LANES), 1)
    lane_group = lane_of // epd

    raw[...] = jnp.zeros(raw.shape, F32)
    hits = contact[...].astype(F32)
    for k in range(2 * HS):
        raw[k, 0:DOF, :] = torque[:, k, :]
        raw[k, DOF : DOF + 1, :] = hits[k : k + 1, :]
    wtmp[...] = jnp.zeros(wtmp.shape, F32)
    wtmp[0:DOF, 0:DOF] = minv[:, 0, :]
    wtmp[40 : 40 + DOF, 0:DOF] = minv[:, 1, :]
    row_of = lax.broadcasted_iota(jnp.int32, (40, LANES), 0)
    lower = lane_of <= row_of
    packed = jnp.where(lower, wtmp[0:40, :], pltpu.roll(wtmp[40:80, :], 1, 1))
    last = jnp.concatenate([packed[32:40], jnp.zeros((8, LANES), F32)], axis=0)
    mtx[...] = packed[0:16] + pltpu.roll(packed[16:32], FOLD, 1) + pltpu.roll(last, 2 * FOLD, 1)
    for h in range(tiles):
        rolled = {}
        for k in range(2 * HS):
            v = raw[k, :, h * LANES : (h + 1) * LANES]
            for r in range(per_tile):
                rolled[k, r] = v if r == 0 else pltpu.roll(v, r * epd, 1)
        for q in range(per_tile):
            acc = rolled[0, (0 - q) % per_tile]
            for k in range(1, 2 * HS):
                acc = jnp.where(lane_group == k, rolled[k, (k - q) % per_tile], acc)
            tx[h * per_tile + q] = acc
    totals = jnp.sum(hits, axis=1, keepdims=True)
    row = jnp.zeros((1, LANES), F32)
    for k in range(2 * HS):
        row = jnp.where(lane_of == 3 * FOLD + k, jnp.broadcast_to(totals[k : k + 1], (1, LANES)), row)
    rowtx[...] = row
    mtx[0:1, :] = mtx[0:1, :] + row

    pl.semaphore_wait(barrier, tm - 1 + (ny - 1) * nz)

    def in_copy(k):
        return pltpu.make_async_remote_copy(
            src_ref=tx.at[lax.rem(z + k, nz)],
            dst_ref=rx.at[my_source],
            send_sem=tsend.at[0],
            recv_sem=trecv.at[my_source],
            device_id={"tm": dest_index(k), "env": me_e},
            device_id_type=MESH,
        )

    def in_arrival(i):
        return pltpu.make_async_remote_copy(
            src_ref=tx.at[0],
            dst_ref=rx.at[i],
            send_sem=tsend.at[0],
            recv_sem=trecv.at[i],
            device_id={"tm": dest_index(0), "env": me_e},
            device_id_type=MESH,
        )

    def mat_copy(k):
        return pltpu.make_async_remote_copy(
            src_ref=mtx,
            dst_ref=mrx.at[my_source],
            send_sem=msend.at[0],
            recv_sem=mrecv.at[my_source],
            device_id={"tm": dest_index(k), "env": me_e},
            device_id_type=MESH,
        )

    def mat_arrival(i):
        return pltpu.make_async_remote_copy(
            src_ref=mtx,
            dst_ref=mrx.at[i],
            send_sem=msend.at[0],
            recv_sem=mrecv.at[i],
            device_id={"tm": dest_index(0), "env": me_e},
            device_id_type=MESH,
        )

    def row_copy(k, r):
        return pltpu.make_async_remote_copy(
            src_ref=rowtx,
            dst_ref=rows.at[r, my_source],
            send_sem=rsend.at[0],
            recv_sem=rrecv.at[0],
            device_id={"tm": dest_index(k), "env": lax.rem(me_e + r, ny)},
            device_id_type=MESH,
        )

    def rows_all():
        return pltpu.make_async_remote_copy(
            src_ref=rows.at[pl.ds(1, ny - 1)],
            dst_ref=rows.at[pl.ds(1, ny - 1)],
            send_sem=rsend.at[0],
            recv_sem=rrecv.at[0],
            device_id={"tm": dest_index(0), "env": lax.rem(me_e + 1, ny)},
            device_id_type=MESH,
        )

    def other(k):
        return jnp.logical_not(jnp.logical_and(own_here, k == 0))

    def other_source(i):
        return jnp.logical_not(jnp.logical_and(own_here, i == my_source))

    for r in range(1, ny):
        for k in range(nz):
            row_copy(k, r).start()
    far_first = sorted(range(nz), key=lambda k: -min(k, nz - k))
    for make in (mat_copy, in_copy):
        for k in far_first:
            @pl.when(other(k))
            def _(k=k, make=make):
                make(k).start()

    @pl.when(own_here)
    def _():
        rx[my_source] = tx[z]
        mrx[my_source] = mtx[...]

    ratio = float(SUB)
    stiff, damp, gravity, cstiff, cdamp = (r[...] for r in (stiff, damp, gravity, cstiff, cdamp))
    to_u = TWO_PI / fine_dt
    scale = jnp.where(lane_of < DOF, TWO_PI, to_u)
    shrink = jnp.where(lane_of < DOF, 1.0 / TWO_PI, 1.0 / to_u)

    for ref in (changes, tstage, hstage, gains, tq, spring, fric, grav, cspring, cfric, ybuf, ubuf, ly, lu, ctmp, stage, wgt, cmap, qmap, bmap):
        clear(ref)
    for h in range(tiles):
        inits[h * LANES : (h + 1) * LANES, :] = (
            pad_rows(init[:, h * LANES : (h + 1) * LANES], LANES).T * shrink
        )
    start_state = inits[pl.ds(pl.multiple_of(z * epd, epd), epd), :]
    first_start = jnp.where(block_t == 0, start_state, 0.0)
    rank = lax.broadcasted_iota(jnp.int32, (DEPTH, DOF), 0)
    col = lax.broadcasted_iota(jnp.int32, (DEPTH, DOF), 1)
    for n in range(slices):
        cut = pl.ds(plan.where[n], DOF)
        ly[:, cut] = jnp.where(rank == col, 1.0, 0.0)
        lu[:, cut] = jnp.where(rank == col + DOF, 1.0, 0.0)
        grav[:, cut] = gravity
        gains[0, :, cut] = TWO_PI * stiff
        gains[1, :, cut] = TWO_PI * cstiff
        gains[2, :, cut] = to_u * damp
        gains[3, :, cut] = to_u * cdamp
        gains[4, :, cut] = TWO_PI * gravity
    ybuf[:, 0:DOF] = first_start[:, 0:DOF]
    ubuf[:, 0:DOF] = first_start[:, DOF : 2 * DOF]

    square_row = lax.broadcasted_iota(jnp.int32, (40, LANES), 0)
    for i in range(nz):
        @pl.when(other_source(i))
        def _(i=i):
            mat_arrival(i).wait_recv()

        folded = mrx[i]
        square = jnp.concatenate(
            [folded, pltpu.roll(folded, LANES - FOLD, 1), pltpu.roll(folded[0:8], LANES - 2 * FOLD, 1)], axis=0
        )
        shifted = pltpu.roll(square, LANES - 1, 1)
        turned = pad_rows(jnp.concatenate([square, shifted], axis=0), LANES).T
        matrices = (
            jnp.where(lane_of <= square_row, square, turned[0:40]),
            jnp.where(lane_of >= square_row, shifted, pltpu.roll(turned[0:40], LANES - 40, 1)),
        )
        for a in range(HS):
            n = HS * i + a
            cut = pl.ds(plan.where[n], DOF)
            g, pos = plan.slot[n]
            stage[g, pl.ds(pos * DOF, DOF), pl.ds(pos * DOF, DOF)] = (
                fine_dt * fine_dt / TWO_PI
            ) * matrices[a][0:DOF, 0:DOF]
    for g, (base, members, a) in enumerate(plan.groups):
        put(wgt, g, stage[g])

    def product(force, g):
        return through(force, wgt[g])

    if ny > 1:
        rows_all().wait_recv()
    counts = []
    for i in range(nz):
        total = mrx[i, 0:1, :]
        for r in range(1, ny):
            total = total + rows[r, i]
        counts.append(total * (1.0 / (env_local * ny)))
    for base, members, a in plan.groups:
        cut = pl.ds(base, LANES)
        for j in range(HS):
            spot = 3 * FOLD + a * HS + j
            mean = counts[members[0]][:, spot : spot + 1]
            for pos, i in enumerate(members):
                mean = jnp.where(lane_of >= pos * DOF, counts[i][:, spot : spot + 1], mean)
            cspring[j, :, cut] = gains[0, :, cut] + gains[4, :, cut] + mean * gains[1, :, cut]
            cfric[j, :, cut] = gains[2, :, cut] + mean * gains[3, :, cut]

    for g, (base, members, a) in enumerate(plan.groups):
        cut = pl.ds(base, LANES)
        y, u = ly[:, cut], lu[:, cut]
        for j in range(HS):
            force = -cspring[j, :, cut] * y - cfric[j, :, cut] * u
            u = u + ratio * product(force, g)
            y = y + ratio * u
        ly[:, cut] = y
        lu[:, cut] = u
    levels = slices.bit_length() - 1
    stacks = []
    for n in range(slices):
        cut = pl.ds(plan.where[n], DOF)
        ctmp[:, 0:DOF] = ly[:, cut]
        ctmp[:, DOF : 2 * DOF] = lu[:, cut]
        stacks.append(ctmp[...])

    def right_half(level):
        step = 1 << level
        found = []
        for m in range(0, slices, 2 * step):
            for i in range(step):
                found.append((level * (slices // 2) + len(found), m + step - 1, m + step + i))
        return found

    def steps(spine):
        return [
            [entry for entry in right_half(level) if ((entry[2] + 1) % (2 << level) == 0) == spine]
            for level in range(levels)
        ]


    for level in range(levels):
        for place, left, n in right_half(level):
            put(cmap, place, stacks[n])
        for place, left, n in right_half(level):
            stacks[n] = through(stacks[left], cmap[place])
    btx[...] = fold_map(stacks[slices - 1], lane_of)
    for n in range(slices):
        put(qmap, n, stacks[n])

    def sweep(ends, k):
        def advance(spine):
            for entries in steps(spine):
                for place, left, n in entries:
                    ends[n] = ends[n] + through(ends[left], cmap[place])

        advance(True)
        stx[k] = ends[slices - 1]
        send_blocks(functools.partial(sweep_copy, k))
        advance(False)
        for n in range(slices):
            ends_buf[n] = ends[n]

    def first_copy(d):
        return pltpu.make_async_remote_copy(
            src_ref=btx,
            dst_ref=brx.at[block_t],
            send_sem=bsend.at[0],
            recv_sem=brecv.at[0],
            device_id={"tm": block_index(block_t + d), "env": me_e},
            device_id_type=MESH,
        )

    def sweep_copy(k, d):
        return pltpu.make_async_remote_copy(
            src_ref=stx.at[k],
            dst_ref=srx.at[k, block_t],
            send_sem=ssend.at[k],
            recv_sem=srecv.at[k],
            device_id={"tm": block_index(block_t + d), "env": me_e},
            device_id_type=MESH,
        )

    def whole_copy(ref, send, recv):
        return pltpu.make_async_remote_copy(
            src_ref=ref, dst_ref=ref, send_sem=send, recv_sem=recv,
            device_id={"tm": block_index(lax.rem(block_t + 1, blocks)), "env": me_e},
            device_id_type=MESH,
        )

    def first_whole(count):
        return whole_copy(brx.at[pl.ds(0, count)], bsend.at[0], brecv.at[0])

    def sweep_whole(k, count):
        return whole_copy(srx.at[k, pl.ds(0, count)], ssend.at[k], srecv.at[k])

    def send_blocks(copy):
        for d in range(1, blocks):
            @pl.when(block_t + d < blocks)
            def _(d=d):
                copy(d).start()

    def await_blocks(whole, skip=0):
        for count in range(1, blocks - skip):
            @pl.when(block_t - skip == count)
            def _(count=count):
                whole(count).wait_recv()

    def drain_blocks(whole):
        for count in range(1, blocks):
            @pl.when(blocks - 1 - block_t == count)
            def _(count=count):
                whole(count).wait_send()

    @pl.when(block_t > 0)
    def _():
        send_blocks(first_copy)

    for part in range(0, nz, plan.per):
        for pos, i in enumerate(range(part, min(part + plan.per, nz))):
            @pl.when(other_source(i))
            def _(i=i):
                in_arrival(i).wait_recv()

            tstage[part // plan.per, pos * DOF : (pos + 1) * DOF, :] = rx[i, 0:DOF, :]
            hstage[part // plan.per, pos * DOF : (pos + 1) * DOF, :] = jnp.broadcast_to(
                rx[i, DOF : DOF + 1, :], (DOF, LANES)
            )
        turned = tstage[part // plan.per].T
        touched = hstage[part // plan.per].T
        for a in range(HS):
            base = (part // plan.per * HS + a) * LANES
            cut = pl.ds(base, LANES)
            for j in range(HS):
                k = a * HS + j
                hit = touched[k * epd : (k + 1) * epd, :]
                tq[j, :, cut] = turned[k * epd : (k + 1) * epd, :]
                spring[j, :, cut] = gains[0, :, cut] + hit * gains[1, :, cut]
                fric[j, :, cut] = gains[2, :, cut] + hit * gains[3, :, cut]

    for g, (base, members, a) in enumerate(plan.groups):
        cut = pl.ds(base, LANES)
        y, u = ybuf[:, cut], ubuf[:, cut]
        for j in range(HS):
            force = tq[j, :, cut] - cspring[j, :, cut] * y - cfric[j, :, cut] * u
            u = u + ratio * product(force, g)
            y = y + ratio * u
        ybuf[:, cut] = y
        ubuf[:, cut] = u

    def packed_state(n):
        cut = pl.ds(plan.where[n], DOF)
        zero = jnp.zeros((epd, LANES - 2 * DOF), F32)
        return jnp.concatenate([ybuf[:, cut], ubuf[:, cut], zero], axis=1)

    ends = [packed_state(n) for n in range(slices)]
    sweep(ends, 0)
    await_blocks(first_whole, 1)
    eye = jnp.where(
        lax.broadcasted_iota(jnp.int32, (DEPTH, LANES), 0) == lane_of, 1.0, 0.0
    )
    maps = {t: jnp.where(t < block_t, unfold_map(brx[t], lane_of), eye) for t in range(1, blocks - 1)}
    pieces = {(t, t): maps[t] for t in maps}

    def join(a, b, c):
        if (a, c) not in pieces:
            slot = weights.setdefault((b, c), len(weights))
            if slot == len(weights) - 1:
                put(bmap, slot, pieces[b, c])
            pieces[a, c] = through(pieces[a, b - 1], bmap[slot])

    weights = {}
    top = blocks - 2
    span = 1
    while span < blocks:
        for last in range(top, 0, -2 * span):
            mid = last - span + 1
            if mid <= 1:
                continue
            for first in range(max(1, mid - span), mid):
                join(first, mid, last)
        span *= 2
    for t in range(blocks - 2):
        if (t + 1, top) not in weights:
            weights[t + 1, top] = len(weights)
            put(bmap, weights[t + 1, top], pieces[t + 1, top])

    def enter(k):
        total = jnp.where(blocks - 2 < block_t, srx[k, blocks - 2], 0.0)
        for t in range(blocks - 2):
            total = total + through(jnp.where(t < block_t, srx[k, t], 0.0), bmap[weights[t + 1, top]])
        return total

    await_blocks(functools.partial(sweep_whole, 0))
    entry = enter(0)
    xs[0] = jnp.where(block_t == 0, start_state, entry)
    for n in range(slices):
        xs[n + 1] = ends_buf[n] + through(entry, qmap[n])

    def largest(k, corrections):
        worst = jnp.zeros((epd, 1), F32)
        for n in range(slices):
            real = changes[n] * scale
            worst = jnp.maximum(worst, jnp.sum(real * real, axis=1, keepdims=True))
        return jnp.where(lane_of == k, jnp.sqrt(worst), corrections)

    def iteration(k, corrections):
        for n in range(slices):
            cut = pl.ds(plan.where[n], DOF)
            ybuf[:, cut] = xs[n, :, 0:DOF]
            ubuf[:, cut] = xs[n, :, DOF : 2 * DOF]
        for j in range(HS):

            def substep(counter, carry):
                result = []
                for g, (base, members, a) in enumerate(plan.groups):
                    y, u = carry[g]
                    cut = pl.ds(base, LANES)
                    t = y - jnp.round(y)
                    s = t * t
                    s2 = s * s
                    poly = ((SIN[0] + SIN[1] * s) + s2 * (SIN[2] + SIN[3] * s)) + (s2 * s2) * (SIN[4] + SIN[5] * s)
                    force = (
                        tq[j, :, cut]
                        - spring[j, :, cut] * y
                        - fric[j, :, cut] * u
                        - (grav[:, cut] * t) * poly
                    )
                    change = product(force, g)
                    result.append(((y + u) + change, u + change))
                return tuple(result)

            first_state = tuple(
                (ybuf[:, pl.ds(base, LANES)], ubuf[:, pl.ds(base, LANES)])
                for base, members, a in plan.groups
            )
            last = lax.fori_loop(0, SUB, substep, first_state, unroll=UNROLL)
            for g, (base, members, a) in enumerate(plan.groups):
                ybuf[:, pl.ds(base, LANES)] = last[g][0]
                ubuf[:, pl.ds(base, LANES)] = last[g][1]

        ends = [packed_state(n) - xs[n + 1] for n in range(slices)]
        sweep(ends, k + 1)
        corrections = largest(k - 1, corrections)
        await_blocks(functools.partial(sweep_whole, k + 1))
        entry = enter(k + 1)
        xs[0] = xs[0] + entry
        for n in range(slices):
            change = ends_buf[n] + through(entry, qmap[n])
            changes[n] = change
            xs[n + 1] = xs[n + 1] + change
        return corrections

    corrections = lax.fori_loop(0, ITERS, iteration, jnp.zeros((epd, LANES), F32))
    corrections = largest(ITERS - 1, corrections)

    turned = pad_rows(corrections, LANES).T
    row = turned[0:1]
    for k in range(1, ITERS):
        row = jnp.where(lane_group == k, pltpu.roll(turned[k : k + 1], k * epd, 1), row)
    ctx[...] = row

    def corr_copy(k):
        return pltpu.make_async_remote_copy(
            src_ref=ctx,
            dst_ref=crx.at[k],
            send_sem=csend.at[0],
            recv_sem=crecv.at[0],
            device_id={"tm": lax.rem(me_t + k, tm), "env": me_e},
            device_id_type=MESH,
        )

    @pl.loop(1, tm, unroll=True)
    def _(k):
        corr_copy(k).start()

    for i in range(nz):
        parts = []
        for a in range(HS):
            real = xs[HS * i + a + 1] * scale
            parts.append(real)
            parts.append(pltpu.roll(real, LANES - DOF, 1))
        otx[i] = jnp.concatenate(parts, axis=0).T[0:ROWS_OUT, :]

    def out_copy(i):
        return pltpu.make_async_remote_copy(
            src_ref=otx.at[i],
            dst_ref=orx.at[z],
            send_sem=osend.at[0],
            recv_sem=orecv.at[z],
            device_id={"tm": source_index(i), "env": me_e},
            device_id_type=MESH,
        )

    def out_arrival(k):
        return pltpu.make_async_remote_copy(
            src_ref=otx.at[0],
            dst_ref=orx.at[lax.rem(z + k, nz)],
            send_sem=osend.at[0],
            recv_sem=orecv.at[lax.rem(z + k, nz)],
            device_id={"tm": dest_index(k), "env": me_e},
            device_id_type=MESH,
        )

    @pl.loop(0, nz)
    def _(i):
        @pl.when(other_source(i))
        def _():
            out_copy(i).start()

    crx[0] = ctx[...]

    @pl.when(own_here)
    def _():
        orx[z] = otx[my_source]

    @pl.loop(0, nz)
    def _(k):
        @pl.when(other(k))
        def _():
            out_arrival(k).wait_recv()

    for h in range(tiles):
        for k in range(2 * HS):
            a, half_state = divmod(k, 2)
            tile = None
            for q in range(per_tile):
                r = (q - k) % per_tile
                v = orx[h * per_tile + q]
                v = v if r == 0 else pltpu.roll(v, r * epd, 1)
                tile = v if tile is None else jnp.where(lane_group == q, v, tile)
            out[half_state * DOF : half_state * DOF + DOF, a, h * LANES : (h + 1) * LANES] = tile[0:DOF]

    pltpu.make_async_remote_copy(
        src_ref=crx.at[pl.ds(1, tm - 1)],
        dst_ref=crx.at[pl.ds(1, tm - 1)],
        send_sem=csend.at[0],
        recv_sem=crecv.at[0],
        device_id={"tm": lax.rem(me_t + 1, tm), "env": me_e},
        device_id_type=MESH,
    ).wait()
    worst = []
    for p in range(nz):
        most = None
        for t in range(blocks):
            sender = t // CORES * line + p * CORES + t % CORES
            value = crx[lax.rem(me_t - sender + tm, tm)]
            most = value if most is None else jnp.maximum(most, value)
        worst.append(most)
    for h in range(tiles):
        for k in range(ITERS):
            tile = None
            for q in range(per_tile):
                r = (q - k) % per_tile
                v = worst[h * per_tile + q]
                v = v if r == 0 else pltpu.roll(v, r * epd, 1)
                tile = v if tile is None else jnp.where(lane_group == q, v, tile)
            corr_out[k : k + 1, h * LANES : (h + 1) * LANES] = tile

    def drain(ref, sem, count):
        whole_copy(ref.at[pl.ds(0, count)], sem.at[0], sem.at[0]).wait_send()

    for ref, sem in ((mrx, msend), (tx, tsend), (otx, osend)):
        @pl.when(own_here)
        def _(ref=ref, sem=sem):
            drain(ref, sem, nz - 1)

        @pl.when(jnp.logical_not(own_here))
        def _(ref=ref, sem=sem):
            drain(ref, sem, nz)

    if ny > 1:
        rows_all().wait_send()

    @pl.when(block_t > 0)
    def _():
        drain_blocks(first_whole)

    for k in range(ITERS + 1):
        drain_blocks(functools.partial(sweep_whole, k))


def body(tm, env, init_state, torque, contact, mass_inverse, stiffness, damping, gravity,
         contact_stiffness, contact_damping):
    nz = NZ
    env_local = init_state.shape[1]
    epd = env_local // nz
    slices = HS * nz
    blocks = tm // (nz * CORES) * CORES
    plan = Plan(nz)
    groups = len(plan.groups)
    lanes = plan.lanes
    vm = pltpu.VMEM
    dma = pltpu.SemaphoreType.DMA
    vmem = pl.BlockSpec(memory_space=pltpu.VMEM)
    both = vm((HS, epd, lanes), F32)
    thin = vm((HS, 1, lanes), F32)
    levels = slices.bit_length() - 1
    prm = [p.reshape(1, DOF) for p in (stiffness, damping, gravity, contact_stiffness, contact_damping)]
    states, corrections = pl.pallas_call(
        functools.partial(kernel, tm, env),
        out_shape=(
            vm((STATE, HS, env_local), F32),
            vm((ITERS, env_local), F32),
        ),
        in_specs=[pl.BlockSpec(memory_space=pl.ANY)] * 9,
        out_specs=(vmem, vmem),
        scratch_shapes=[
            vm(init_state.shape, F32), vm((DOF, 2 * HS, env_local), F32), vm(contact.shape, jnp.int32),
            vm((DOF, HS, DOF), F32), *[vm((1, DOF), F32)] * 5,
            vm((nz, ROWS_IN, LANES), F32), vm((nz, ROWS_IN, LANES), F32),
            vm((ROWS_MAT, LANES), F32), vm((nz, ROWS_MAT, LANES), F32),
            vm((1, LANES), F32), vm((env, nz, 1, LANES), F32),
            vm((2 * HS, 40, env_local), F32), vm((env_local, LANES), F32),
            *[vm((-(-nz // plan.per), LANES, LANES), F32)] * 2, vm((5, 1, lanes), F32),
            both, both, both, vm((1, lanes), F32), thin, thin,
            vm((groups, WIDE, WIDE), BF16), vm((groups, LANES, LANES), F32), vm((LANES, LANES), F32),
            vm((epd, lanes), F32), vm((epd, lanes), F32),
            vm((DEPTH, lanes), F32), vm((DEPTH, lanes), F32),
            vm((levels * slices // 2, WIDE, WIDE), BF16),
            vm((slices, WIDE, WIDE), BF16), vm((2 * blocks, WIDE, WIDE), BF16),
            vm((DEPTH, LANES), F32),
            vm((slices + 1, epd, LANES), F32), vm((slices, epd, LANES), F32), vm((slices, epd, LANES), F32),
            vm((ROWS_MAP, LANES), F32), vm((blocks, ROWS_MAP, LANES), F32),
            vm((ITERS + 1, epd, LANES), F32), vm((ITERS + 1, blocks, epd, LANES), F32),
            vm((nz, ROWS_OUT, LANES), F32), vm((nz, ROWS_OUT, LANES), F32),
            vm((1, LANES), F32), vm((tm, 1, LANES), F32),
            dma((9,)), dma((1,)), dma((nz,)), dma((1,)), dma((nz,)), dma((1,)), dma((1,)),
            dma((1,)), dma((1,)), dma((ITERS + 1,)), dma((ITERS + 1,)),
            dma((1,)), dma((nz,)), dma((1,)), dma((1,)),
        ],
        compiler_params=pltpu.CompilerParams(collective_id=0, has_side_effects=True),
        name="parareal",
    )(
        init_state, torque.transpose(1, 0, 2), contact, mass_inverse.transpose(1, 0, 2), *prm
    )
    return states.transpose(1, 0, 2), corrections


def solution(mesh):
    placed = (
        P(None, "env"),
        P("tm", None, "env"),
        P("tm", "env"),
        P("tm", None, None),
        P(),
        P(),
        P(),
        P(),
        P(),
    )
    return jax.shard_map(
        functools.partial(body, mesh.shape["tm"], mesh.shape["env"]),
        mesh=mesh,
        in_specs=placed,
        out_specs=(P("tm", None, "env"), P(None, "env")),
        check_vma=False,
    )
```

```python
import functools
import math

import jax
import jax.numpy as jnp
from jax import lax
from jax.experimental import pallas as pl
from jax.experimental.pallas import tpu as pltpu
from jax.sharding import PartitionSpec as P

DOF = 35
STATE = 70
HS = 2
SUB = 32
ITERS = 3
LANES = 128
WIDE = 256
NZ = 8
CORES = 2
UNROLL = 32

step_length = 0.05
fine_dt = step_length / SUB
TWO_PI = 2.0 * math.pi
MESH = pl.DeviceIdType.MESH
F32 = jnp.float32
BF16 = jnp.bfloat16

SIN = (
    6.283182818551188, -41.341421398631915, 81.59618387021051,
    -76.58010048603072, 41.205394649903326, -12.271261959178284,
)

ROWS_IN = 40
ROWS_MAT = 16
FOLD = 36
ROWS_OUT = 40
DEPTH = 72
ROWS_MAP = 48


def split(value):
    high = value.astype(BF16)
    return high, (value - high.astype(F32)).astype(BF16)


def dot(left, right):
    return jnp.dot(left, right, preferred_element_type=F32)


def through(state, weight):
    high, low = split(state)
    both = dot(jnp.concatenate([high, low], axis=1), weight)
    return both[:, :LANES] + both[:, LANES:]


def clear(ref):
    ref[...] = jnp.zeros(ref.shape, ref.dtype)


def put(ref, n, value):
    high, low = split(value)
    rows = value.shape[0]
    ref[n, 0:rows, 0:LANES] = high
    ref[n, LANES : LANES + rows, 0:LANES] = high
    ref[n, 0:rows, LANES:] = low


def pad_rows(value, rows):
    return jnp.concatenate([value, jnp.zeros((rows - value.shape[0], value.shape[1]), F32)], axis=0)


def fold_map(value, lane_of):
    value = jnp.where(lane_of < DOF, value, 0.0), jnp.where(lane_of < DOF, pltpu.roll(value, LANES - DOF, 1), 0.0)
    tall = jnp.concatenate(value, axis=0)
    first, second, third = (tall[r : r + ROWS_MAP] for r in range(0, 2 * DEPTH, ROWS_MAP))
    return first + pltpu.roll(second, DOF, 1) + pltpu.roll(third, 2 * DOF, 1)


def unfold_map(value, lane_of):
    tall = jnp.concatenate(
        [value, pltpu.roll(value, LANES - DOF, 1), pltpu.roll(value, LANES - 2 * DOF, 1)], axis=0
    )
    right = jnp.where(lane_of < 2 * DOF, pltpu.roll(tall[DEPTH:], DOF, 1), 0.0)
    return jnp.where(lane_of < DOF, tall[0:DEPTH], right)


class Plan:
    def __init__(self, sources):
        self.per = LANES // DOF
        self.groups = []
        self.slot = {}
        for first in range(0, sources, self.per):
            members = range(first, min(first + self.per, sources))
            for a in range(HS):
                for pos, i in enumerate(members):
                    self.slot[HS * i + a] = (len(self.groups), pos)
                self.groups.append((len(self.groups) * LANES, members, a))
        self.where = [self.slot[n][0] * LANES + self.slot[n][1] * DOF for n in range(HS * sources)]
        self.lanes = len(self.groups) * LANES


def kernel(
    tm, ny,
    init_hbm, torque_hbm, contact_hbm, minv_hbm, stiff_hbm, damp_hbm, gravity_hbm, cstiff_hbm, cdamp_hbm,
    out, corr_out,
    init, torque, contact, minv, stiff, damp, gravity, cstiff, cdamp,
    tx, rx, mtx, mrx, rowtx, rows, raw, inits,
    tstage, hstage, gains, tq, spring, fric, grav, cspring, cfric, wgt, stage, wtmp, ybuf, ubuf, ly, lu,
    cmap, qmap, bmap, ctmp, xs, ends_buf, changes,
    btx, brx, stx, srx, otx, orx, ctx, crx,
    lsem, tsend, trecv, msend, mrecv, rsend, rrecv, bsend, brecv, ssend, srecv, osend, orecv, csend, crecv,
):
    pairs = (
        (torque_hbm, torque), (contact_hbm, contact), (minv_hbm, minv), (init_hbm, init), (stiff_hbm, stiff),
        (damp_hbm, damp), (gravity_hbm, gravity), (cstiff_hbm, cstiff), (cdamp_hbm, cdamp),
    )
    local = [pltpu.make_async_copy(src, dst, lsem.at[i]) for i, (src, dst) in enumerate(pairs)]
    nz = NZ
    half = nz // 2
    line = nz * CORES
    blocks = tm // line * CORES
    env_local = init.shape[1]
    epd = env_local // nz
    slices = HS * nz
    per_tile = LANES // epd
    tiles = env_local // LANES
    plan = Plan(nz)
    me_t = lax.axis_index("tm")
    me_e = lax.axis_index("env")
    x = me_t // line
    z = lax.rem(me_t // CORES, nz)
    c = lax.rem(me_t, CORES)
    block_t = x * CORES + c
    dest_core = z // half
    my_source = lax.rem(z, half) * CORES + c
    own_here = dest_core == c
    barrier = pltpu.get_barrier_semaphore()

    def source_index(i):
        return x * line + (c * half + i // CORES) * CORES + lax.rem(i, CORES)

    def dest_index(k):
        return x * line + lax.rem(z + k, nz) * CORES + dest_core

    def block_index(t):
        return t // CORES * line + z * CORES + lax.rem(t, CORES)

    for r in range(1, ny):
        @pl.loop(0, nz, unroll=True)
        def _(i, r=r):
            pl.semaphore_signal(
                barrier, inc=1,
                device_id={"tm": source_index(i), "env": lax.rem(me_e + r, ny)},
                device_id_type=MESH,
            )

    @pl.loop(1, tm, unroll=True)
    def _(k):
        pl.semaphore_signal(
            barrier, inc=1, device_id={"tm": lax.rem(me_t + k, tm), "env": me_e}, device_id_type=MESH
        )

    for copy in local:
        copy.start()

    for copy in local:
        copy.wait()
    lane_of = lax.broadcasted_iota(jnp.int32, (1, LANES), 1)
    lane_group = lane_of // epd

    raw[...] = jnp.zeros(raw.shape, F32)
    hits = contact[...].astype(F32)
    for k in range(2 * HS):
        raw[k, 0:DOF, :] = torque[:, k, :]
        raw[k, DOF : DOF + 1, :] = hits[k : k + 1, :]
    wtmp[...] = jnp.zeros(wtmp.shape, F32)
    wtmp[0:DOF, 0:DOF] = minv[:, 0, :]
    wtmp[40 : 40 + DOF, 0:DOF] = minv[:, 1, :]
    row_of = lax.broadcasted_iota(jnp.int32, (40, LANES), 0)
    lower = lane_of <= row_of
    packed = jnp.where(lower, wtmp[0:40, :], pltpu.roll(wtmp[40:80, :], 1, 1))
    last = jnp.concatenate([packed[32:40], jnp.zeros((8, LANES), F32)], axis=0)
    mtx[...] = packed[0:16] + pltpu.roll(packed[16:32], FOLD, 1) + pltpu.roll(last, 2 * FOLD, 1)
    for h in range(tiles):
        rolled = {}
        for k in range(2 * HS):
            v = raw[k, :, h * LANES : (h + 1) * LANES]
            for r in range(per_tile):
                rolled[k, r] = v if r == 0 else pltpu.roll(v, r * epd, 1)
        for q in range(per_tile):
            acc = rolled[0, (0 - q) % per_tile]
            for k in range(1, 2 * HS):
                acc = jnp.where(lane_group == k, rolled[k, (k - q) % per_tile], acc)
            tx[h * per_tile + q] = acc
    totals = jnp.sum(hits, axis=1, keepdims=True)
    row = jnp.zeros((1, LANES), F32)
    for k in range(2 * HS):
        row = jnp.where(lane_of == 3 * FOLD + k, jnp.broadcast_to(totals[k : k + 1], (1, LANES)), row)
    rowtx[...] = row
    mtx[0:1, :] = mtx[0:1, :] + row

    pl.semaphore_wait(barrier, tm - 1 + (ny - 1) * nz)

    def in_copy(k):
        return pltpu.make_async_remote_copy(
            src_ref=tx.at[lax.rem(z + k, nz)],
            dst_ref=rx.at[my_source],
            send_sem=tsend.at[0],
            recv_sem=trecv.at[my_source],
            device_id={"tm": dest_index(k), "env": me_e},
            device_id_type=MESH,
        )

    def in_arrival(i):
        return pltpu.make_async_remote_copy(
            src_ref=tx.at[0],
            dst_ref=rx.at[i],
            send_sem=tsend.at[0],
            recv_sem=trecv.at[i],
            device_id={"tm": dest_index(0), "env": me_e},
            device_id_type=MESH,
        )

    def mat_copy(k):
        return pltpu.make_async_remote_copy(
            src_ref=mtx,
            dst_ref=mrx.at[my_source],
            send_sem=msend.at[0],
            recv_sem=mrecv.at[my_source],
            device_id={"tm": dest_index(k), "env": me_e},
            device_id_type=MESH,
        )

    def mat_arrival(i):
        return pltpu.make_async_remote_copy(
            src_ref=mtx,
            dst_ref=mrx.at[i],
            send_sem=msend.at[0],
            recv_sem=mrecv.at[i],
            device_id={"tm": dest_index(0), "env": me_e},
            device_id_type=MESH,
        )

    def row_copy(k, r):
        return pltpu.make_async_remote_copy(
            src_ref=rowtx,
            dst_ref=rows.at[r, my_source],
            send_sem=rsend.at[0],
            recv_sem=rrecv.at[0],
            device_id={"tm": dest_index(k), "env": lax.rem(me_e + r, ny)},
            device_id_type=MESH,
        )

    def rows_all():
        return pltpu.make_async_remote_copy(
            src_ref=rows.at[pl.ds(1, ny - 1)],
            dst_ref=rows.at[pl.ds(1, ny - 1)],
            send_sem=rsend.at[0],
            recv_sem=rrecv.at[0],
            device_id={"tm": dest_index(0), "env": lax.rem(me_e + 1, ny)},
            device_id_type=MESH,
        )

    def other(k):
        return jnp.logical_not(jnp.logical_and(own_here, k == 0))

    def other_source(i):
        return jnp.logical_not(jnp.logical_and(own_here, i == my_source))

    for r in range(1, ny):
        for k in range(nz):
            row_copy(k, r).start()
    far_first = sorted(range(nz), key=lambda k: -min(k, nz - k))
    for make in (mat_copy, in_copy):
        for k in far_first:
            @pl.when(other(k))
            def _(k=k, make=make):
                make(k).start()

    @pl.when(own_here)
    def _():
        rx[my_source] = tx[z]
        mrx[my_source] = mtx[...]

    ratio = float(SUB)
    stiff, damp, gravity, cstiff, cdamp = (r[...] for r in (stiff, damp, gravity, cstiff, cdamp))
    to_u = TWO_PI / fine_dt
    scale = jnp.where(lane_of < DOF, TWO_PI, to_u)
    shrink = jnp.where(lane_of < DOF, 1.0 / TWO_PI, 1.0 / to_u)

    for ref in (changes, tstage, hstage, gains, tq, spring, fric, grav, cspring, cfric, ybuf, ubuf, ly, lu, ctmp, stage, wgt, cmap, qmap, bmap):
        clear(ref)
    for h in range(tiles):
        inits[h * LANES : (h + 1) * LANES, :] = (
            pad_rows(init[:, h * LANES : (h + 1) * LANES], LANES).T * shrink
        )
    start_state = inits[pl.ds(pl.multiple_of(z * epd, epd), epd), :]
    first_start = jnp.where(block_t == 0, start_state, 0.0)
    rank = lax.broadcasted_iota(jnp.int32, (DEPTH, DOF), 0)
    col = lax.broadcasted_iota(jnp.int32, (DEPTH, DOF), 1)
    for n in range(slices):
        cut = pl.ds(plan.where[n], DOF)
        ly[:, cut] = jnp.where(rank == col, 1.0, 0.0)
        lu[:, cut] = jnp.where(rank == col + DOF, 1.0, 0.0)
        grav[:, cut] = gravity
        gains[0, :, cut] = TWO_PI * stiff
        gains[1, :, cut] = TWO_PI * cstiff
        gains[2, :, cut] = to_u * damp
        gains[3, :, cut] = to_u * cdamp
        gains[4, :, cut] = TWO_PI * gravity
    ybuf[:, 0:DOF] = first_start[:, 0:DOF]
    ubuf[:, 0:DOF] = first_start[:, DOF : 2 * DOF]

    square_row = lax.broadcasted_iota(jnp.int32, (40, LANES), 0)
    for i in range(nz):
        @pl.when(other_source(i))
        def _(i=i):
            mat_arrival(i).wait_recv()

        folded = mrx[i]
        square = jnp.concatenate(
            [folded, pltpu.roll(folded, LANES - FOLD, 1), pltpu.roll(folded[0:8], LANES - 2 * FOLD, 1)], axis=0
        )
        shifted = pltpu.roll(square, LANES - 1, 1)
        turned = pad_rows(jnp.concatenate([square, shifted], axis=0), LANES).T
        matrices = (
            jnp.where(lane_of <= square_row, square, turned[0:40]),
            jnp.where(lane_of >= square_row, shifted, pltpu.roll(turned[0:40], LANES - 40, 1)),
        )
        for a in range(HS):
            n = HS * i + a
            cut = pl.ds(plan.where[n], DOF)
            g, pos = plan.slot[n]
            stage[g, pl.ds(pos * DOF, DOF), pl.ds(pos * DOF, DOF)] = (
                fine_dt * fine_dt / TWO_PI
            ) * matrices[a][0:DOF, 0:DOF]
    for g, (base, members, a) in enumerate(plan.groups):
        put(wgt, g, stage[g])

    def product(force, g):
        return through(force, wgt[g])

    if ny > 1:
        rows_all().wait_recv()
    counts = []
    for i in range(nz):
        total = mrx[i, 0:1, :]
        for r in range(1, ny):
            total = total + rows[r, i]
        counts.append(total * (1.0 / (env_local * ny)))
    for base, members, a in plan.groups:
        cut = pl.ds(base, LANES)
        for j in range(HS):
            spot = 3 * FOLD + a * HS + j
            mean = counts[members[0]][:, spot : spot + 1]
            for pos, i in enumerate(members):
                mean = jnp.where(lane_of >= pos * DOF, counts[i][:, spot : spot + 1], mean)
            cspring[j, :, cut] = gains[0, :, cut] + gains[4, :, cut] + mean * gains[1, :, cut]
            cfric[j, :, cut] = gains[2, :, cut] + mean * gains[3, :, cut]

    for g, (base, members, a) in enumerate(plan.groups):
        cut = pl.ds(base, LANES)
        y, u = ly[:, cut], lu[:, cut]
        for j in range(HS):
            force = -cspring[j, :, cut] * y - cfric[j, :, cut] * u
            u = u + ratio * product(force, g)
            y = y + ratio * u
        ly[:, cut] = y
        lu[:, cut] = u
    levels = slices.bit_length() - 1
    stacks = []
    for n in range(slices):
        cut = pl.ds(plan.where[n], DOF)
        ctmp[:, 0:DOF] = ly[:, cut]
        ctmp[:, DOF : 2 * DOF] = lu[:, cut]
        stacks.append(ctmp[...])

    def right_half(level):
        step = 1 << level
        found = []
        for m in range(0, slices, 2 * step):
            for i in range(step):
                found.append((level * (slices // 2) + len(found), m + step - 1, m + step + i))
        return found

    def steps(spine):
        return [
            [entry for entry in right_half(level) if ((entry[2] + 1) % (2 << level) == 0) == spine]
            for level in range(levels)
        ]


    for level in range(levels):
        for place, left, n in right_half(level):
            put(cmap, place, stacks[n])
        for place, left, n in right_half(level):
            stacks[n] = through(stacks[left], cmap[place])
    btx[...] = fold_map(stacks[slices - 1], lane_of)
    for n in range(slices):
        put(qmap, n, stacks[n])

    def sweep(ends, k):
        def advance(spine):
            for entries in steps(spine):
                for place, left, n in entries:
                    ends[n] = ends[n] + through(ends[left], cmap[place])

        advance(True)
        stx[k] = ends[slices - 1]
        send_blocks(functools.partial(sweep_copy, k))
        advance(False)
        for n in range(slices):
            ends_buf[n] = ends[n]

    def first_copy(d):
        return pltpu.make_async_remote_copy(
            src_ref=btx,
            dst_ref=brx.at[block_t],
            send_sem=bsend.at[0],
            recv_sem=brecv.at[0],
            device_id={"tm": block_index(block_t + d), "env": me_e},
            device_id_type=MESH,
        )

    def sweep_copy(k, d):
        return pltpu.make_async_remote_copy(
            src_ref=stx.at[k],
            dst_ref=srx.at[k, block_t],
            send_sem=ssend.at[k],
            recv_sem=srecv.at[k],
            device_id={"tm": block_index(block_t + d), "env": me_e},
            device_id_type=MESH,
        )

    def whole_copy(ref, send, recv):
        return pltpu.make_async_remote_copy(
            src_ref=ref, dst_ref=ref, send_sem=send, recv_sem=recv,
            device_id={"tm": block_index(lax.rem(block_t + 1, blocks)), "env": me_e},
            device_id_type=MESH,
        )

    def first_whole(count):
        return whole_copy(brx.at[pl.ds(0, count)], bsend.at[0], brecv.at[0])

    def sweep_whole(k, count):
        return whole_copy(srx.at[k, pl.ds(0, count)], ssend.at[k], srecv.at[k])

    def send_blocks(copy):
        for d in range(1, blocks):
            @pl.when(block_t + d < blocks)
            def _(d=d):
                copy(d).start()

    def await_blocks(whole, skip=0):
        for count in range(1, blocks - skip):
            @pl.when(block_t - skip == count)
            def _(count=count):
                whole(count).wait_recv()

    def drain_blocks(whole):
        for count in range(1, blocks):
            @pl.when(blocks - 1 - block_t == count)
            def _(count=count):
                whole(count).wait_send()

    @pl.when(block_t > 0)
    def _():
        send_blocks(first_copy)

    for part in range(0, nz, plan.per):
        for pos, i in enumerate(range(part, min(part + plan.per, nz))):
            @pl.when(other_source(i))
            def _(i=i):
                in_arrival(i).wait_recv()

            tstage[part // plan.per, pos * DOF : (pos + 1) * DOF, :] = rx[i, 0:DOF, :]
            hstage[part // plan.per, pos * DOF : (pos + 1) * DOF, :] = jnp.broadcast_to(
                rx[i, DOF : DOF + 1, :], (DOF, LANES)
            )
        turned = tstage[part // plan.per].T
        touched = hstage[part // plan.per].T
        for a in range(HS):
            base = (part // plan.per * HS + a) * LANES
            cut = pl.ds(base, LANES)
            for j in range(HS):
                k = a * HS + j
                hit = touched[k * epd : (k + 1) * epd, :]
                tq[j, :, cut] = turned[k * epd : (k + 1) * epd, :]
                spring[j, :, cut] = gains[0, :, cut] + hit * gains[1, :, cut]
                fric[j, :, cut] = gains[2, :, cut] + hit * gains[3, :, cut]

    for g, (base, members, a) in enumerate(plan.groups):
        cut = pl.ds(base, LANES)
        y, u = ybuf[:, cut], ubuf[:, cut]
        for j in range(HS):
            force = tq[j, :, cut] - cspring[j, :, cut] * y - cfric[j, :, cut] * u
            u = u + ratio * product(force, g)
            y = y + ratio * u
        ybuf[:, cut] = y
        ubuf[:, cut] = u

    def packed_state(n):
        cut = pl.ds(plan.where[n], DOF)
        zero = jnp.zeros((epd, LANES - 2 * DOF), F32)
        return jnp.concatenate([ybuf[:, cut], ubuf[:, cut], zero], axis=1)

    ends = [packed_state(n) for n in range(slices)]
    sweep(ends, 0)
    await_blocks(first_whole, 1)
    eye = jnp.where(
        lax.broadcasted_iota(jnp.int32, (DEPTH, LANES), 0) == lane_of, 1.0, 0.0
    )
    maps = {t: jnp.where(t < block_t, unfold_map(brx[t], lane_of), eye) for t in range(1, blocks - 1)}
    pieces = {(t, t): maps[t] for t in maps}

    def join(a, b, c):
        if (a, c) not in pieces:
            slot = weights.setdefault((b, c), len(weights))
            if slot == len(weights) - 1:
                put(bmap, slot, pieces[b, c])
            pieces[a, c] = through(pieces[a, b - 1], bmap[slot])

    weights = {}
    top = blocks - 2
    span = 1
    while span < blocks:
        for last in range(top, 0, -2 * span):
            mid = last - span + 1
            if mid <= 1:
                continue
            for first in range(max(1, mid - span), mid):
                join(first, mid, last)
        span *= 2
    for t in range(blocks - 2):
        if (t + 1, top) not in weights:
            weights[t + 1, top] = len(weights)
            put(bmap, weights[t + 1, top], pieces[t + 1, top])

    def enter(k):
        total = jnp.where(blocks - 2 < block_t, srx[k, blocks - 2], 0.0)
        for t in range(blocks - 2):
            total = total + through(jnp.where(t < block_t, srx[k, t], 0.0), bmap[weights[t + 1, top]])
        return total

    await_blocks(functools.partial(sweep_whole, 0))
    entry = enter(0)
    xs[0] = jnp.where(block_t == 0, start_state, entry)
    for n in range(slices):
        xs[n + 1] = ends_buf[n] + through(entry, qmap[n])

    def largest(k, corrections):
        worst = jnp.zeros((epd, 1), F32)
        for n in range(slices):
            real = changes[n] * scale
            worst = jnp.maximum(worst, jnp.sum(real * real, axis=1, keepdims=True))
        return jnp.where(lane_of == k, jnp.sqrt(worst), corrections)

    def iteration(k, corrections):
        for n in range(slices):
            cut = pl.ds(plan.where[n], DOF)
            ybuf[:, cut] = xs[n, :, 0:DOF]
            ubuf[:, cut] = xs[n, :, DOF : 2 * DOF]
        for j in range(HS):

            def substep(counter, carry):
                result = []
                for g, (base, members, a) in enumerate(plan.groups):
                    y, u = carry[g]
                    cut = pl.ds(base, LANES)
                    t = y - jnp.round(y)
                    s = t * t
                    s2 = s * s
                    poly = ((SIN[0] + SIN[1] * s) + s2 * (SIN[2] + SIN[3] * s)) + (s2 * s2) * (SIN[4] + SIN[5] * s)
                    force = (
                        tq[j, :, cut]
                        - spring[j, :, cut] * y
                        - fric[j, :, cut] * u
                        - (grav[:, cut] * t) * poly
                    )
                    change = product(force, g)
                    result.append(((y + u) + change, u + change))
                return tuple(result)

            first_state = tuple(
                (ybuf[:, pl.ds(base, LANES)], ubuf[:, pl.ds(base, LANES)])
                for base, members, a in plan.groups
            )
            last = lax.fori_loop(0, SUB, substep, first_state, unroll=UNROLL)
            for g, (base, members, a) in enumerate(plan.groups):
                ybuf[:, pl.ds(base, LANES)] = last[g][0]
                ubuf[:, pl.ds(base, LANES)] = last[g][1]

        ends = [packed_state(n) - xs[n + 1] for n in range(slices)]
        sweep(ends, k + 1)
        corrections = largest(k - 1, corrections)
        await_blocks(functools.partial(sweep_whole, k + 1))
        entry = enter(k + 1)
        xs[0] = xs[0] + entry
        for n in range(slices):
            change = ends_buf[n] + through(entry, qmap[n])
            changes[n] = change
            xs[n + 1] = xs[n + 1] + change
        return corrections

    corrections = lax.fori_loop(0, ITERS, iteration, jnp.zeros((epd, LANES), F32))
    corrections = largest(ITERS - 1, corrections)

    turned = pad_rows(corrections, LANES).T
    row = turned[0:1]
    for k in range(1, ITERS):
        row = jnp.where(lane_group == k, pltpu.roll(turned[k : k + 1], k * epd, 1), row)
    ctx[...] = row

    def corr_copy(k):
        return pltpu.make_async_remote_copy(
            src_ref=ctx,
            dst_ref=crx.at[k],
            send_sem=csend.at[0],
            recv_sem=crecv.at[0],
            device_id={"tm": lax.rem(me_t + k, tm), "env": me_e},
            device_id_type=MESH,
        )

    @pl.loop(1, tm, unroll=True)
    def _(k):
        corr_copy(k).start()

    for i in range(nz):
        parts = []
        for a in range(HS):
            real = xs[HS * i + a + 1] * scale
            parts.append(real)
            parts.append(pltpu.roll(real, LANES - DOF, 1))
        otx[i] = jnp.concatenate(parts, axis=0).T[0:ROWS_OUT, :]

    def out_copy(i):
        return pltpu.make_async_remote_copy(
            src_ref=otx.at[i],
            dst_ref=orx.at[z],
            send_sem=osend.at[0],
            recv_sem=orecv.at[z],
            device_id={"tm": source_index(i), "env": me_e},
            device_id_type=MESH,
        )

    def out_arrival(k):
        return pltpu.make_async_remote_copy(
            src_ref=otx.at[0],
            dst_ref=orx.at[lax.rem(z + k, nz)],
            send_sem=osend.at[0],
            recv_sem=orecv.at[lax.rem(z + k, nz)],
            device_id={"tm": dest_index(k), "env": me_e},
            device_id_type=MESH,
        )

    @pl.loop(0, nz)
    def _(i):
        @pl.when(other_source(i))
        def _():
            out_copy(i).start()

    crx[0] = ctx[...]

    @pl.when(own_here)
    def _():
        orx[z] = otx[my_source]

    @pl.loop(0, nz)
    def _(k):
        @pl.when(other(k))
        def _():
            out_arrival(k).wait_recv()

    for h in range(tiles):
        for k in range(2 * HS):
            a, half_state = divmod(k, 2)
            tile = None
            for q in range(per_tile):
                r = (q - k) % per_tile
                v = orx[h * per_tile + q]
                v = v if r == 0 else pltpu.roll(v, r * epd, 1)
                tile = v if tile is None else jnp.where(lane_group == q, v, tile)
            out[half_state * DOF : half_state * DOF + DOF, a, h * LANES : (h + 1) * LANES] = tile[0:DOF]

    pltpu.make_async_remote_copy(
        src_ref=crx.at[pl.ds(1, tm - 1)],
        dst_ref=crx.at[pl.ds(1, tm - 1)],
        send_sem=csend.at[0],
        recv_sem=crecv.at[0],
        device_id={"tm": lax.rem(me_t + 1, tm), "env": me_e},
        device_id_type=MESH,
    ).wait()
    worst = []
    for p in range(nz):
        most = None
        for t in range(blocks):
            sender = t // CORES * line + p * CORES + t % CORES
            value = crx[lax.rem(me_t - sender + tm, tm)]
            most = value if most is None else jnp.maximum(most, value)
        worst.append(most)
    for h in range(tiles):
        for k in range(ITERS):
            tile = None
            for q in range(per_tile):
                r = (q - k) % per_tile
                v = worst[h * per_tile + q]
                v = v if r == 0 else pltpu.roll(v, r * epd, 1)
                tile = v if tile is None else jnp.where(lane_group == q, v, tile)
            corr_out[k : k + 1, h * LANES : (h + 1) * LANES] = tile

    def drain(ref, sem, count):
        whole_copy(ref.at[pl.ds(0, count)], sem.at[0], sem.at[0]).wait_send()

    for ref, sem in ((mrx, msend), (tx, tsend), (otx, osend)):
        @pl.when(own_here)
        def _(ref=ref, sem=sem):
            drain(ref, sem, nz - 1)

        @pl.when(jnp.logical_not(own_here))
        def _(ref=ref, sem=sem):
            drain(ref, sem, nz)

    if ny > 1:
        rows_all().wait_send()

    @pl.when(block_t > 0)
    def _():
        drain_blocks(first_whole)

    for k in range(ITERS + 1):
        drain_blocks(functools.partial(sweep_whole, k))


def body(tm, env, init_state, torque, contact, mass_inverse, stiffness, damping, gravity,
         contact_stiffness, contact_damping):
    nz = NZ
    env_local = init_state.shape[1]
    epd = env_local // nz
    slices = HS * nz
    blocks = tm // (nz * CORES) * CORES
    plan = Plan(nz)
    groups = len(plan.groups)
    lanes = plan.lanes
    vm = pltpu.VMEM
    dma = pltpu.SemaphoreType.DMA
    vmem = pl.BlockSpec(memory_space=pltpu.VMEM)
    both = vm((HS, epd, lanes), F32)
    thin = vm((HS, 1, lanes), F32)
    levels = slices.bit_length() - 1
    prm = [p.reshape(1, DOF) for p in (stiffness, damping, gravity, contact_stiffness, contact_damping)]
    states, corrections = pl.pallas_call(
        functools.partial(kernel, tm, env),
        out_shape=(
            vm((STATE, HS, env_local), F32),
            vm((ITERS, env_local), F32),
        ),
        in_specs=[pl.BlockSpec(memory_space=pl.ANY)] * 9,
        out_specs=(vmem, vmem),
        scratch_shapes=[
            vm(init_state.shape, F32), vm((DOF, 2 * HS, env_local), F32), vm(contact.shape, jnp.int32),
            vm((DOF, HS, DOF), F32), *[vm((1, DOF), F32)] * 5,
            vm((nz, ROWS_IN, LANES), F32), vm((nz, ROWS_IN, LANES), F32),
            vm((ROWS_MAT, LANES), F32), vm((nz, ROWS_MAT, LANES), F32),
            vm((1, LANES), F32), vm((env, nz, 1, LANES), F32),
            vm((2 * HS, 40, env_local), F32), vm((env_local, LANES), F32),
            *[vm((-(-nz // plan.per), LANES, LANES), F32)] * 2, vm((5, 1, lanes), F32),
            both, both, both, vm((1, lanes), F32), thin, thin,
            vm((groups, WIDE, WIDE), BF16), vm((groups, LANES, LANES), F32), vm((LANES, LANES), F32),
            vm((epd, lanes), F32), vm((epd, lanes), F32),
            vm((DEPTH, lanes), F32), vm((DEPTH, lanes), F32),
            vm((levels * slices // 2, WIDE, WIDE), BF16),
            vm((slices, WIDE, WIDE), BF16), vm((2 * blocks, WIDE, WIDE), BF16),
            vm((DEPTH, LANES), F32),
            vm((slices + 1, epd, LANES), F32), vm((slices, epd, LANES), F32), vm((slices, epd, LANES), F32),
            vm((ROWS_MAP, LANES), F32), vm((blocks, ROWS_MAP, LANES), F32),
            vm((ITERS + 1, epd, LANES), F32), vm((ITERS + 1, blocks, epd, LANES), F32),
            vm((nz, ROWS_OUT, LANES), F32), vm((nz, ROWS_OUT, LANES), F32),
            vm((1, LANES), F32), vm((tm, 1, LANES), F32),
            dma((9,)), dma((1,)), dma((nz,)), dma((1,)), dma((nz,)), dma((1,)), dma((1,)),
            dma((1,)), dma((1,)), dma((ITERS + 1,)), dma((ITERS + 1,)),
            dma((1,)), dma((nz,)), dma((1,)), dma((1,)),
        ],
        compiler_params=pltpu.CompilerParams(collective_id=0, has_side_effects=True),
        name="parareal",
    )(
        init_state, torque.transpose(1, 0, 2), contact, mass_inverse.transpose(1, 0, 2), *prm
    )
    return states.transpose(1, 0, 2), corrections


def solution(mesh):
    placed = (
        P(None, "env"),
        P("tm", None, "env"),
        P("tm", "env"),
        P("tm", None, None),
        P(),
        P(),
        P(),
        P(),
        P(),
    )
    return jax.shard_map(
        functools.partial(body, mesh.shape["tm"], mesh.shape["env"]),
        mesh=mesh,
        in_specs=placed,
        out_specs=(P("tm", None, "env"), P(None, "env")),
        check_vma=False,
    )
```
